128 devices in a mesh: dp: 1, ep: 128 (over z, y, x, core).
Axes of the slice: x: 4, y: 4, z: 4, core: 2. Of those that a mesh axis runs over, the one named last changes fastest.
Arguments:
- tok_x: bfloat16 [16384, 2048], P(('dp', 'ep'))
- expert_ids: int32 [16384, 8], P(('dp', 'ep'))
- gates: float32 [16384, 8], P(('dp', 'ep'))
- hot_tok: int32 [8192], P(('dp', 'ep'))
- hot_gates: float32 [8192], P(('dp', 'ep'))
- w_gate: bfloat16 [128, 2048, 768], P('ep')
- w_up: bfloat16 [128, 2048, 768], P('ep')
- w_down: bfloat16 [128, 768, 2048], P('ep')
Outputs:
- output: bfloat16 [16384, 2048], P(('dp', 'ep'))
All inputs are finite; a program needn't handle non-finite values.
Results may differ from the reference program's by a relative error of at most 0.00787365.
Values are sent between devices in bfloat16 or wider.
A program may use at most 1 GiB of HBM per device.

```python
import jax
import jax.numpy as jnp
from jax import lax

GROUP_SIZE = 128
TOKENS = 128
D_MODEL = 2048
D_FF = 768
EXPERTS = 128
TOP_K = 8
HOT_ROWS = 64

COLD_CAP = (TOKENS * TOP_K + EXPERTS - 2) // (EXPERTS - 1)


def draw_routing(key):
    key_rows, key_label, key_hot = jax.random.split(key, 3)
    row_perm = jax.random.permutation(key_rows, TOKENS)
    label_perm = jax.random.permutation(key_label, EXPERTS - 1)
    route_num = (row_perm[:, None] * TOP_K + jnp.arange(TOP_K)[None, :]) % (EXPERTS - 1)
    chip_ids = 1 + label_perm[route_num]
    hot_list = jax.random.permutation(key_hot, TOKENS)[:HOT_ROWS]
    return chip_ids.astype(jnp.int32), hot_list.astype(jnp.int32)


def setup_inputs(seed: int = 0, part: int = 0) -> dict:
    base_key = jax.random.key(seed)
    key_wg, key_wu, key_wd = jax.random.split(base_key, 3)
    part_key = jax.random.fold_in(base_key, part)
    key_x, key_route, key_gate, key_hot = jax.random.split(part_key, 4)
    row_count = GROUP_SIZE * TOKENS
    tok_x = jax.random.normal(key_x, (row_count, D_MODEL), jnp.float32).astype(jnp.bfloat16)
    chip_ids, hot_list = jax.vmap(draw_routing)(jax.random.split(key_route, GROUP_SIZE))
    gates = jax.random.uniform(key_gate, (row_count, TOP_K), jnp.float32, 0.5, 1.5) * TOP_K ** -0.5
    hot_gates = jax.random.uniform(key_hot, (GROUP_SIZE * HOT_ROWS,), jnp.float32, 0.5, 1.5)
    w_gate = (jax.random.normal(key_wg, (EXPERTS, D_MODEL, D_FF), jnp.float32) * D_MODEL ** -0.5).astype(jnp.bfloat16)
    w_up = (jax.random.normal(key_wu, (EXPERTS, D_MODEL, D_FF), jnp.float32) * D_MODEL ** -0.5).astype(jnp.bfloat16)
    w_down = (jax.random.normal(key_wd, (EXPERTS, D_FF, D_MODEL), jnp.float32) * D_FF ** -0.5).astype(jnp.bfloat16)
    return {'tok_x': tok_x, 'expert_ids': chip_ids.reshape(row_count, TOP_K), 'gates': gates,
            'hot_tok': hot_list.reshape(GROUP_SIZE * HOT_ROWS), 'hot_gates': hot_gates,
            'w_gate': w_gate, 'w_up': w_up, 'w_down': w_down}


def swiglu_rows(in_rows, w_gate_e, w_up_e, w_down_e):
    gate_act = jnp.dot(in_rows, w_gate_e, preferred_element_type=jnp.float32)
    up_act = jnp.dot(in_rows, w_up_e, preferred_element_type=jnp.float32)
    hidden = (jax.nn.silu(gate_act) * up_act).astype(jnp.bfloat16)
    return jnp.dot(hidden, w_down_e, preferred_element_type=jnp.float32).astype(jnp.bfloat16)


def reference(tok_x, expert_ids, gates, hot_tok, hot_gates, w_gate, w_up, w_down):
    routes = GROUP_SIZE * TOKENS * TOP_K
    flat_ids = expert_ids.reshape(routes)
    flat_gates = gates.reshape(routes)
    max_rows = GROUP_SIZE * COLD_CAP

    def expert_step(y_sum, expert_args):
        expert, w_gate_e, w_up_e, w_down_e = expert_args
        found_pos = jnp.nonzero(flat_ids == expert, size=max_rows, fill_value=routes)[0]
        in_range = found_pos < routes
        safe_pos = jnp.minimum(found_pos, routes - 1)
        tok_rows = safe_pos // TOP_K
        weight = jnp.where(in_range, flat_gates[safe_pos], 0.0)
        expert_out = swiglu_rows(tok_x[tok_rows], w_gate_e, w_up_e, w_down_e)
        y_sum = y_sum.at[tok_rows].add(weight[:, None] * expert_out.astype(jnp.float32))
        return y_sum, None

    y_start = jnp.zeros((GROUP_SIZE * TOKENS, D_MODEL), jnp.float32)
    y_sum, unused = lax.scan(expert_step, y_start, (jnp.arange(EXPERTS, dtype=jnp.int32), w_gate, w_up, w_down))
    chip_base = (jnp.arange(GROUP_SIZE * HOT_ROWS, dtype=jnp.int32) // HOT_ROWS) * TOKENS
    hot_rows_idx = chip_base + hot_tok
    hot_out = swiglu_rows(tok_x[hot_rows_idx], w_gate[0], w_up[0], w_down[0])
    y_sum = y_sum.at[hot_rows_idx].add(hot_gates[:, None] * hot_out.astype(jnp.float32))
    return y_sum.astype(jnp.bfloat16)
```

```python
import functools

import jax
import jax.numpy as jnp
from jax import lax
from jax.experimental import pallas as pl
from jax.experimental.pallas import tpu as pltpu
from jax.sharding import PartitionSpec as P

F32 = jnp.float32
BF16 = jnp.bfloat16
SLOTS = 8
FOLD = 8
VMEM_LIMIT = 60 * 1024 * 1024


def dotf(a, b):
    return jnp.dot(a, b, preferred_element_type=F32)


def iota(shape, dim):
    return lax.broadcasted_iota(jnp.int32, shape, dim)


def dispatch_kernel(ids_ref, x_ref, out_ref):
    top_k, tokens = ids_ref.shape
    d_model = x_ref.shape[1]
    rows = out_ref.shape[0]
    piece = d_model // FOLD
    row = iota((rows, tokens), 0)
    expert = row // SLOTS
    member = jnp.zeros((rows, tokens), jnp.bool_)
    for j in range(top_k):
        member = jnp.logical_or(member, ids_ref[j:j + 1, :] == expert)
    member_f = jnp.where(member, 1.0, 0.0)
    earlier = jnp.where(iota((tokens, tokens), 0) < iota((tokens, tokens), 1), 1.0, 0.0).astype(BF16)
    rank = dotf(member_f.astype(BF16), earlier)
    slot = (row % SLOTS).astype(F32)
    pick = jnp.where(rank == slot, member_f, 0.0).astype(BF16)
    ninth = jnp.where(rank == float(SLOTS), member_f, 0.0)
    for c in range(0, d_model, 512):
        out_ref[:, c:c + 512] = dotf(pick, x_ref[:, c:c + 512]).astype(BF16)
    total = jnp.zeros((rows, piece), F32)
    for f in range(FOLD):
        pick_f = jnp.where(slot == float(f), ninth, 0.0).astype(BF16)
        total += dotf(pick_f, x_ref[:, f * piece:(f + 1) * piece])
    out_ref[:, d_model:] = total.astype(BF16)


def expert_kernel(in_ref, wg_ref, wu_ref, wd_ref, out_ref, x_ref, u_ref):
    step = pl.program_id(0)
    rows = in_ref.shape[0]
    d_model = wg_ref.shape[0]
    width = wg_ref.shape[1]
    groups = rows // SLOTS
    piece = d_model // FOLD
    all_rows = rows + groups

    @pl.when(step == 0)
    def _():
        x_ref[:rows] = in_ref[:, :d_model]
        for f in range(FOLD):
            pick = jnp.where(iota((groups, rows), 1) == iota((groups, rows), 0) * FOLD + f, 1.0, 0.0).astype(BF16)
            x_ref[rows:, f * piece:(f + 1) * piece] = dotf(pick, in_ref[:, d_model:]).astype(BF16)

    half = all_rows // 2
    for m in range(2):
        sl = slice(m * half, (m + 1) * half)
        gate = dotf(x_ref[sl], wg_ref[...])
        up = dotf(x_ref[sl], wu_ref[...])
        u_ref[sl, pl.ds(pl.multiple_of(step * width, width), width)] = (jax.nn.silu(gate) * up).astype(BF16)

    @pl.when(step == pl.num_programs(0) - 1)
    def _():
        total = jnp.zeros((rows, piece), F32)
        for f in range(FOLD):
            cols = slice(f * piece, (f + 1) * piece)
            out = dotf(u_ref[...], wd_ref[:, cols]).astype(BF16)
            out_ref[:, cols] = out[:rows]
            spread = jnp.where(iota((rows, groups), 0) == iota((rows, groups), 1) * FOLD + f, 1.0, 0.0).astype(BF16)
            total += dotf(spread, out[rows:])
        out_ref[:, d_model:] = total.astype(BF16)


def hot_kernel(x_ref, wg_ref, wu_ref, wd_ref, out_ref, acc_ref):
    step = pl.program_id(0)
    gate = dotf(x_ref[...], wg_ref[...])
    up = dotf(x_ref[...], wu_ref[...])
    part = dotf((jax.nn.silu(gate) * up).astype(BF16), wd_ref[...])

    @pl.when(step == 0)
    def _():
        acc_ref[...] = part

    @pl.when(step > 0)
    def _():
        acc_ref[...] += part

    @pl.when(step == pl.num_programs(0) - 1)
    def _():
        out_ref[...] = acc_ref[...].astype(BF16)


def three_terms(a):
    hi = a.astype(BF16)
    rest = a - hi.astype(F32)
    mid = rest.astype(BF16)
    low = (rest - mid.astype(F32)).astype(BF16)
    return jnp.concatenate([hi, mid, low], axis=0)


def combine_kernel(ids_ref, gates_ref, hot_tok_ref, hot_gate_ref, hot_ref, back_ref, y_ref):
    tokens, top_k = ids_ref.shape
    rows = back_ref.shape[0]
    d_model = y_ref.shape[1]
    piece = d_model // FOLD
    col = iota((tokens, rows), 1)
    expert = col // SLOTS
    member = jnp.zeros((tokens, rows), jnp.bool_)
    weight = jnp.zeros((tokens, rows), F32)
    for j in range(top_k):
        here = ids_ref[:, j:j + 1] == expert
        member = jnp.logical_or(member, here)
        weight = jnp.where(here, gates_ref[:, j:j + 1], weight)
    earlier = jnp.where(iota((tokens, tokens), 1) < iota((tokens, tokens), 0), 1.0, 0.0).astype(BF16)
    rank = dotf(earlier, jnp.where(member, 1.0, 0.0).astype(BF16))
    slot = (col % SLOTS).astype(F32)
    main = three_terms(jnp.where(rank == slot, weight, 0.0))
    ninth = three_terms(jnp.where(rank == float(SLOTS), weight, 0.0))
    slot3 = (iota((3 * tokens, rows), 1) % SLOTS)
    count = hot_tok_ref.shape[1]
    same = iota((tokens, count), 0) == hot_tok_ref[...]
    hot_weight = jnp.sum(jnp.where(same, hot_gate_ref[...], 0.0), axis=1, keepdims=True)
    is_hot = jnp.sum(jnp.where(same, 1.0, 0.0), axis=1, keepdims=True) > 0.5
    for f in range(FOLD):
        cols = slice(f * piece, (f + 1) * piece)
        ninth_f = jnp.where(slot3 == f, ninth, jnp.zeros_like(ninth))
        terms = dotf(main, back_ref[:, cols]) + dotf(ninth_f, back_ref[:, d_model:])
        total = terms[2 * tokens:] + terms[tokens:2 * tokens] + terms[:tokens]
        hot = jnp.where(is_hot, hot_weight * hot_ref[:, cols].astype(F32), 0.0)
        y_ref[:, cols] = (total + hot).astype(BF16)


def vmem(n):
    return [pl.BlockSpec(memory_space=pltpu.VMEM)] * n


def params(**kw):
    return pltpu.CompilerParams(vmem_limit_bytes=VMEM_LIMIT, **kw)


def solution(mesh):
    group_size = mesh.shape['ep']
    row_spec = P(('dp', 'ep'), None)
    list_spec = P(('dp', 'ep'))
    expert_spec = P('ep', None, None)

    def local_layer(x, ids, gates, hot_tok, hot_gates, wg, wu, wd):
        wg, wu, wd = wg[0], wu[0], wd[0]
        tokens, d_model = x.shape
        d_ff = wg.shape[1]
        rows = group_size * SLOTS
        width = d_model + d_model // FOLD
        split = 3
        blk = d_ff // split

        first = lax.axis_index('ep') == 0
        hot_w = [lax.psum(jnp.where(first, w, jnp.zeros_like(w)), 'ep') for w in (wg, wu, wd)]

        send = pl.pallas_call(
            dispatch_kernel, out_shape=jax.ShapeDtypeStruct((rows, width), BF16),
            in_specs=vmem(2), out_specs=vmem(1)[0], compiler_params=params(), name="dispatch",
        )(ids.T, x)
        recv = lax.all_to_all(send.reshape(group_size, SLOTS, width), 'ep', 0, 0, tiled=True)
        whole = lambda shape: pl.BlockSpec(shape, lambda i: (0, 0))
        wide = pl.BlockSpec((d_model, blk), lambda i: (0, i))
        out = pl.pallas_call(
            expert_kernel, out_shape=jax.ShapeDtypeStruct((rows, width), BF16), grid=(split,),
            in_specs=[whole((rows, width)), wide, wide, whole((d_ff, d_model))],
            out_specs=whole((rows, width)),
            scratch_shapes=[pltpu.VMEM((rows + group_size, d_model), BF16), pltpu.VMEM((rows + group_size, d_ff), BF16)],
            compiler_params=params(), name="expert",
        )(recv.reshape(rows, width), wg, wu, wd)
        back = lax.all_to_all(out.reshape(group_size, SLOTS, width), 'ep', 0, 0, tiled=True)
        hot_out = pl.pallas_call(
            hot_kernel, out_shape=jax.ShapeDtypeStruct((tokens, d_model), BF16), grid=(split,),
            in_specs=[whole((tokens, d_model)), wide, wide, pl.BlockSpec((blk, d_model), lambda i: (i, 0))],
            out_specs=whole((tokens, d_model)), scratch_shapes=[pltpu.VMEM((tokens, d_model), F32)],
            compiler_params=params(), name="hot",
            cost_estimate=pl.CostEstimate(flops=6 * tokens * d_model * d_ff, bytes_accessed=6 * d_model * d_ff, transcendentals=0),
        )(x, *hot_w)
        return pl.pallas_call(
            combine_kernel, out_shape=jax.ShapeDtypeStruct((tokens, d_model), BF16),
            in_specs=vmem(6), out_specs=vmem(1)[0], compiler_params=params(), name="combine",
        )(ids, gates, hot_tok[None, :], hot_gates[None, :], hot_out, back.reshape(rows, width))

    return jax.shard_map(local_layer, mesh=mesh,
                         in_specs=(row_spec, row_spec, row_spec, list_spec, list_spec, expert_spec, expert_spec, expert_spec),
                         out_specs=row_spec, check_vma=False)
```

```python
import functools

import jax
import jax.numpy as jnp
from jax import lax
from jax.experimental import pallas as pl
from jax.experimental.pallas import tpu as pltpu
from jax.sharding import PartitionSpec as P

F32 = jnp.float32
BF16 = jnp.bfloat16
SLOTS = 8
FOLD = 8
VMEM_LIMIT = 60 * 1024 * 1024


def dotf(a, b):
    return jnp.dot(a, b, preferred_element_type=F32)


def iota(shape, dim):
    return lax.broadcasted_iota(jnp.int32, shape, dim)


def ones_where(mask):
    return jnp.where(mask, 1.0, 0.0).astype(BF16)


def three_terms(a):
    hi = a.astype(BF16)
    rest = a - hi.astype(F32)
    mid = rest.astype(BF16)
    low = (rest - mid.astype(F32)).astype(BF16)
    return jnp.concatenate([hi, mid, low], axis=0)


def layer_kernel(n, ids_t_ref, ids_ref, gates_ref, hot_tok_ref, hot_gate_ref, x_ref, wg_ref, wu_ref, wd_ref, y_ref,
                 send, recv, out, back, wg, wu, wd, hot_g, hot_u, hot_d, stage_g, stage_u, stage_d,
                 rows_ref, u_ref, fold_ref, weight_ref, acc_ref,
                 load_sem, send_sem, recv_sem, ret_sem, back_sem, from_sem, to_sem):
    me = lax.axis_index('ep')
    devices = 2 * n * n * n
    c, mx, my, mz = me % 2, (me // 2) % n, (me // (2 * n)) % n, me // (2 * n * n)
    blocks = 2 * n * n
    tokens, d_model = x_ref.shape
    d_ff = wd_ref.shape[0]
    top_k = ids_ref.shape[1]
    piece = d_model // FOLD
    main = blocks * SLOTS
    chunk_rows = main + blocks

    def device(z, y, x, core):
        return ((z % n * n + y % n) * n + x % n) * 2 + core % 2

    def peer(q, i, sign):
        kc, kx, ky = i % 2, (i // 2) % n, i // (2 * n)
        kz = (q + 2 * n - kx - ky) % n
        if sign > 0:
            return device(mz + kz, my + ky, mx + kx, c + kc)
        return device(mz + n - kz, my + n - ky, mx + n - kx, c + kc)

    def remote(src, dst, s_sem, r_sem, to):
        return pltpu.make_async_remote_copy(src_ref=src, dst_ref=dst, send_sem=s_sem, recv_sem=r_sem, device_id={'ep': to},
                                            device_id_type=pl.DeviceIdType.MESH)

    def wait_for(ref, sem):
        pltpu.make_async_copy(ref, ref, sem).wait()

    def rows_at(ref, start, size, unit):
        return ref.at[pl.ds(pl.multiple_of(start, unit), size)]

    barrier = pltpu.get_barrier_semaphore()

    @pl.loop(1, devices)
    def _(i):
        pl.semaphore_signal(barrier, inc=1, device_id={'ep': (me + i) % devices}, device_id_type=pl.DeviceIdType.MESH)

    own = [pltpu.make_async_copy(src, dst, load_sem.at[p])
           for p, (src, dst) in enumerate(((wg_ref, wg), (wu_ref, wu), (wd_ref, wd)))]
    for copy in own:
        copy.start()

    unit = d_model // (2 * n * n * n)
    unit_d, unit_c = d_ff // (n * n), d_model // (2 * n)
    parts = ((wg_ref, hot_g, stage_g, mz, (my, mx)), (wu_ref, hot_u, stage_u, mx, (mz, my)), (wd_ref, hot_d, stage_d, my, (mx, mz)))

    def line_device(p, k, core):
        return (device(k, my, mx, core), device(mz, my, k, core), device(mz, k, mx, core))[p]

    def plane_device(p, a, b):
        return (device(mz, a, b, c), device(a, b, mx, c), device(b, my, a, c))[p]

    def quarter(p, ref, half, k):
        if p < 2:
            size = n * n * unit
            return rows_at(ref, half * (d_model // 2) + k * size, size, 16)
        size = n * unit_d
        return ref.at[pl.ds(pl.multiple_of(k * size, 16), size), pl.ds(pl.multiple_of(half * (d_model // 2), 128), d_model // 2)]

    def hot_piece(p, ref, half, k, a, b):
        if p < 2:
            return rows_at(ref, half * (d_model // 2) + k * (n * n * unit) + (a * n + b) * unit, unit, 16)
        return ref.at[pl.ds(pl.multiple_of(k * (n * unit_d) + a * unit_d, 16), unit_d),
                      pl.ds(pl.multiple_of(half * (d_model // 2) + b * unit_c, 128), unit_c)]

    def stage_piece(p, ref, a, b):
        if p < 2:
            return rows_at(ref, (a * n + b) * unit, unit, 16)
        return ref.at[pl.ds(pl.multiple_of(a * unit_d, 16), unit_d), pl.ds(pl.multiple_of(b * unit_c, 128), unit_c)]

    def pieces_like(p, ref):
        if p < 2:
            return ref.at[pl.ds(0, (n * n - 1) * unit)]
        return ref.at[pl.ds(0, (n * n - 1) * unit_d), pl.ds(0, unit_c)]

    def on_line(p):
        plane = parts[p][4]
        return jnp.logical_and(plane[0] == 0, plane[1] == 0)

    def hot_root():
        @pl.when(me == 0)
        def _():
            for p, (src, _, stage, _, _) in enumerate(parts):
                for k in range(n):
                    for half in range(2):
                        if k == 0 and half == 0:
                            pltpu.make_async_copy(quarter(p, src, 0, 0), stage, to_sem.at[0, p]).start()
                        else:
                            remote(quarter(p, src, half, k), stage, from_sem.at[0, p], to_sem.at[0, p], line_device(p, k, half)).start()

    def hot_scatter():
        for p, (_, hot, stage, line, _) in enumerate(parts):
            @pl.when(on_line(p))
            def _(p=p, hot=hot, stage=stage, line=line):
                wait_for(stage, to_sem.at[0, p])

                @pl.loop(1, n * n)
                def _(j):
                    a, b = j // n, j % n
                    remote(stage_piece(p, stage, a, b), hot_piece(p, hot, c, line, a, b), from_sem.at[1, p], to_sem.at[1, p],
                           plane_device(p, a, b)).start()
                hot_piece(p, hot, c, line, 0, 0)[...] = stage_piece(p, stage, 0, 0)[...]

    def hot_plane():
        for p, (_, hot, _, line, plane) in enumerate(parts):
            mine = hot_piece(p, hot, c, line, plane[0], plane[1])

            @pl.when(jnp.logical_not(on_line(p)))
            def _(p=p, mine=mine):
                wait_for(mine, to_sem.at[1, p])

            @pl.loop(1, n * n)
            def _(j, p=p, mine=mine, plane=plane):
                remote(mine, mine, from_sem.at[2, p], to_sem.at[2, p], plane_device(p, plane[0] + j // n, plane[1] + j % n)).start()

    def hot_line():
        for p, (_, hot, _, line, _) in enumerate(parts):
            wait_for(pieces_like(p, hot), to_sem.at[2, p])
            mine = quarter(p, hot, c, line)
            for j in range(1, n):
                remote(mine, mine, from_sem.at[3, p], to_sem.at[3, p], line_device(p, line + j, c)).start()

    def line_like(p, ref):
        if p < 2:
            return ref.at[pl.ds(0, (n - 1) * n * n * unit)]
        return ref.at[pl.ds(0, (n - 1) * n * unit_d), pl.ds(0, d_model // 2)]

    def half_of(p, ref, half):
        if p < 2:
            return rows_at(ref, half * (d_model // 2), d_model // 2, 16)
        return ref.at[:, pl.ds(pl.multiple_of(half * (d_model // 2), 128), d_model // 2)]

    def hot_core():
        for p, (_, hot, _, _, _) in enumerate(parts):
            wait_for(line_like(p, hot), to_sem.at[3, p])
            mine = half_of(p, hot, c)
            remote(mine, mine, from_sem.at[4, p], to_sem.at[4, p], device(mz, my, mx, c + 1)).start()

    def hot_finish():
        for p, (_, hot, _, _, _) in enumerate(parts):
            wait_for(half_of(p, hot, 1 - c), to_sem.at[4, p])
        gate = dotf(x_ref[...], hot_g[...])
        up = dotf(x_ref[...], hot_u[...])
        u = (jax.nn.silu(gate) * up).astype(BF16)
        count = hot_tok_ref.shape[1]
        same = iota((tokens, count), 0) == hot_tok_ref[...]
        weight = jnp.sum(jnp.where(same, hot_gate_ref[...], 0.0), axis=1, keepdims=True)
        is_hot = jnp.sum(jnp.where(same, 1.0, 0.0), axis=1, keepdims=True) > 0.5
        for f in range(FOLD):
            cols = slice(f * piece, (f + 1) * piece)
            h = dotf(u, hot_d[:, cols]).astype(BF16)
            acc_ref[:, cols] = jnp.where(is_hot, weight * h.astype(F32), 0.0)

    def hot_sends_done():
        for p, (src, hot, _, line, _) in enumerate(parts):
            @pl.when(me == 0)
            def _(p=p, src=src):
                if p < 2:
                    wait_for(src.at[pl.ds(0, (2 * n - 1) * n * n * unit)], from_sem.at[0, p])
                else:
                    wait_for(src.at[pl.ds(0, (2 * n - 1) * n * unit_d // 2)], from_sem.at[0, p])

            @pl.when(on_line(p))
            def _(p=p, hot=hot):
                wait_for(pieces_like(p, hot), from_sem.at[1, p])
            wait_for(pieces_like(p, hot), from_sem.at[2, p])
            wait_for(line_like(p, hot), from_sem.at[3, p])
            wait_for(half_of(p, hot, c), from_sem.at[4, p])

    def expert_of(q, i):
        return peer(q, i, 1)

    def fold(pieces):
        r = iota((main, main), 0)
        return dotf(ones_where(iota((main, main), 1) == r % FOLD * blocks + r // FOLD), pieces).astype(BF16)

    def unfold(folded):
        r = iota((main, main), 0)
        return dotf(ones_where(iota((main, main), 1) == r % blocks * FOLD + r // blocks), folded).astype(BF16)

    def pick_rows(q, count, slots):
        row = iota((count, tokens), 0)
        expert = expert_of(q, row // slots)
        member = ids_t_ref[0:1, :] == expert
        for j in range(1, top_k):
            member = jnp.logical_or(member, ids_t_ref[j:j + 1, :] == expert)
        earlier = ones_where(iota((tokens, tokens), 0) < iota((tokens, tokens), 1))
        member_f = jnp.where(member, 1.0, 0.0)
        rank = dotf(member_f.astype(BF16), earlier)
        slot = (row % slots).astype(F32) if slots > 1 else float(SLOTS)
        return jnp.where(rank == slot, member_f, 0.0).astype(BF16)

    def fill(q):
        pick = pick_rows(q, main, SLOTS)
        ninth = pick_rows(q, blocks, 1)
        for f in range(FOLD):
            cols = slice(f * piece, (f + 1) * piece)
            send[q, :, :, cols] = dotf(pick, x_ref[:, cols]).astype(BF16).reshape(blocks, SLOTS, piece)
            fold_ref[f * blocks:(f + 1) * blocks] = dotf(ninth, x_ref[:, cols]).astype(BF16)
        send[q, :, :, d_model:] = fold(fold_ref[...]).reshape(blocks, FOLD, piece)

    def start_sends(q, src, dst, s_sem, r_sem, sign):
        @pl.loop(0, blocks)
        def _(i):
            @pl.when(jnp.logical_or(q > 0, i > 0))
            def _():
                remote(src.at[q, i], dst.at[q, i], s_sem.at[q], r_sem.at[q], peer(q, i, sign)).start()

    def wait_chunk(q, buf, sem):
        @pl.when(q == 0)
        def _():
            wait_for(buf.at[0, pl.ds(1, blocks - 1)], sem.at[0])

        @pl.when(q > 0)
        def _():
            wait_for(buf.at[q], sem.at[q])

    def load_rows(q, buf):
        rows_ref[:main] = buf[q, :, :, :d_model].reshape(main, d_model)
        pieces = unfold(buf[q, :, :, d_model:].reshape(main, piece))
        for f in range(FOLD):
            rows_ref[main:, f * piece:(f + 1) * piece] = pieces[f * blocks:(f + 1) * blocks]

    @pl.loop(0, n)
    def _(q):
        fill(q)

    recv[0, 0] = send[0, 0]
    pl.semaphore_wait(barrier, devices - 1)
    hot_root()

    @pl.loop(0, n)
    def _(q):
        start_sends(q, send, recv, send_sem, recv_sem, 1)

    for copy in own:
        copy.wait()

    width = 256 if d_ff % 256 == 0 else d_ff

    @pl.loop(0, n)
    def _(q):
        wait_chunk(q, recv, recv_sem)
        load_rows(q, recv)
        for w in range(d_ff // width):
            cols = slice(w * width, (w + 1) * width)
            gate = dotf(rows_ref[...], wg[:, cols])
            up = dotf(rows_ref[...], wu[:, cols])
            u_ref[:, cols] = (jax.nn.silu(gate) * up).astype(BF16)
        for f in range(FOLD):
            cols = slice(f * piece, (f + 1) * piece)
            res = dotf(u_ref[...], wd[:, cols]).astype(BF16)
            out[q, :, :, cols] = res[:main].reshape(blocks, SLOTS, piece)
            fold_ref[f * blocks:(f + 1) * blocks] = res[main:]
        out[q, :, :, d_model:] = fold(fold_ref[...]).reshape(blocks, FOLD, piece)
        start_sends(q, out, back, ret_sem, back_sem, -1)

        @pl.when(q == 0)
        def _():
            back[0, 0] = out[0, 0]
            hot_scatter()

        @pl.when(q == 1)
        def _():
            hot_plane()

    hot_line()

    @pl.loop(0, n)
    def _(q):
        def weights(count, slots):
            col = iota((tokens, count), 1)
            expert = expert_of(q, col // slots)
            member = ids_ref[:, 0:1] == expert
            weight = jnp.where(member, gates_ref[:, 0:1], 0.0)
            for j in range(1, top_k):
                here = ids_ref[:, j:j + 1] == expert
                member = jnp.logical_or(member, here)
                weight = jnp.where(here, gates_ref[:, j:j + 1], weight)
            earlier = ones_where(iota((tokens, tokens), 1) < iota((tokens, tokens), 0))
            rank = dotf(earlier, ones_where(member))
            slot = (col % slots).astype(F32) if slots > 1 else float(SLOTS)
            return three_terms(jnp.where(rank == slot, weight, 0.0))
        weight_ref[q, :, :main] = weights(main, SLOTS)
        weight_ref[q, :, main:] = weights(blocks, 1)

    hot_core()
    hot_finish()

    @pl.loop(0, n)
    def _(q):
        wait_chunk(q, back, back_sem)
        load_rows(q, back)
        for f in range(FOLD):
            cols = slice(f * piece, (f + 1) * piece)
            terms = dotf(weight_ref[q], rows_ref[:, cols])
            acc_ref[:, cols] += terms[2 * tokens:] + terms[tokens:2 * tokens] + terms[:tokens]

    y_ref[...] = acc_ref[...].astype(BF16)

    @pl.loop(0, n)
    def _(q):
        wait_chunk(q, send, send_sem)
        wait_chunk(q, out, ret_sem)
    hot_sends_done()


def solution(mesh):
    group_size = mesh.shape['ep']
    n = 1
    while 2 * n * n * n < group_size:
        n += 1
    row_spec = P(('dp', 'ep'), None)
    list_spec = P(('dp', 'ep'))
    expert_spec = P('ep', None, None)

    def local_layer(x, ids, gates, hot_tok, hot_gates, wg, wu, wd):
        wg, wu, wd = wg[0], wu[0], wd[0]
        tokens, d_model = x.shape
        d_ff = wg.shape[1]
        blocks = 2 * n * n
        piece = d_model // FOLD
        main = blocks * SLOTS
        block_buf = pltpu.VMEM((n, blocks, SLOTS, d_model + piece), BF16)
        in_vmem = pl.BlockSpec(memory_space=pltpu.VMEM)
        in_hbm = pl.BlockSpec(memory_space=pl.ANY)
        dma = pltpu.SemaphoreType.DMA
        weights = [pltpu.VMEM((d_model, d_ff), BF16)] * 2 + [pltpu.VMEM((d_ff, d_model), BF16)]
        return pl.pallas_call(
            functools.partial(layer_kernel, n),
            out_shape=jax.ShapeDtypeStruct((tokens, d_model), BF16),
            in_specs=[in_vmem] * 6 + [in_hbm] * 3,
            out_specs=in_vmem,
            scratch_shapes=[block_buf] * 4 + weights + weights
            + [pltpu.VMEM((d_model // (2 * n), d_ff), BF16)] * 2 + [pltpu.VMEM((d_ff // n, d_model // 2), BF16)]
            + [pltpu.VMEM((main + blocks, d_model), BF16), pltpu.VMEM((main + blocks, d_ff), BF16),
               pltpu.VMEM((main, piece), BF16), pltpu.VMEM((n, 3 * tokens, main + blocks), BF16), pltpu.VMEM((tokens, d_model), F32)]
            + [dma((3,)), dma((n,)), dma((n,)), dma((n,)), dma((n,)), dma((5, 3)), dma((5, 3))],
            compiler_params=pltpu.CompilerParams(vmem_limit_bytes=VMEM_LIMIT, collective_id=0, has_side_effects=True),
            name="moe_layer",
        )(ids.T, ids, gates, hot_tok[None, :], hot_gates[None, :], x, wg, wu, wd)

    return jax.shard_map(local_layer, mesh=mesh,
                         in_specs=(row_spec, row_spec, row_spec, list_spec, list_spec, expert_spec, expert_spec, expert_spec),
                         out_specs=row_spec, check_vma=False)
```

```python
import functools

import jax
import jax.numpy as jnp
from jax import lax
from jax.experimental import pallas as pl
from jax.experimental.pallas import tpu as pltpu
from jax.sharding import PartitionSpec as P

F32 = jnp.float32
BF16 = jnp.bfloat16
SLOTS = 8
FOLD = 8
VMEM_LIMIT = 60 * 1024 * 1024


def dotf(a, b):
    return jnp.dot(a, b, preferred_element_type=F32)


def iota(shape, dim):
    return lax.broadcasted_iota(jnp.int32, shape, dim)


def ones_where(mask):
    return jnp.where(mask, 1.0, 0.0).astype(BF16)


def three_terms(a):
    hi = a.astype(BF16)
    rest = a - hi.astype(F32)
    mid = rest.astype(BF16)
    low = (rest - mid.astype(F32)).astype(BF16)
    return jnp.concatenate([hi, mid, low], axis=0)


def layer_kernel(n, ids_ref, gates_ref, hot_tok_ref, hot_gate_ref, x_ref, wg_ref, wu_ref, wd_ref, y_ref,
                 send, recv, out, back, wg, wu, wd, hot_g, hot_u, hot_d, stage_g, stage_u, stage_d,
                 rows_ref, u_ref, fold_ref, weight_ref, acc_ref,
                 load_sem, send_sem, recv_sem, ret_sem, back_sem, from_sem, to_sem):
    me = lax.axis_index('ep')
    devices = 2 * n * n * n
    c, mx, my, mz = me % 2, (me // 2) % n, (me // (2 * n)) % n, me // (2 * n * n)
    blocks = 2 * n * n
    tokens, d_model = x_ref.shape
    d_ff = wd_ref.shape[0]
    top_k = ids_ref.shape[0]
    piece = d_model // FOLD
    main = blocks * SLOTS
    chunk_rows = main + blocks

    def device(z, y, x, core):
        return ((z % n * n + y % n) * n + x % n) * 2 + core % 2

    def peer(q, i, sign):
        kc, kx, ky = i % 2, (i // 2) % n, i // (2 * n)
        kz = (q + 2 * n - kx - ky) % n
        if sign > 0:
            return device(mz + kz, my + ky, mx + kx, c + kc)
        return device(mz + n - kz, my + n - ky, mx + n - kx, c + kc)

    def remote(src, dst, s_sem, r_sem, to):
        return pltpu.make_async_remote_copy(src_ref=src, dst_ref=dst, send_sem=s_sem, recv_sem=r_sem, device_id={'ep': to},
                                            device_id_type=pl.DeviceIdType.MESH)

    def wait_for(ref, sem):
        pltpu.make_async_copy(ref, ref, sem).wait()

    def rows_at(ref, start, size, unit):
        return ref.at[pl.ds(pl.multiple_of(start, unit), size)]

    barrier = pltpu.get_barrier_semaphore()

    @pl.loop(1, devices)
    def _(i):
        pl.semaphore_signal(barrier, inc=1, device_id={'ep': (me + i) % devices}, device_id_type=pl.DeviceIdType.MESH)

    own = [pltpu.make_async_copy(src, dst, load_sem.at[p])
           for p, (src, dst) in enumerate(((wg_ref, wg), (wu_ref, wu), (wd_ref, wd)))]
    for copy in own:
        copy.start()

    unit = d_model // (2 * n * n * n)
    unit_d, unit_c = d_ff // (n * n), d_model // (2 * n)
    parts = ((wg_ref, hot_g, stage_g, mz, (my, mx)), (wu_ref, hot_u, stage_u, mx, (mz, my)), (wd_ref, hot_d, stage_d, my, (mx, mz)))

    def line_device(p, k, core):
        return (device(k, my, mx, core), device(mz, my, k, core), device(mz, k, mx, core))[p]

    def plane_device(p, a, b):
        return (device(mz, a, b, c), device(a, b, mx, c), device(b, my, a, c))[p]

    def quarter(p, ref, half, k):
        if p < 2:
            size = n * n * unit
            return rows_at(ref, half * (d_model // 2) + k * size, size, 16)
        size = n * unit_d
        return ref.at[pl.ds(pl.multiple_of(k * size, 16), size), pl.ds(pl.multiple_of(half * (d_model // 2), 128), d_model // 2)]

    def hot_piece(p, ref, half, k, a, b):
        if p < 2:
            return rows_at(ref, half * (d_model // 2) + k * (n * n * unit) + (a * n + b) * unit, unit, 16)
        return ref.at[pl.ds(pl.multiple_of(k * (n * unit_d) + a * unit_d, 16), unit_d),
                      pl.ds(pl.multiple_of(half * (d_model // 2) + b * unit_c, 128), unit_c)]

    def stage_piece(p, ref, a, b):
        if p < 2:
            return rows_at(ref, (a * n + b) * unit, unit, 16)
        return ref.at[pl.ds(pl.multiple_of(a * unit_d, 16), unit_d), pl.ds(pl.multiple_of(b * unit_c, 128), unit_c)]

    def pieces_like(p, ref):
        if p < 2:
            return ref.at[pl.ds(0, (n * n - 1) * unit)]
        return ref.at[pl.ds(0, (n * n - 1) * unit_d), pl.ds(0, unit_c)]

    def on_line(p):
        plane = parts[p][4]
        return jnp.logical_and(plane[0] == 0, plane[1] == 0)

    def hot_root():
        @pl.when(me == 0)
        def _():
            for p, (src, _, stage, _, _) in enumerate(parts):
                for k in range(n):
                    for half in range(2):
                        if k == 0 and half == 0:
                            pltpu.make_async_copy(quarter(p, src, 0, 0), stage, to_sem.at[0, p]).start()
                        else:
                            remote(quarter(p, src, half, k), stage, from_sem.at[0, p], to_sem.at[0, p], line_device(p, k, half)).start()

    def hot_scatter():
        for p, (_, hot, stage, line, _) in enumerate(parts):
            @pl.when(on_line(p))
            def _(p=p, hot=hot, stage=stage, line=line):
                wait_for(stage, to_sem.at[0, p])

                @pl.loop(1, n * n)
                def _(j):
                    a, b = j // n, j % n
                    remote(stage_piece(p, stage, a, b), hot_piece(p, hot, c, line, a, b), from_sem.at[1, p], to_sem.at[1, p],
                           plane_device(p, a, b)).start()
                hot_piece(p, hot, c, line, 0, 0)[...] = stage_piece(p, stage, 0, 0)[...]

    def hot_plane():
        for p, (_, hot, _, line, plane) in enumerate(parts):
            mine = hot_piece(p, hot, c, line, plane[0], plane[1])

            @pl.when(jnp.logical_not(on_line(p)))
            def _(p=p, mine=mine):
                wait_for(mine, to_sem.at[1, p])

            @pl.loop(1, n * n)
            def _(j, p=p, mine=mine, plane=plane):
                remote(mine, mine, from_sem.at[2, p], to_sem.at[2, p], plane_device(p, plane[0] + j // n, plane[1] + j % n)).start()

    def hot_line():
        for p, (_, hot, _, line, _) in enumerate(parts):
            wait_for(pieces_like(p, hot), to_sem.at[2, p])
            mine = quarter(p, hot, c, line)
            for j in range(1, n):
                remote(mine, mine, from_sem.at[3, p], to_sem.at[3, p], line_device(p, line + j, c)).start()

    def line_like(p, ref):
        if p < 2:
            return ref.at[pl.ds(0, (n - 1) * n * n * unit)]
        return ref.at[pl.ds(0, (n - 1) * n * unit_d), pl.ds(0, d_model // 2)]

    def half_of(p, ref, half):
        if p < 2:
            return rows_at(ref, half * (d_model // 2), d_model // 2, 16)
        return ref.at[:, pl.ds(pl.multiple_of(half * (d_model // 2), 128), d_model // 2)]

    def hot_core():
        for p, (_, hot, _, _, _) in enumerate(parts):
            wait_for(line_like(p, hot), to_sem.at[3, p])
            mine = half_of(p, hot, c)
            remote(mine, mine, from_sem.at[4, p], to_sem.at[4, p], device(mz, my, mx, c + 1)).start()

    def hot_finish():
        for p, (_, hot, _, _, _) in enumerate(parts):
            wait_for(half_of(p, hot, 1 - c), to_sem.at[4, p])
        gate = dotf(x_ref[...], hot_g[...])
        up = dotf(x_ref[...], hot_u[...])
        u = (jax.nn.silu(gate) * up).astype(BF16)
        count = hot_tok_ref.shape[1]
        same = iota((tokens, count), 0) == hot_tok_ref[...]
        weight = jnp.sum(jnp.where(same, hot_gate_ref[...], 0.0), axis=1, keepdims=True)
        is_hot = jnp.sum(jnp.where(same, 1.0, 0.0), axis=1, keepdims=True) > 0.5
        for f in range(FOLD):
            cols = slice(f * piece, (f + 1) * piece)
            h = dotf(u, hot_d[:, cols]).astype(BF16)
            acc_ref[:, cols] = jnp.where(is_hot, weight * h.astype(F32), 0.0)

    def hot_sends_done():
        for p, (src, hot, _, line, _) in enumerate(parts):
            @pl.when(me == 0)
            def _(p=p, src=src):
                if p < 2:
                    wait_for(src.at[pl.ds(0, (2 * n - 1) * n * n * unit)], from_sem.at[0, p])
                else:
                    wait_for(src.at[pl.ds(0, (2 * n - 1) * n * unit_d // 2)], from_sem.at[0, p])

            @pl.when(on_line(p))
            def _(p=p, hot=hot):
                wait_for(pieces_like(p, hot), from_sem.at[1, p])
            wait_for(pieces_like(p, hot), from_sem.at[2, p])
            wait_for(line_like(p, hot), from_sem.at[3, p])
            wait_for(half_of(p, hot, c), from_sem.at[4, p])

    def expert_of(q, i):
        return peer(q, i, 1)

    def fold(pieces):
        r = iota((main, main), 0)
        return dotf(ones_where(iota((main, main), 1) == r % FOLD * blocks + r // FOLD), pieces).astype(BF16)

    def unfold(folded):
        r = iota((main, main), 0)
        return dotf(ones_where(iota((main, main), 1) == r % blocks * FOLD + r // blocks), folded).astype(BF16)

    def pick_rows(q, count, slots):
        row = iota((count, tokens), 0)
        expert = expert_of(q, row // slots)
        member = ids_ref[0:1, :] == expert
        for j in range(1, top_k):
            member = jnp.logical_or(member, ids_ref[j:j + 1, :] == expert)
        earlier = ones_where(iota((tokens, tokens), 0) < iota((tokens, tokens), 1))
        member_f = jnp.where(member, 1.0, 0.0)
        rank = dotf(member_f.astype(BF16), earlier)
        slot = (row % slots).astype(F32) if slots > 1 else float(SLOTS)
        return jnp.where(rank == slot, member_f, 0.0).astype(BF16)

    def fill(q):
        pick = pick_rows(q, main, SLOTS)
        ninth = pick_rows(q, blocks, 1)
        for f in range(FOLD):
            cols = slice(f * piece, (f + 1) * piece)
            send[q, :, :, cols] = dotf(pick, x_ref[:, cols]).astype(BF16).reshape(blocks, SLOTS, piece)
            fold_ref[f * blocks:(f + 1) * blocks] = dotf(ninth, x_ref[:, cols]).astype(BF16)
        send[q, :, :, d_model:] = fold(fold_ref[...]).reshape(blocks, FOLD, piece)

    def start_sends(q, src, dst, s_sem, r_sem, sign):
        @pl.loop(0, blocks)
        def _(i):
            @pl.when(jnp.logical_or(q > 0, i > 0))
            def _():
                remote(src.at[q, i], dst.at[q, i], s_sem.at[q], r_sem.at[q], peer(q, i, sign)).start()

    def wait_chunk(q, buf, sem):
        @pl.when(q == 0)
        def _():
            wait_for(buf.at[0, pl.ds(1, blocks - 1)], sem.at[0])

        @pl.when(q > 0)
        def _():
            wait_for(buf.at[q], sem.at[q])

    def load_rows(q, buf):
        rows_ref[:main] = buf[q, :, :, :d_model].reshape(main, d_model)
        pieces = unfold(buf[q, :, :, d_model:].reshape(main, piece))
        for f in range(FOLD):
            rows_ref[main:, f * piece:(f + 1) * piece] = pieces[f * blocks:(f + 1) * blocks]

    def send_chunk(q):
        start_sends(q, send, recv, send_sem, recv_sem, 1)

    width = 256 if d_ff % 256 == 0 else d_ff

    def expert(q):
        with jax.named_scope("wrecv"):
            wait_chunk(q, recv, recv_sem)
        load_rows(q, recv)
        for w in range(d_ff // width):
            cols = slice(w * width, (w + 1) * width)
            gate = dotf(rows_ref[...], wg[:, cols])
            up = dotf(rows_ref[...], wu[:, cols])
            u_ref[:, cols] = (jax.nn.silu(gate) * up).astype(BF16)
        for f in range(FOLD):
            cols = slice(f * piece, (f + 1) * piece)
            res = dotf(u_ref[...], wd[:, cols]).astype(BF16)
            out[q, :, :, cols] = res[:main].reshape(blocks, SLOTS, piece)
            fold_ref[f * blocks:(f + 1) * blocks] = res[main:]
        out[q, :, :, d_model:] = fold(fold_ref[...]).reshape(blocks, FOLD, piece)

    def return_chunk(q):
        start_sends(q, out, back, ret_sem, back_sem, -1)

    def fill_weights(q):
        def weights(count, slots):
            row = iota((count, tokens), 0)
            expert = expert_of(q, row // slots)
            member = ids_ref[0:1, :] == expert
            weight = jnp.where(member, gates_ref[0:1, :], 0.0)
            for j in range(1, top_k):
                here = ids_ref[j:j + 1, :] == expert
                member = jnp.logical_or(member, here)
                weight = jnp.where(here, gates_ref[j:j + 1, :], weight)
            earlier = ones_where(iota((tokens, tokens), 0) < iota((tokens, tokens), 1))
            rank = dotf(ones_where(member), earlier)
            slot = (row % slots).astype(F32) if slots > 1 else float(SLOTS)
            return jnp.where(rank == slot, weight, 0.0)
        weight_ref[q, :, :main] = three_terms(weights(main, SLOTS).T)
        weight_ref[q, :, main:] = three_terms(weights(blocks, 1).T)

    def combine(q):
        with jax.named_scope("wback"):
            wait_chunk(q, back, back_sem)
        load_rows(q, back)
        for f in range(FOLD):
            cols = slice(f * piece, (f + 1) * piece)
            terms = dotf(weight_ref[q], rows_ref[:, cols])
            acc_ref[:, cols] += terms[2 * tokens:] + terms[tokens:2 * tokens] + terms[:tokens]

    def fill_step(q):
        with jax.named_scope("fill"):
            fill(q)

        @pl.when(q == 0)
        def _():
            with jax.named_scope("barrier"):
                pl.semaphore_wait(barrier, devices - 1)
            with jax.named_scope("hroot"):
                hot_root()
            send_chunk(0)

    pl.loop(0, n)(fill_step)
    recv[0, 0] = send[0, 0]
    with jax.named_scope("hscatter"):
        hot_scatter()
    send_chunk(1)
    with jax.named_scope("hplane"):
        hot_plane()
    for copy in own:
        copy.wait()

    with jax.named_scope("send23"):
        pl.loop(2, n)(send_chunk)
    with jax.named_scope("fweights"):
        pl.loop(0, n)(fill_weights)

    @pl.loop(0, n)
    def _(q):
        expert(q)

        @pl.when(q == 0)
        def _():
            back[0, 0] = out[0, 0]
            with jax.named_scope("hline"):
                hot_line()

        return_chunk(q)

        @pl.when(q == n - 1)
        def _():
            with jax.named_scope("hcore"):
                hot_core()

    with jax.named_scope("hfinish"):
        hot_finish()
    pl.loop(0, n)(combine)
    y_ref[...] = acc_ref[...].astype(BF16)

    @pl.loop(0, n)
    def _(q):
        wait_chunk(q, send, send_sem)
        wait_chunk(q, out, ret_sem)
    with jax.named_scope("hsend"):
        hot_sends_done()


def solution(mesh):
    group_size = mesh.shape['ep']
    n = 1
    while 2 * n * n * n < group_size:
        n += 1
    row_spec = P(('dp', 'ep'), None)
    list_spec = P(('dp', 'ep'))
    expert_spec = P('ep', None, None)

    def local_layer(x, ids, gates, hot_tok, hot_gates, wg, wu, wd):
        wg, wu, wd = wg[0], wu[0], wd[0]
        tokens, d_model = x.shape
        d_ff = wg.shape[1]
        blocks = 2 * n * n
        piece = d_model // FOLD
        main = blocks * SLOTS
        block_buf = pltpu.VMEM((n, blocks, SLOTS, d_model + piece), BF16)
        in_vmem = pl.BlockSpec(memory_space=pltpu.VMEM)
        in_hbm = pl.BlockSpec(memory_space=pl.ANY)
        dma = pltpu.SemaphoreType.DMA
        weights = [pltpu.VMEM((d_model, d_ff), BF16)] * 2 + [pltpu.VMEM((d_ff, d_model), BF16)]
        return pl.pallas_call(
            functools.partial(layer_kernel, n),
            out_shape=jax.ShapeDtypeStruct((tokens, d_model), BF16),
            in_specs=[in_vmem] * 5 + [in_hbm] * 3,
            out_specs=in_vmem,
            scratch_shapes=[block_buf] * 4 + weights + weights
            + [pltpu.VMEM((d_model // (2 * n), d_ff), BF16)] * 2 + [pltpu.VMEM((d_ff // n, d_model // 2), BF16)]
            + [pltpu.VMEM((main + blocks, d_model), BF16), pltpu.VMEM((main + blocks, d_ff), BF16),
               pltpu.VMEM((main, piece), BF16), pltpu.VMEM((n, 3 * tokens, main + blocks), BF16), pltpu.VMEM((tokens, d_model), F32)]
            + [dma((3,)), dma((n,)), dma((n,)), dma((n,)), dma((n,)), dma((5, 3)), dma((5, 3))],
            compiler_params=pltpu.CompilerParams(vmem_limit_bytes=VMEM_LIMIT, collective_id=0, has_side_effects=True),
            name="moe_layer",
        )(ids.T, gates.T, hot_tok[None, :], hot_gates[None, :], x, wg, wu, wd)

    return jax.shard_map(local_layer, mesh=mesh,
                         in_specs=(row_spec, row_spec, row_spec, list_spec, list_spec, expert_spec, expert_spec, expert_spec),
                         out_specs=row_spec, check_vma=False)
```

```python
import functools

import jax
import jax.numpy as jnp
from jax import lax
from jax.experimental import pallas as pl
from jax.experimental.pallas import tpu as pltpu
from jax.sharding import PartitionSpec as P

F32 = jnp.float32
BF16 = jnp.bfloat16
SLOTS = 8
FOLD = 8
VMEM_LIMIT = 60 * 1024 * 1024


def dotf(a, b):
    return jnp.dot(a, b, preferred_element_type=F32)


def iota(shape, dim):
    return lax.broadcasted_iota(jnp.int32, shape, dim)


def ones_where(mask):
    return jnp.where(mask, 1.0, 0.0).astype(BF16)


def three_terms(a):
    hi = a.astype(BF16)
    rest = a - hi.astype(F32)
    mid = rest.astype(BF16)
    low = (rest - mid.astype(F32)).astype(BF16)
    return jnp.concatenate([hi, mid, low], axis=0)


def layer_kernel(n, ids_ref, gates_ref, hot_tok_ref, hot_gate_ref, x_ref, wg_ref, wu_ref, wd_ref, y_ref,
                 send, recv, out, back, wg, wu, wd, hot_g, hot_u, hot_d, stage_g, stage_u, stage_d,
                 rows_ref, u_ref, fold_ref, weight_ref, acc_ref,
                 load_sem, send_sem, recv_sem, ret_sem, back_sem, from_sem, to_sem):
    me = lax.axis_index('ep')
    devices = 2 * n * n * n
    c, mx, my, mz = me % 2, (me // 2) % n, (me // (2 * n)) % n, me // (2 * n * n)
    blocks = 2 * n * n
    tokens, d_model = x_ref.shape
    d_ff = wd_ref.shape[0]
    top_k = ids_ref.shape[0]
    piece = d_model // FOLD
    main = blocks * SLOTS
    chunk_rows = main + blocks

    def device(z, y, x, core):
        return ((z % n * n + y % n) * n + x % n) * 2 + core % 2

    def peer(q, i, sign):
        kc, kx, ky = i % 2, (i // 2) % n, i // (2 * n)
        kz = (q + 2 * n - kx - ky) % n
        if sign > 0:
            return device(mz + kz, my + ky, mx + kx, c + kc)
        return device(mz + n - kz, my + n - ky, mx + n - kx, c + kc)

    def remote(src, dst, s_sem, r_sem, to):
        return pltpu.make_async_remote_copy(src_ref=src, dst_ref=dst, send_sem=s_sem, recv_sem=r_sem, device_id={'ep': to},
                                            device_id_type=pl.DeviceIdType.MESH)

    def wait_for(ref, sem):
        pltpu.make_async_copy(ref, ref, sem).wait()

    def rows_at(ref, start, size, unit):
        return ref.at[pl.ds(pl.multiple_of(start, unit), size)]

    barrier = pltpu.get_barrier_semaphore()

    @pl.loop(1, devices)
    def _(i):
        pl.semaphore_signal(barrier, inc=1, device_id={'ep': (me + i) % devices}, device_id_type=pl.DeviceIdType.MESH)

    own = [pltpu.make_async_copy(src, dst, load_sem.at[p])
           for p, (src, dst) in enumerate(((wg_ref, wg), (wu_ref, wu), (wd_ref, wd)))]
    for copy in own:
        copy.start()

    unit = d_model // (2 * n * n * n)
    unit_d, unit_c = d_ff // (n * n), d_model // (2 * n)
    parts = ((wg_ref, hot_g, stage_g, mz, (my, mx)), (wu_ref, hot_u, stage_u, mx, (mz, my)), (wd_ref, hot_d, stage_d, my, (mx, mz)))

    def line_device(p, k, core):
        return (device(k, my, mx, core), device(mz, my, k, core), device(mz, k, mx, core))[p]

    def plane_device(p, a, b):
        return (device(mz, a, b, c), device(a, b, mx, c), device(b, my, a, c))[p]

    def quarter(p, ref, half, k):
        if p < 2:
            size = n * n * unit
            return rows_at(ref, half * (d_model // 2) + k * size, size, 16)
        size = n * unit_d
        return ref.at[pl.ds(pl.multiple_of(k * size, 16), size), pl.ds(pl.multiple_of(half * (d_model // 2), 128), d_model // 2)]

    def hot_piece(p, ref, half, k, a, b):
        if p < 2:
            return rows_at(ref, half * (d_model // 2) + k * (n * n * unit) + (a * n + b) * unit, unit, 16)
        return ref.at[pl.ds(pl.multiple_of(k * (n * unit_d) + a * unit_d, 16), unit_d),
                      pl.ds(pl.multiple_of(half * (d_model // 2) + b * unit_c, 128), unit_c)]

    def stage_piece(p, ref, a, b):
        if p < 2:
            return rows_at(ref, (a * n + b) * unit, unit, 16)
        return ref.at[pl.ds(pl.multiple_of(a * unit_d, 16), unit_d), pl.ds(pl.multiple_of(b * unit_c, 128), unit_c)]

    def pieces_like(p, ref):
        if p < 2:
            return ref.at[pl.ds(0, (n * n - 1) * unit)]
        return ref.at[pl.ds(0, (n * n - 1) * unit_d), pl.ds(0, unit_c)]

    def on_line(p):
        plane = parts[p][4]
        return jnp.logical_and(plane[0] == 0, plane[1] == 0)

    def hot_root():
        @pl.when(me == 0)
        def _():
            for p, (src, _, stage, _, _) in enumerate(parts):
                for k in range(n):
                    for half in range(2):
                        if k == 0 and half == 0:
                            pltpu.make_async_copy(quarter(p, src, 0, 0), stage, to_sem.at[0, p]).start()
                        else:
                            remote(quarter(p, src, half, k), stage, from_sem.at[0, p], to_sem.at[0, p], line_device(p, k, half)).start()

    def hot_scatter():
        for p, (_, hot, stage, line, _) in enumerate(parts):
            @pl.when(on_line(p))
            def _(p=p, hot=hot, stage=stage, line=line):
                wait_for(stage, to_sem.at[0, p])

                @pl.loop(1, n * n)
                def _(j):
                    a, b = j // n, j % n
                    remote(stage_piece(p, stage, a, b), hot_piece(p, hot, c, line, a, b), from_sem.at[1, p], to_sem.at[1, p],
                           plane_device(p, a, b)).start()
                hot_piece(p, hot, c, line, 0, 0)[...] = stage_piece(p, stage, 0, 0)[...]

    def hot_plane():
        for p, (_, hot, _, line, plane) in enumerate(parts):
            mine = hot_piece(p, hot, c, line, plane[0], plane[1])

            @pl.when(jnp.logical_not(on_line(p)))
            def _(p=p, mine=mine):
                wait_for(mine, to_sem.at[1, p])

            @pl.loop(1, n * n)
            def _(j, p=p, mine=mine, plane=plane):
                remote(mine, mine, from_sem.at[2, p], to_sem.at[2, p], plane_device(p, plane[0] + j // n, plane[1] + j % n)).start()

    def hot_line():
        for p, (_, hot, _, line, _) in enumerate(parts):
            wait_for(pieces_like(p, hot), to_sem.at[2, p])
            mine = quarter(p, hot, c, line)
            for j in range(1, n):
                remote(mine, mine, from_sem.at[3, p], to_sem.at[3, p], line_device(p, line + j, c)).start()

    def line_like(p, ref):
        if p < 2:
            return ref.at[pl.ds(0, (n - 1) * n * n * unit)]
        return ref.at[pl.ds(0, (n - 1) * n * unit_d), pl.ds(0, d_model // 2)]

    def half_of(p, ref, half):
        if p < 2:
            return rows_at(ref, half * (d_model // 2), d_model // 2, 16)
        return ref.at[:, pl.ds(pl.multiple_of(half * (d_model // 2), 128), d_model // 2)]

    def hot_core():
        for p, (_, hot, _, _, _) in enumerate(parts):
            wait_for(line_like(p, hot), to_sem.at[3, p])
            mine = half_of(p, hot, c)
            remote(mine, mine, from_sem.at[4, p], to_sem.at[4, p], device(mz, my, mx, c + 1)).start()

    def hot_finish():
        for p, (_, hot, _, _, _) in enumerate(parts):
            wait_for(half_of(p, hot, 1 - c), to_sem.at[4, p])
        gate = dotf(x_ref[...], hot_g[...])
        up = dotf(x_ref[...], hot_u[...])
        u = (jax.nn.silu(gate) * up).astype(BF16)
        count = hot_tok_ref.shape[1]
        same = iota((tokens, count), 0) == hot_tok_ref[...]
        weight = jnp.sum(jnp.where(same, hot_gate_ref[...], 0.0), axis=1, keepdims=True)
        is_hot = jnp.sum(jnp.where(same, 1.0, 0.0), axis=1, keepdims=True) > 0.5
        for f in range(FOLD):
            cols = slice(f * piece, (f + 1) * piece)
            h = dotf(u, hot_d[:, cols]).astype(BF16)
            acc_ref[:, cols] += jnp.where(is_hot, weight * h.astype(F32), 0.0)

    def hot_sends_done():
        for p, (src, hot, _, line, _) in enumerate(parts):
            @pl.when(me == 0)
            def _(p=p, src=src):
                if p < 2:
                    wait_for(src.at[pl.ds(0, (2 * n - 1) * n * n * unit)], from_sem.at[0, p])
                else:
                    wait_for(src.at[pl.ds(0, (2 * n - 1) * n * unit_d // 2)], from_sem.at[0, p])

            @pl.when(on_line(p))
            def _(p=p, hot=hot):
                wait_for(pieces_like(p, hot), from_sem.at[1, p])
            wait_for(pieces_like(p, hot), from_sem.at[2, p])
            wait_for(line_like(p, hot), from_sem.at[3, p])
            wait_for(half_of(p, hot, c), from_sem.at[4, p])

    def expert_of(q, i):
        return peer(q, i, 1)

    def fold(pieces):
        r = iota((main, main), 0)
        return dotf(ones_where(iota((main, main), 1) == r % FOLD * blocks + r // FOLD), pieces).astype(BF16)

    def unfold(folded):
        r = iota((main, main), 0)
        return dotf(ones_where(iota((main, main), 1) == r % blocks * FOLD + r // blocks), folded).astype(BF16)

    def pick_rows(q, count, slots):
        row = iota((count, tokens), 0)
        expert = expert_of(q, row // slots)
        member = ids_ref[0:1, :] == expert
        for j in range(1, top_k):
            member = jnp.logical_or(member, ids_ref[j:j + 1, :] == expert)
        earlier = ones_where(iota((tokens, tokens), 0) < iota((tokens, tokens), 1))
        member_f = jnp.where(member, 1.0, 0.0)
        rank = dotf(member_f.astype(BF16), earlier)
        slot = (row % slots).astype(F32) if slots > 1 else float(SLOTS)
        return jnp.where(rank == slot, member_f, 0.0).astype(BF16)

    def fill(q):
        pick = pick_rows(q, main, SLOTS)
        ninth = pick_rows(q, blocks, 1)
        for f in range(FOLD):
            cols = slice(f * piece, (f + 1) * piece)
            send[q, :, :, cols] = dotf(pick, x_ref[:, cols]).astype(BF16).reshape(blocks, SLOTS, piece)
            fold_ref[f * blocks:(f + 1) * blocks] = dotf(ninth, x_ref[:, cols]).astype(BF16)
        send[q, :, :, d_model:] = fold(fold_ref[...]).reshape(blocks, FOLD, piece)

    def start_sends(q, src, dst, s_sem, r_sem, sign):
        @pl.loop(jnp.where(q == 0, 1, 0) if not isinstance(q, int) else int(q == 0), blocks)
        def _(i):
            remote(src.at[q, i], dst.at[q, i], s_sem.at[q], r_sem.at[q], peer(q, i, sign)).start()

    def wait_chunk(q, buf, sem):
        if isinstance(q, int):
            wait_for(buf.at[0, pl.ds(1, blocks - 1)] if q == 0 else buf.at[q], sem.at[q])
            return

        @pl.when(q == 0)
        def _():
            wait_for(buf.at[0, pl.ds(1, blocks - 1)], sem.at[0])

        @pl.when(q > 0)
        def _():
            wait_for(buf.at[q], sem.at[q])

    def load_rows(q, buf):
        rows_ref[:main] = buf[q, :, :, :d_model].reshape(main, d_model)
        pieces = unfold(buf[q, :, :, d_model:].reshape(main, piece))
        for f in range(FOLD):
            rows_ref[main:, f * piece:(f + 1) * piece] = pieces[f * blocks:(f + 1) * blocks]

    def send_chunk(q):
        start_sends(q, send, recv, send_sem, recv_sem, 1)

    width = 256 if d_ff % 256 == 0 else d_ff

    def expert(q):
        with jax.named_scope("wrecv"):
            wait_chunk(q, recv, recv_sem)
        load_rows(q, recv)
        for w in range(d_ff // width):
            cols = slice(w * width, (w + 1) * width)
            gate = dotf(rows_ref[...], wg[:, cols])
            up = dotf(rows_ref[...], wu[:, cols])
            u_ref[:, cols] = (jax.nn.silu(gate) * up).astype(BF16)
        for f in range(FOLD):
            cols = slice(f * piece, (f + 1) * piece)
            res = dotf(u_ref[...], wd[:, cols]).astype(BF16)
            out[q, :, :, cols] = res[:main].reshape(blocks, SLOTS, piece)
            fold_ref[f * blocks:(f + 1) * blocks] = res[main:]
        out[q, :, :, d_model:] = fold(fold_ref[...]).reshape(blocks, FOLD, piece)

    def return_chunk(q):
        start_sends(q, out, back, ret_sem, back_sem, -1)

    def fill_weights(q):
        def weights(count, slots):
            row = iota((count, tokens), 0)
            expert = expert_of(q, row // slots)
            member = ids_ref[0:1, :] == expert
            weight = jnp.where(member, gates_ref[0:1, :], 0.0)
            for j in range(1, top_k):
                here = ids_ref[j:j + 1, :] == expert
                member = jnp.logical_or(member, here)
                weight = jnp.where(here, gates_ref[j:j + 1, :], weight)
            earlier = ones_where(iota((tokens, tokens), 0) < iota((tokens, tokens), 1))
            rank = dotf(ones_where(member), earlier)
            slot = (row % slots).astype(F32) if slots > 1 else float(SLOTS)
            return jnp.where(rank == slot, weight, 0.0)
        weight_ref[q, :, :main] = three_terms(weights(main, SLOTS).T)
        weight_ref[q, :, main:] = three_terms(weights(blocks, 1).T)

    def add_returned(q):
        with jax.named_scope("wback"):
            wait_chunk(q, back, back_sem)
        load_rows(q, back)
        for f in range(FOLD):
            cols = slice(f * piece, (f + 1) * piece)
            terms = dotf(weight_ref[q], rows_ref[:, cols])
            acc_ref[:, cols] += terms[2 * tokens:] + terms[tokens:2 * tokens] + terms[:tokens]

    def fill_step(q):
        with jax.named_scope("fill"):
            fill(q)

        @pl.when(q == 0)
        def _():
            with jax.named_scope("barrier"):
                pl.semaphore_wait(barrier, devices - 1)
            hot_root()
            send_chunk(0)

    pl.loop(0, n)(fill_step)
    recv[0, 0] = send[0, 0]
    acc_ref[...] = jnp.zeros_like(acc_ref)
    with jax.named_scope("fweights"):
        pl.loop(0, n)(fill_weights)
    for copy in own:
        copy.wait()
    with jax.named_scope("wsend0"):
        wait_chunk(0, send, send_sem)
    send_chunk(1)

    @pl.loop(0, n)
    def _(q):
        expert(q)

        @pl.when(q == 0)
        def _():
            back[0, 0] = out[0, 0]

        return_chunk(q)

        @pl.when(q == 0)
        def _():
            with jax.named_scope("hscatter"):
                hot_scatter()

        @pl.when(q == n // 2 - 1)
        def _():
            with jax.named_scope("hplane"):
                hot_plane()

        @pl.when(q == n // 2)
        def _():
            with jax.named_scope("hline"):
                hot_line()

        @pl.when(q < n - 2)
        def _():
            with jax.named_scope("wsend"):
                wait_chunk(q + 1, send, send_sem)
            send_chunk(q + 2)

    pl.loop(0, n // 2)(add_returned)
    with jax.named_scope("hcore"):
        hot_core()
    pl.loop(n // 2, n - 1)(add_returned)
    with jax.named_scope("hfinish"):
        hot_finish()
    add_returned(n - 1)
    y_ref[...] = acc_ref[...].astype(BF16)

    wait_chunk(n - 1, send, send_sem)

    @pl.loop(0, n)
    def _(q):
        wait_chunk(q, out, ret_sem)
    with jax.named_scope("hsend"):
        hot_sends_done()


def solution(mesh):
    group_size = mesh.shape['ep']
    n = 1
    while 2 * n * n * n < group_size:
        n += 1
    row_spec = P(('dp', 'ep'), None)
    list_spec = P(('dp', 'ep'))
    expert_spec = P('ep', None, None)

    def local_layer(x, ids, gates, hot_tok, hot_gates, wg, wu, wd):
        wg, wu, wd = wg[0], wu[0], wd[0]
        tokens, d_model = x.shape
        d_ff = wg.shape[1]
        blocks = 2 * n * n
        piece = d_model // FOLD
        main = blocks * SLOTS
        block_buf = pltpu.VMEM((n, blocks, SLOTS, d_model + piece), BF16)
        in_vmem = pl.BlockSpec(memory_space=pltpu.VMEM)
        in_hbm = pl.BlockSpec(memory_space=pl.ANY)
        dma = pltpu.SemaphoreType.DMA
        weights = [pltpu.VMEM((d_model, d_ff), BF16)] * 2 + [pltpu.VMEM((d_ff, d_model), BF16)]
        return pl.pallas_call(
            functools.partial(layer_kernel, n),
            out_shape=jax.ShapeDtypeStruct((tokens, d_model), BF16),
            in_specs=[in_vmem] * 5 + [in_hbm] * 3,
            out_specs=in_vmem,
            scratch_shapes=[block_buf] * 4 + weights + weights
            + [pltpu.VMEM((d_model // (2 * n), d_ff), BF16)] * 2 + [pltpu.VMEM((d_ff // n, d_model // 2), BF16)]
            + [pltpu.VMEM((main + blocks, d_model), BF16), pltpu.VMEM((main + blocks, d_ff), BF16),
               pltpu.VMEM((main, piece), BF16), pltpu.VMEM((n, 3 * tokens, main + blocks), BF16), pltpu.VMEM((tokens, d_model), F32)]
            + [dma((3,)), dma((n,)), dma((n,)), dma((n,)), dma((n,)), dma((5, 3)), dma((5, 3))],
            compiler_params=pltpu.CompilerParams(vmem_limit_bytes=VMEM_LIMIT, collective_id=0, has_side_effects=True),
            name="moe_layer",
        )(ids.T, gates.T, hot_tok[None, :], hot_gates[None, :], x, wg, wu, wd)

    return jax.shard_map(local_layer, mesh=mesh,
                         in_specs=(row_spec, row_spec, row_spec, list_spec, list_spec, expert_spec, expert_spec, expert_spec),
                         out_specs=row_spec, check_vma=False)
```

```python
import functools

import jax
import jax.numpy as jnp
from jax import lax
from jax.experimental import pallas as pl
from jax.experimental.pallas import tpu as pltpu
from jax.sharding import PartitionSpec as P

F32 = jnp.float32
BF16 = jnp.bfloat16
SLOTS = 8
FOLD = 8
VMEM_LIMIT = 60 * 1024 * 1024


def dotf(a, b):
    return jnp.dot(a, b, preferred_element_type=F32)


def iota(shape, dim):
    return lax.broadcasted_iota(jnp.int32, shape, dim)


def ones_where(mask):
    return jnp.where(mask, 1.0, 0.0).astype(BF16)


def three_terms(a):
    hi = a.astype(BF16)
    rest = a - hi.astype(F32)
    mid = rest.astype(BF16)
    low = (rest - mid.astype(F32)).astype(BF16)
    return jnp.concatenate([hi, mid, low], axis=0)


def layer_kernel(n, ids_ref, gates_ref, hot_tok_ref, hot_gate_ref, x_ref, wg_ref, wu_ref, wd_ref, y_ref,
                 send, recv, out, back, wg, wu, wd, hot_g, hot_u, hot_d, stage_g, stage_u, stage_d,
                 rows_ref, u_ref, fold_ref, weight_ref, acc_ref,
                 load_sem, send_sem, recv_sem, ret_sem, back_sem, from_sem, to_sem):
    me = lax.axis_index('ep')
    devices = 2 * n * n * n
    c, mx, my, mz = me % 2, (me // 2) % n, (me // (2 * n)) % n, me // (2 * n * n)
    blocks = 2 * n * n
    tokens, d_model = x_ref.shape
    d_ff = wd_ref.shape[0]
    top_k = ids_ref.shape[0]
    piece = d_model // FOLD
    main = blocks * SLOTS
    chunk_rows = main + blocks

    def device(z, y, x, core):
        return ((z % n * n + y % n) * n + x % n) * 2 + core % 2

    def peer(q, i, sign):
        kc, kx, ky = i % 2, (i // 2) % n, i // (2 * n)
        kz = (q + 2 * n - kx - ky) % n
        if sign > 0:
            return device(mz + kz, my + ky, mx + kx, c + kc)
        return device(mz + n - kz, my + n - ky, mx + n - kx, c + kc)

    def remote(src, dst, s_sem, r_sem, to):
        return pltpu.make_async_remote_copy(src_ref=src, dst_ref=dst, send_sem=s_sem, recv_sem=r_sem, device_id={'ep': to},
                                            device_id_type=pl.DeviceIdType.MESH)

    def wait_for(ref, sem):
        pltpu.make_async_copy(ref, ref, sem).wait()

    def rows_at(ref, start, size, unit):
        return ref.at[pl.ds(pl.multiple_of(start, unit), size)]

    barrier = pltpu.get_barrier_semaphore()

    def signal_all():
        @pl.loop(1, devices)
        def _(i):
            pl.semaphore_signal(barrier, inc=1, device_id={'ep': (me + i) % devices}, device_id_type=pl.DeviceIdType.MESH)

    pl.when(me != 0)(signal_all)

    own = [pltpu.make_async_copy(src, dst, load_sem.at[p])
           for p, (src, dst) in enumerate(((wg_ref, wg), (wu_ref, wu), (wd_ref, wd)))]
    for copy in own:
        copy.start()

    unit = d_model // (2 * n * n * n)
    unit_d, unit_c = d_ff // (n * n), d_model // (2 * n)
    parts = ((wg, hot_g, stage_g, mz, (my, mx)), (wu, hot_u, stage_u, mx, (mz, my)), (wd, hot_d, stage_d, my, (mx, mz)))

    def line_device(p, k, core):
        return (device(k, my, mx, core), device(mz, my, k, core), device(mz, k, mx, core))[p]

    def plane_device(p, a, b):
        return (device(mz, a, b, c), device(a, b, mx, c), device(b, my, a, c))[p]

    def quarter(p, ref, half, k):
        if p < 2:
            size = n * n * unit
            return rows_at(ref, half * (d_model // 2) + k * size, size, 16)
        size = n * unit_d
        return ref.at[pl.ds(pl.multiple_of(k * size, 16), size), pl.ds(pl.multiple_of(half * (d_model // 2), 128), d_model // 2)]

    def hot_piece(p, ref, half, k, a, b):
        if p < 2:
            return rows_at(ref, half * (d_model // 2) + k * (n * n * unit) + (a * n + b) * unit, unit, 16)
        return ref.at[pl.ds(pl.multiple_of(k * (n * unit_d) + a * unit_d, 16), unit_d),
                      pl.ds(pl.multiple_of(half * (d_model // 2) + b * unit_c, 128), unit_c)]

    def stage_piece(p, ref, a, b):
        if p < 2:
            return rows_at(ref, (a * n + b) * unit, unit, 16)
        return ref.at[pl.ds(pl.multiple_of(a * unit_d, 16), unit_d), pl.ds(pl.multiple_of(b * unit_c, 128), unit_c)]

    def pieces_like(p, ref):
        if p < 2:
            return ref.at[pl.ds(0, (n * n - 1) * unit)]
        return ref.at[pl.ds(0, (n * n - 1) * unit_d), pl.ds(0, unit_c)]

    def on_line(p):
        plane = parts[p][4]
        return jnp.logical_and(plane[0] == 0, plane[1] == 0)

    def hot_root():
        for copy in own:
            copy.wait()
        pl.semaphore_wait(barrier, devices - 1)
        for k in (*range(n // 2, 0, -1), *range(n - 1, n // 2, -1), 0):
            for half in range(2):
                for p, (src, _, stage, _, _) in enumerate(parts):
                    if k > 0 or half > 0:
                        remote(quarter(p, src, half, k), stage, from_sem.at[0, p], to_sem.at[0, p], line_device(p, k, half)).start()
        for p, (src, _, stage, _, _) in enumerate(parts):
            stage[...] = quarter(p, src, 0, 0)[...]
        for p, (src, _, _, _, _) in enumerate(parts):
            wait_for(src.at[pl.ds(0, (2 * n - 1) * (n * n * unit if p < 2 else n * unit_d // 2))], from_sem.at[0, p])
        signal_all()

    def hot_scatter():
        for p, (_, hot, stage, line, _) in enumerate(parts):
            @pl.when(on_line(p))
            def _(p=p, hot=hot, stage=stage, line=line):
                @pl.when(me != 0)
                def _():
                    wait_for(stage, to_sem.at[0, p])

                @pl.loop(1, n * n)
                def _(j):
                    a, b = j // n, j % n
                    remote(stage_piece(p, stage, a, b), hot_piece(p, hot, c, line, a, b), from_sem.at[1, p], to_sem.at[1, p],
                           plane_device(p, a, b)).start()
                hot_piece(p, hot, c, line, 0, 0)[...] = stage_piece(p, stage, 0, 0)[...]

    def hot_plane():
        for p, (_, hot, _, line, plane) in enumerate(parts):
            mine = hot_piece(p, hot, c, line, plane[0], plane[1])

            @pl.when(jnp.logical_not(on_line(p)))
            def _(p=p, mine=mine):
                wait_for(mine, to_sem.at[1, p])

            @pl.loop(1, n * n)
            def _(j, p=p, mine=mine, plane=plane):
                remote(mine, mine, from_sem.at[2, p], to_sem.at[2, p], plane_device(p, plane[0] + j // n, plane[1] + j % n)).start()

    def hot_line():
        for p, (_, hot, _, line, _) in enumerate(parts):
            wait_for(pieces_like(p, hot), to_sem.at[2, p])
            mine = quarter(p, hot, c, line)
            for j in range(1, n):
                remote(mine, mine, from_sem.at[3, p], to_sem.at[3, p], line_device(p, line + j, c)).start()

    def line_like(p, ref):
        if p < 2:
            return ref.at[pl.ds(0, (n - 1) * n * n * unit)]
        return ref.at[pl.ds(0, (n - 1) * n * unit_d), pl.ds(0, d_model // 2)]

    def half_of(p, ref, half):
        if p < 2:
            return rows_at(ref, half * (d_model // 2), d_model // 2, 16)
        return ref.at[:, pl.ds(pl.multiple_of(half * (d_model // 2), 128), d_model // 2)]

    def hot_core():
        for p, (_, hot, _, _, _) in enumerate(parts):
            wait_for(line_like(p, hot), to_sem.at[3, p])
            mine = half_of(p, hot, c)
            remote(mine, mine, from_sem.at[4, p], to_sem.at[4, p], device(mz, my, mx, c + 1)).start()

    def hot_finish():
        for p, (_, hot, _, _, _) in enumerate(parts):
            wait_for(half_of(p, hot, 1 - c), to_sem.at[4, p])
        gate = dotf(x_ref[...], hot_g[...])
        up = dotf(x_ref[...], hot_u[...])
        u = (jax.nn.silu(gate) * up).astype(BF16)
        count = hot_tok_ref.shape[1]
        same = iota((tokens, count), 0) == hot_tok_ref[...]
        weight = jnp.sum(jnp.where(same, hot_gate_ref[...], 0.0), axis=1, keepdims=True)
        is_hot = jnp.sum(jnp.where(same, 1.0, 0.0), axis=1, keepdims=True) > 0.5
        for f in range(FOLD):
            cols = slice(f * piece, (f + 1) * piece)
            h = dotf(u, hot_d[:, cols]).astype(BF16)
            acc_ref[:, cols] += jnp.where(is_hot, weight * h.astype(F32), 0.0)

    def hot_sends_done():
        for p, (_, hot, _, _, _) in enumerate(parts):
            @pl.when(on_line(p))
            def _(p=p, hot=hot):
                wait_for(pieces_like(p, hot), from_sem.at[1, p])
            wait_for(pieces_like(p, hot), from_sem.at[2, p])
            wait_for(line_like(p, hot), from_sem.at[3, p])
            wait_for(half_of(p, hot, c), from_sem.at[4, p])

    def expert_of(q, i):
        return peer(q, i, 1)

    def fold(pieces):
        r = iota((main, main), 0)
        return dotf(ones_where(iota((main, main), 1) == r % FOLD * blocks + r // FOLD), pieces).astype(BF16)

    def unfold(folded):
        r = iota((main, main), 0)
        return dotf(ones_where(iota((main, main), 1) == r % blocks * FOLD + r // blocks), folded).astype(BF16)

    def pick_rows(q, count, slots):
        row = iota((count, tokens), 0)
        expert = expert_of(q, row // slots)
        member = ids_ref[0:1, :] == expert
        for j in range(1, top_k):
            member = jnp.logical_or(member, ids_ref[j:j + 1, :] == expert)
        earlier = ones_where(iota((tokens, tokens), 0) < iota((tokens, tokens), 1))
        member_f = jnp.where(member, 1.0, 0.0)
        rank = dotf(member_f.astype(BF16), earlier)
        slot = (row % slots).astype(F32) if slots > 1 else float(SLOTS)
        return jnp.where(rank == slot, member_f, 0.0).astype(BF16)

    def fill(q):
        pick = pick_rows(q, main, SLOTS)
        ninth = pick_rows(q, blocks, 1)
        for f in range(FOLD):
            cols = slice(f * piece, (f + 1) * piece)
            send[q, :, :, cols] = dotf(pick, x_ref[:, cols]).astype(BF16).reshape(blocks, SLOTS, piece)
            fold_ref[f * blocks:(f + 1) * blocks] = dotf(ninth, x_ref[:, cols]).astype(BF16)
        send[q, :, :, d_model:] = fold(fold_ref[...]).reshape(blocks, FOLD, piece)

    def start_sends(q, src, dst, s_sem, r_sem, sign):
        @pl.loop(jnp.where(q == 0, 1, 0) if not isinstance(q, int) else int(q == 0), blocks)
        def _(i):
            remote(src.at[q, i], dst.at[q, i], s_sem.at[q], r_sem.at[q], peer(q, i, sign)).start()

    def wait_chunk(q, buf, sem):
        if isinstance(q, int):
            wait_for(buf.at[0, pl.ds(1, blocks - 1)] if q == 0 else buf.at[q], sem.at[q])
            return

        @pl.when(q == 0)
        def _():
            wait_for(buf.at[0, pl.ds(1, blocks - 1)], sem.at[0])

        @pl.when(q > 0)
        def _():
            wait_for(buf.at[q], sem.at[q])

    def load_rows(q, buf):
        rows_ref[:main] = buf[q, :, :, :d_model].reshape(main, d_model)
        pieces = unfold(buf[q, :, :, d_model:].reshape(main, piece))
        for f in range(FOLD):
            rows_ref[main:, f * piece:(f + 1) * piece] = pieces[f * blocks:(f + 1) * blocks]

    def send_chunk(q):
        start_sends(q, send, recv, send_sem, recv_sem, 1)

    width = 256 if d_ff % 256 == 0 else d_ff

    def expert(q):
        with jax.named_scope("wrecv"):
            wait_chunk(q, recv, recv_sem)
        load_rows(q, recv)
        for w in range(d_ff // width):
            cols = slice(w * width, (w + 1) * width)
            gate = dotf(rows_ref[...], wg[:, cols])
            up = dotf(rows_ref[...], wu[:, cols])
            u_ref[:, cols] = (jax.nn.silu(gate) * up).astype(BF16)
        for f in range(FOLD):
            cols = slice(f * piece, (f + 1) * piece)
            res = dotf(u_ref[...], wd[:, cols]).astype(BF16)
            out[q, :, :, cols] = res[:main].reshape(blocks, SLOTS, piece)
            fold_ref[f * blocks:(f + 1) * blocks] = res[main:]
        out[q, :, :, d_model:] = fold(fold_ref[...]).reshape(blocks, FOLD, piece)

    def return_chunk(q):
        start_sends(q, out, back, ret_sem, back_sem, -1)

    def fill_weights(q):
        def weights(count, slots):
            row = iota((count, tokens), 0)
            expert = expert_of(q, row // slots)
            member = ids_ref[0:1, :] == expert
            weight = jnp.where(member, gates_ref[0:1, :], 0.0)
            for j in range(1, top_k):
                here = ids_ref[j:j + 1, :] == expert
                member = jnp.logical_or(member, here)
                weight = jnp.where(here, gates_ref[j:j + 1, :], weight)
            earlier = ones_where(iota((tokens, tokens), 0) < iota((tokens, tokens), 1))
            rank = dotf(ones_where(member), earlier)
            slot = (row % slots).astype(F32) if slots > 1 else float(SLOTS)
            return jnp.where(rank == slot, weight, 0.0)
        weight_ref[q, :, :main] = three_terms(weights(main, SLOTS).T)
        weight_ref[q, :, main:] = three_terms(weights(blocks, 1).T)

    def add_returned(q):
        with jax.named_scope("wback"):
            wait_chunk(q, back, back_sem)
        load_rows(q, back)
        for f in range(FOLD):
            cols = slice(f * piece, (f + 1) * piece)
            terms = dotf(weight_ref[q], rows_ref[:, cols])
            acc_ref[:, cols] += terms[2 * tokens:] + terms[tokens:2 * tokens] + terms[:tokens]

    def others_wait():
        for copy in own:
            copy.wait()
        pl.semaphore_wait(barrier, devices - 1)

    with jax.named_scope("fill"):
        pl.loop(0, n)(fill)
    recv[0, 0] = send[0, 0]
    acc_ref[...] = jnp.zeros_like(acc_ref)
    with jax.named_scope("root"):
        pl.when(me == 0)(hot_root)
    with jax.named_scope("barrier"):
        pl.when(me != 0)(others_wait)
    with jax.named_scope("hscatter"):
        hot_scatter()
    send_chunk(0)
    with jax.named_scope("hplane"):
        hot_plane()
    send_chunk(1)
    with jax.named_scope("fweights"):
        pl.loop(0, n)(fill_weights)

    @pl.loop(0, n)
    def _(q):
        expert(q)

        @pl.when(q == 0)
        def _():
            back[0, 0] = out[0, 0]
            with jax.named_scope("hline"):
                hot_line()

        return_chunk(q)

        @pl.when(q < n - 2)
        def _():
            send_chunk(q + 2)

    pl.loop(0, n // 2)(add_returned)
    with jax.named_scope("hcore"):
        hot_core()
    pl.loop(n // 2, n - 1)(add_returned)
    with jax.named_scope("hfinish"):
        hot_finish()
    add_returned(n - 1)
    y_ref[...] = acc_ref[...].astype(BF16)

    @pl.loop(0, n)
    def _(q):
        wait_chunk(q, send, send_sem)
        wait_chunk(q, out, ret_sem)
    with jax.named_scope("hsend"):
        hot_sends_done()


def solution(mesh):
    group_size = mesh.shape['ep']
    n = 1
    while 2 * n * n * n < group_size:
        n += 1
    row_spec = P(('dp', 'ep'), None)
    list_spec = P(('dp', 'ep'))
    expert_spec = P('ep', None, None)

    def local_layer(x, ids, gates, hot_tok, hot_gates, wg, wu, wd):
        wg, wu, wd = wg[0], wu[0], wd[0]
        tokens, d_model = x.shape
        d_ff = wg.shape[1]
        blocks = 2 * n * n
        piece = d_model // FOLD
        main = blocks * SLOTS
        block_buf = pltpu.VMEM((n, blocks, SLOTS, d_model + piece), BF16)
        in_vmem = pl.BlockSpec(memory_space=pltpu.VMEM)
        in_hbm = pl.BlockSpec(memory_space=pl.ANY)
        dma = pltpu.SemaphoreType.DMA
        weights = [pltpu.VMEM((d_model, d_ff), BF16)] * 2 + [pltpu.VMEM((d_ff, d_model), BF16)]
        return pl.pallas_call(
            functools.partial(layer_kernel, n),
            out_shape=jax.ShapeDtypeStruct((tokens, d_model), BF16),
            in_specs=[in_vmem] * 5 + [in_hbm] * 3,
            out_specs=in_vmem,
            scratch_shapes=[block_buf] * 4 + weights + weights
            + [pltpu.VMEM((d_model // (2 * n), d_ff), BF16)] * 2 + [pltpu.VMEM((d_ff // n, d_model // 2), BF16)]
            + [pltpu.VMEM((main + blocks, d_model), BF16), pltpu.VMEM((main + blocks, d_ff), BF16),
               pltpu.VMEM((main, piece), BF16), pltpu.VMEM((n, 3 * tokens, main + blocks), BF16), pltpu.VMEM((tokens, d_model), F32)]
            + [dma((3,)), dma((n,)), dma((n,)), dma((n,)), dma((n,)), dma((5, 3)), dma((5, 3))],
            compiler_params=pltpu.CompilerParams(vmem_limit_bytes=VMEM_LIMIT, collective_id=0, has_side_effects=True),
            name="moe_layer",
        )(ids.T, gates.T, hot_tok[None, :], hot_gates[None, :], x, wg, wu, wd)

    return jax.shard_map(local_layer, mesh=mesh,
                         in_specs=(row_spec, row_spec, row_spec, list_spec, list_spec, expert_spec, expert_spec, expert_spec),
                         out_specs=row_spec, check_vma=False)
```

```python
import functools

import jax
import jax.numpy as jnp
from jax import lax
from jax.experimental import pallas as pl
from jax.experimental.pallas import tpu as pltpu
from jax.sharding import PartitionSpec as P

F32 = jnp.float32
BF16 = jnp.bfloat16
SLOTS = 8
FOLD = 8
VMEM_LIMIT = 60 * 1024 * 1024


def dotf(a, b):
    return jnp.dot(a, b, preferred_element_type=F32)


def iota(shape, dim):
    return lax.broadcasted_iota(jnp.int32, shape, dim)


def ones_where(mask):
    return jnp.where(mask, 1.0, 0.0).astype(BF16)


def three_terms(a):
    hi = a.astype(BF16)
    rest = a - hi.astype(F32)
    mid = rest.astype(BF16)
    low = (rest - mid.astype(F32)).astype(BF16)
    return jnp.concatenate([hi, mid, low], axis=0)


def layer_kernel(n, ids_ref, gates_ref, hot_tok_ref, hot_gate_ref, x_ref, wg_ref, wu_ref, wd_ref, y_ref,
                 send, recv, out, back, relay_out, relay_back, wg, wu, wd, hot_g, hot_u, hot_d, stage_g, stage_u, stage_d,
                 rows_ref, u_ref, fold_ref, weight_ref, acc_ref,
                 load_sem, send_sem, recv_sem, ret_sem, back_sem, mid_sem, on_sem, from_sem, to_sem):
    me = lax.axis_index('ep')
    devices = 2 * n * n * n
    c, mx, my, mz = me % 2, (me // 2) % n, (me // (2 * n)) % n, me // (2 * n * n)
    blocks = 2 * n * n
    tokens, d_model = x_ref.shape
    d_ff = wd_ref.shape[0]
    top_k = ids_ref.shape[0]
    piece = d_model // FOLD
    main = blocks * SLOTS
    chunk_rows = main + blocks

    def device(z, y, x, core):
        return ((z % n * n + y % n) * n + x % n) * 2 + core % 2

    def steps(q, i):
        kx, ky = (i // 2) % n, i // (2 * n)
        return i % 2, kx, ky, (q + 2 * n - kx - ky) % n

    def peer(q, i, sign):
        kc, kx, ky, kz = steps(q, i)
        if sign > 0:
            return device(mz + kz, my + ky, mx + kx, c + kc)
        return device(mz + n - kz, my + n - ky, mx + n - kx, c + kc)

    relayed = n == 4

    def opposite(k):
        return k == n // 2

    def is_relayed(q, i):
        _, kx, ky, kz = steps(q, i)
        return jnp.logical_or(jnp.logical_or(opposite(kx), opposite(ky)), opposite(kz))

    def relay_count(q):
        pairs = [(kx, ky) for kx in range(n) for ky in range(n)]
        return 2 * sum(kx == n // 2 or ky == n // 2 or (q - kx - ky) % n == n // 2 for kx, ky in pairs)

    def hop(q, i, sign, leg):
        kc, kx, ky, kz = steps(q, i)
        way = jnp.where(kc == 0, 1, n - 1)
        move = [jnp.where(opposite(k), way, k if leg == 0 else 0) for k in (kz, ky, kx)]
        if sign < 0:
            move = [n - m for m in move]
        return device(mz + move[0], my + move[1], mx + move[2], c + kc if leg == 0 else c)

    def remote(src, dst, s_sem, r_sem, to):
        return pltpu.make_async_remote_copy(src_ref=src, dst_ref=dst, send_sem=s_sem, recv_sem=r_sem, device_id={'ep': to},
                                            device_id_type=pl.DeviceIdType.MESH)

    def wait_for(ref, sem):
        pltpu.make_async_copy(ref, ref, sem).wait()

    def rows_at(ref, start, size, unit):
        return ref.at[pl.ds(pl.multiple_of(start, unit), size)]

    barrier = pltpu.get_barrier_semaphore()

    def signal_all():
        @pl.loop(1, devices)
        def _(i):
            pl.semaphore_signal(barrier, inc=1, device_id={'ep': (me + i) % devices}, device_id_type=pl.DeviceIdType.MESH)

    pl.when(me != 0)(signal_all)

    own = [pltpu.make_async_copy(src, dst, load_sem.at[p])
           for p, (src, dst) in enumerate(((wg_ref, wg), (wu_ref, wu), (wd_ref, wd)))]
    for copy in own:
        copy.start()

    unit = d_model // (2 * n * n * n)
    unit_d, unit_c = d_ff // (n * n), d_model // (2 * n)
    parts = ((wg, hot_g, stage_g, mz, (my, mx)), (wu, hot_u, stage_u, mx, (mz, my)), (wd, hot_d, stage_d, my, (mx, mz)))

    def line_device(p, k, core):
        return (device(k, my, mx, core), device(mz, my, k, core), device(mz, k, mx, core))[p]

    def plane_device(p, a, b):
        return (device(mz, a, b, c), device(a, b, mx, c), device(b, my, a, c))[p]

    def quarter(p, ref, half, k):
        if p < 2:
            size = n * n * unit
            return rows_at(ref, half * (d_model // 2) + k * size, size, 16)
        size = n * unit_d
        return ref.at[pl.ds(pl.multiple_of(k * size, 16), size), pl.ds(pl.multiple_of(half * (d_model // 2), 128), d_model // 2)]

    def hot_piece(p, ref, half, k, a, b):
        if p < 2:
            return rows_at(ref, half * (d_model // 2) + k * (n * n * unit) + (a * n + b) * unit, unit, 16)
        return ref.at[pl.ds(pl.multiple_of(k * (n * unit_d) + a * unit_d, 16), unit_d),
                      pl.ds(pl.multiple_of(half * (d_model // 2) + b * unit_c, 128), unit_c)]

    def stage_piece(p, ref, a, b):
        if p < 2:
            return rows_at(ref, (a * n + b) * unit, unit, 16)
        return ref.at[pl.ds(pl.multiple_of(a * unit_d, 16), unit_d), pl.ds(pl.multiple_of(b * unit_c, 128), unit_c)]

    def pieces_like(p, ref):
        if p < 2:
            return ref.at[pl.ds(0, (n * n - 1) * unit)]
        return ref.at[pl.ds(0, (n * n - 1) * unit_d), pl.ds(0, unit_c)]

    def on_line(p):
        plane = parts[p][4]
        return jnp.logical_and(plane[0] == 0, plane[1] == 0)

    def hot_root():
        for copy in own:
            copy.wait()
        pl.semaphore_wait(barrier, devices - 1)
        for k in (*range(n // 2, 0, -1), *range(n - 1, n // 2, -1), 0):
            for half in range(2):
                for p, (src, _, stage, _, _) in enumerate(parts):
                    if k > 0 or half > 0:
                        remote(quarter(p, src, half, k), stage, from_sem.at[0, p], to_sem.at[0, p], line_device(p, k, half)).start()
        for p, (src, _, stage, _, _) in enumerate(parts):
            stage[...] = quarter(p, src, 0, 0)[...]
        for p, (src, _, _, _, _) in enumerate(parts):
            wait_for(src.at[pl.ds(0, (2 * n - 1) * (n * n * unit if p < 2 else n * unit_d // 2))], from_sem.at[0, p])
        signal_all()

    def hot_scatter():
        for p, (_, hot, stage, line, _) in enumerate(parts):
            @pl.when(on_line(p))
            def _(p=p, hot=hot, stage=stage, line=line):
                @pl.when(me != 0)
                def _():
                    wait_for(stage, to_sem.at[0, p])

                @pl.loop(1, n * n)
                def _(j):
                    a, b = j // n, j % n
                    remote(stage_piece(p, stage, a, b), hot_piece(p, hot, c, line, a, b), from_sem.at[1, p], to_sem.at[1, p],
                           plane_device(p, a, b)).start()
                hot_piece(p, hot, c, line, 0, 0)[...] = stage_piece(p, stage, 0, 0)[...]

    def hot_plane():
        for p, (_, hot, _, line, plane) in enumerate(parts):
            mine = hot_piece(p, hot, c, line, plane[0], plane[1])

            @pl.when(jnp.logical_not(on_line(p)))
            def _(p=p, mine=mine):
                wait_for(mine, to_sem.at[1, p])

            @pl.loop(1, n * n)
            def _(j, p=p, mine=mine, plane=plane):
                remote(mine, mine, from_sem.at[2, p], to_sem.at[2, p], plane_device(p, plane[0] + j // n, plane[1] + j % n)).start()

    def part_of_quarter(p, ref, half, k, which):
        if p < 2:
            size = n * n * unit // 2
            return rows_at(ref, half * (d_model // 2) + (2 * k + which) * size, size, 16)
        size = n * unit_d // 2
        return ref.at[pl.ds(pl.multiple_of((2 * k + which) * size, 16), size), pl.ds(pl.multiple_of(half * (d_model // 2), 128), d_model // 2)]

    def hot_line():
        for p, (_, hot, _, line, _) in enumerate(parts):
            wait_for(pieces_like(p, hot), to_sem.at[2, p])
            mine = quarter(p, hot, c, line)
            remote(mine, mine, from_sem.at[3, p], to_sem.at[3, p], line_device(p, line + 1, c)).start()
            if n > 2:
                remote(mine, mine, from_sem.at[3, p], to_sem.at[3, p], line_device(p, line + n - 1, c)).start()

    def hot_opposite():
        for p, (_, hot, _, line, _) in enumerate(parts):
            wait_for(neighbours_like(p, hot), to_sem.at[3, p])
            if n > 2:
                first = part_of_quarter(p, hot, c, (line + n - 1) % n, 0)
                second = part_of_quarter(p, hot, c, (line + 1) % n, 1)
                remote(first, first, from_sem.at[5, p], to_sem.at[5, p], line_device(p, line + 1, c)).start()
                remote(second, second, from_sem.at[5, p], to_sem.at[5, p], line_device(p, line + n - 1, c)).start()

    def neighbours_like(p, ref):
        count = min(2, n - 1)
        if p < 2:
            return ref.at[pl.ds(0, count * n * n * unit)]
        return ref.at[pl.ds(0, count * n * unit_d), pl.ds(0, d_model // 2)]

    def half_of(p, ref, half):
        if p < 2:
            return rows_at(ref, half * (d_model // 2), d_model // 2, 16)
        return ref.at[:, pl.ds(pl.multiple_of(half * (d_model // 2), 128), d_model // 2)]

    def hot_core():
        for p, (_, hot, _, _, _) in enumerate(parts):
            if n > 2:
                wait_for(quarter(p, hot, c, 0), to_sem.at[5, p])
            mine = half_of(p, hot, c)
            remote(mine, mine, from_sem.at[4, p], to_sem.at[4, p], device(mz, my, mx, c + 1)).start()

    def hot_finish():
        for p, (_, hot, _, _, _) in enumerate(parts):
            wait_for(half_of(p, hot, 1 - c), to_sem.at[4, p])
        gate = dotf(x_ref[...], hot_g[...])
        up = dotf(x_ref[...], hot_u[...])
        u = (jax.nn.silu(gate) * up).astype(BF16)
        count = hot_tok_ref.shape[1]
        same = iota((tokens, count), 0) == hot_tok_ref[...]
        weight = jnp.sum(jnp.where(same, hot_gate_ref[...], 0.0), axis=1, keepdims=True)
        is_hot = jnp.sum(jnp.where(same, 1.0, 0.0), axis=1, keepdims=True) > 0.5
        for f in range(FOLD):
            cols = slice(f * piece, (f + 1) * piece)
            h = dotf(u, hot_d[:, cols]).astype(BF16)
            acc_ref[:, cols] += jnp.where(is_hot, weight * h.astype(F32), 0.0)

    def hot_sends_done():
        for p, (_, hot, _, _, _) in enumerate(parts):
            @pl.when(on_line(p))
            def _(p=p, hot=hot):
                wait_for(pieces_like(p, hot), from_sem.at[1, p])
            wait_for(pieces_like(p, hot), from_sem.at[2, p])
            wait_for(neighbours_like(p, hot), from_sem.at[3, p])
            if n > 2:
                wait_for(quarter(p, hot, c, 0), from_sem.at[5, p])
            wait_for(half_of(p, hot, c), from_sem.at[4, p])

    def expert_of(q, i):
        return peer(q, i, 1)

    def fold(pieces):
        r = iota((main, main), 0)
        return dotf(ones_where(iota((main, main), 1) == r % FOLD * blocks + r // FOLD), pieces).astype(BF16)

    def unfold(folded):
        r = iota((main, main), 0)
        return dotf(ones_where(iota((main, main), 1) == r % blocks * FOLD + r // blocks), folded).astype(BF16)

    def pick_rows(q, count, slots):
        row = iota((count, tokens), 0)
        expert = expert_of(q, row // slots)
        member = ids_ref[0:1, :] == expert
        for j in range(1, top_k):
            member = jnp.logical_or(member, ids_ref[j:j + 1, :] == expert)
        earlier = ones_where(iota((tokens, tokens), 0) < iota((tokens, tokens), 1))
        member_f = jnp.where(member, 1.0, 0.0)
        rank = dotf(member_f.astype(BF16), earlier)
        slot = (row % slots).astype(F32) if slots > 1 else float(SLOTS)
        return jnp.where(rank == slot, member_f, 0.0).astype(BF16)

    def fill(q):
        pick = pick_rows(q, main, SLOTS)
        ninth = pick_rows(q, blocks, 1)
        for f in range(FOLD):
            cols = slice(f * piece, (f + 1) * piece)
            send[q, :, :, cols] = dotf(pick, x_ref[:, cols]).astype(BF16).reshape(blocks, SLOTS, piece)
            fold_ref[f * blocks:(f + 1) * blocks] = dotf(ninth, x_ref[:, cols]).astype(BF16)
        send[q, :, :, d_model:] = fold(fold_ref[...]).reshape(blocks, FOLD, piece)

    def start_sends(q, src, dst, relay, way, s_sem, r_sem, sign):
        first = int(q == 0) if isinstance(q, int) else jnp.where(q == 0, 1, 0)
        if relayed:
            @pl.loop(0, blocks)
            def _(i):
                @pl.when(is_relayed(q, i))
                def _():
                    remote(src.at[q, i], relay.at[q, i], s_sem.at[q], mid_sem.at[way, q], hop(q, i, sign, 0)).start()

        @pl.loop(first, blocks)
        def _(i):
            def direct():
                remote(src.at[q, i], dst.at[q, i], s_sem.at[q], r_sem.at[q], peer(q, i, sign)).start()
            if relayed:
                pl.when(jnp.logical_not(is_relayed(q, i)))(direct)
            else:
                direct()

    def wait_relay(q, relay, sem):
        for count in sorted({relay_count(k) for k in range(n)}):
            chunks = [k for k in range(n) if relay_count(k) == count]
            if isinstance(q, int):
                if q in chunks:
                    wait_for(relay.at[q, pl.ds(0, count)], sem)
            else:
                same = functools.reduce(jnp.logical_or, [q == k for k in chunks])

                @pl.when(same)
                def _(count=count):
                    wait_for(relay.at[q, pl.ds(0, count)], sem)

    def pass_on(q, dst, relay, way, r_sem, sign):
        if not relayed:
            return
        wait_relay(q, relay, mid_sem.at[way, q])

        @pl.loop(0, blocks)
        def _(i):
            @pl.when(is_relayed(q, i))
            def _():
                remote(relay.at[q, i], dst.at[q, i], on_sem.at[way, q], r_sem.at[q], hop(q, i, sign, 1)).start()

    def pass_on_sent(q):
        pass_on(q, recv, relay_out, 0, recv_sem, 1)

    def pass_on_returned(q):
        pass_on(q, back, relay_back, 1, back_sem, -1)

    def wait_chunk(q, buf, sem):
        if isinstance(q, int):
            wait_for(buf.at[0, pl.ds(1, blocks - 1)] if q == 0 else buf.at[q], sem.at[q])
            return

        @pl.when(q == 0)
        def _():
            wait_for(buf.at[0, pl.ds(1, blocks - 1)], sem.at[0])

        @pl.when(q > 0)
        def _():
            wait_for(buf.at[q], sem.at[q])

    def load_rows(q, buf):
        rows_ref[:main] = buf[q, :, :, :d_model].reshape(main, d_model)
        pieces = unfold(buf[q, :, :, d_model:].reshape(main, piece))
        for f in range(FOLD):
            rows_ref[main:, f * piece:(f + 1) * piece] = pieces[f * blocks:(f + 1) * blocks]

    def send_chunk(q):
        start_sends(q, send, recv, relay_out, 0, send_sem, recv_sem, 1)

    width = 256 if d_ff % 256 == 0 else d_ff

    def expert(q):
        with jax.named_scope("wrecv"):
            wait_chunk(q, recv, recv_sem)
        load_rows(q, recv)
        for w in range(d_ff // width):
            cols = slice(w * width, (w + 1) * width)
            gate = dotf(rows_ref[...], wg[:, cols])
            up = dotf(rows_ref[...], wu[:, cols])
            u_ref[:, cols] = (jax.nn.silu(gate) * up).astype(BF16)
        for f in range(FOLD):
            cols = slice(f * piece, (f + 1) * piece)
            res = dotf(u_ref[...], wd[:, cols]).astype(BF16)
            out[q, :, :, cols] = res[:main].reshape(blocks, SLOTS, piece)
            fold_ref[f * blocks:(f + 1) * blocks] = res[main:]
        out[q, :, :, d_model:] = fold(fold_ref[...]).reshape(blocks, FOLD, piece)

    def return_chunk(q):
        start_sends(q, out, back, relay_back, 1, ret_sem, back_sem, -1)

    def fill_weights(q):
        def weights(count, slots):
            row = iota((count, tokens), 0)
            expert = expert_of(q, row // slots)
            member = ids_ref[0:1, :] == expert
            weight = jnp.where(member, gates_ref[0:1, :], 0.0)
            for j in range(1, top_k):
                here = ids_ref[j:j + 1, :] == expert
                member = jnp.logical_or(member, here)
                weight = jnp.where(here, gates_ref[j:j + 1, :], weight)
            earlier = ones_where(iota((tokens, tokens), 0) < iota((tokens, tokens), 1))
            rank = dotf(ones_where(member), earlier)
            slot = (row % slots).astype(F32) if slots > 1 else float(SLOTS)
            return jnp.where(rank == slot, weight, 0.0)
        weight_ref[q, :, :main] = three_terms(weights(main, SLOTS).T)
        weight_ref[q, :, main:] = three_terms(weights(blocks, 1).T)

    def add_returned(q):
        with jax.named_scope("wback"):
            wait_chunk(q, back, back_sem)
        load_rows(q, back)
        for f in range(FOLD):
            cols = slice(f * piece, (f + 1) * piece)
            terms = dotf(weight_ref[q], rows_ref[:, cols])
            acc_ref[:, cols] += terms[2 * tokens:] + terms[tokens:2 * tokens] + terms[:tokens]

    def others_wait():
        for copy in own:
            copy.wait()
        pl.semaphore_wait(barrier, devices - 1)

    with jax.named_scope("fill"):
        pl.loop(0, n)(fill)
    recv[0, 0] = send[0, 0]
    acc_ref[...] = jnp.zeros_like(acc_ref)
    with jax.named_scope("root"):
        pl.when(me == 0)(hot_root)
    with jax.named_scope("barrier"):
        pl.when(me != 0)(others_wait)
    with jax.named_scope("hscatter"):
        hot_scatter()
    send_chunk(0)
    with jax.named_scope("hplane"):
        hot_plane()
    send_chunk(1)
    with jax.named_scope("fweights"):
        pl.loop(0, n)(fill_weights)
    with jax.named_scope("psent0"):
        pass_on_sent(0)

    @pl.loop(0, n)
    def _(q):
        expert(q)

        @pl.when(q == 0)
        def _():
            back[0, 0] = out[0, 0]

        return_chunk(q)

        @pl.when(q < n - 1)
        def _():
            with jax.named_scope("psent"):
                pass_on_sent(q + 1)

        @pl.when(q < n - 2)
        def _():
            send_chunk(q + 2)

        @pl.when(q > 0)
        def _():
            with jax.named_scope("pret"):
                pass_on_returned(q - 1)

        @pl.when(q == 0)
        def _():
            with jax.named_scope("hline"):
                hot_line()

        @pl.when(q == 1)
        def _():
            with jax.named_scope("hopp"):
                hot_opposite()

    with jax.named_scope("hcore"):
        hot_core()
    pl.loop(0, n // 2)(add_returned)
    with jax.named_scope("pretlast"):
        pass_on_returned(n - 1)
    pl.loop(n // 2, n - 1)(add_returned)
    with jax.named_scope("hfinish"):
        hot_finish()
    add_returned(n - 1)
    y_ref[...] = acc_ref[...].astype(BF16)

    @pl.loop(0, n)
    def _(q):
        wait_chunk(q, send, send_sem)
        wait_chunk(q, out, ret_sem)
        if relayed:
            wait_relay(q, relay_out, on_sem.at[0, q])
            wait_relay(q, relay_back, on_sem.at[1, q])
    with jax.named_scope("hsend"):
        hot_sends_done()


def solution(mesh):
    group_size = mesh.shape['ep']
    n = 1
    while 2 * n * n * n < group_size:
        n += 1
    row_spec = P(('dp', 'ep'), None)
    list_spec = P(('dp', 'ep'))
    expert_spec = P('ep', None, None)

    def local_layer(x, ids, gates, hot_tok, hot_gates, wg, wu, wd):
        wg, wu, wd = wg[0], wu[0], wd[0]
        tokens, d_model = x.shape
        d_ff = wg.shape[1]
        blocks = 2 * n * n
        piece = d_model // FOLD
        main = blocks * SLOTS
        block_buf = pltpu.VMEM((n, blocks, SLOTS, d_model + piece), BF16)
        in_vmem = pl.BlockSpec(memory_space=pltpu.VMEM)
        in_hbm = pl.BlockSpec(memory_space=pl.ANY)
        dma = pltpu.SemaphoreType.DMA
        weights = [pltpu.VMEM((d_model, d_ff), BF16)] * 2 + [pltpu.VMEM((d_ff, d_model), BF16)]
        return pl.pallas_call(
            functools.partial(layer_kernel, n),
            out_shape=jax.ShapeDtypeStruct((tokens, d_model), BF16),
            in_specs=[in_vmem] * 5 + [in_hbm] * 3,
            out_specs=in_vmem,
            scratch_shapes=[block_buf] * 6 + weights + weights
            + [pltpu.VMEM((d_model // (2 * n), d_ff), BF16)] * 2 + [pltpu.VMEM((d_ff // n, d_model // 2), BF16)]
            + [pltpu.VMEM((main + blocks, d_model), BF16), pltpu.VMEM((main + blocks, d_ff), BF16),
               pltpu.VMEM((main, piece), BF16), pltpu.VMEM((n, 3 * tokens, main + blocks), BF16), pltpu.VMEM((tokens, d_model), F32)]
            + [dma((3,)), dma((n,)), dma((n,)), dma((n,)), dma((n,)), dma((2, n)), dma((2, n)), dma((6, 3)), dma((6, 3))],
            compiler_params=pltpu.CompilerParams(vmem_limit_bytes=VMEM_LIMIT, collective_id=0, has_side_effects=True),
            name="moe_layer",
        )(ids.T, gates.T, hot_tok[None, :], hot_gates[None, :], x, wg, wu, wd)

    return jax.shard_map(local_layer, mesh=mesh,
                         in_specs=(row_spec, row_spec, row_spec, list_spec, list_spec, expert_spec, expert_spec, expert_spec),
                         out_specs=row_spec, check_vma=False)
```

```python
import functools

import jax
import jax.numpy as jnp
from jax import lax
from jax.experimental import pallas as pl
from jax.experimental.pallas import tpu as pltpu
from jax.sharding import PartitionSpec as P

F32 = jnp.float32
BF16 = jnp.bfloat16
SLOTS = 8
FOLD = 8
VMEM_LIMIT = 60 * 1024 * 1024
SPLIT = 2
AHEAD = 6
LEAD = 2


def dotf(a, b):
    return jnp.dot(a, b, preferred_element_type=F32)


def iota(shape, dim):
    return lax.broadcasted_iota(jnp.int32, shape, dim)


def ones_where(mask):
    return jnp.where(mask, 1.0, 0.0).astype(BF16)


def three_terms(a):
    hi = a.astype(BF16)
    rest = a - hi.astype(F32)
    mid = rest.astype(BF16)
    low = (rest - mid.astype(F32)).astype(BF16)
    return jnp.concatenate([hi, mid, low], axis=0)


def layer_kernel(n, ids_ref, gates_ref, hot_tok_ref, hot_gate_ref, x_ref, wg_ref, wu_ref, wd_ref, y_ref,
                 send, recv, out, back, relay_out, relay_back, wg, wu, wd, hot_g, hot_u, hot_d, stage_g, stage_u, stage_d,
                 rows_ref, u_ref, fold_ref, weight_ref, acc_ref,
                 load_sem, send_sem, recv_sem, ret_sem, back_sem, mid_sem, on_sem, from_sem, to_sem):
    me = lax.axis_index('ep')
    devices = 2 * n * n * n
    c, mx, my, mz = me % 2, (me // 2) % n, (me // (2 * n)) % n, me // (2 * n * n)
    chunks = SPLIT * n
    blocks = 2 * n * n // SPLIT
    tokens, d_model = x_ref.shape
    d_ff = wd_ref.shape[0]
    top_k = ids_ref.shape[0]
    piece = d_model // FOLD
    main = blocks * SLOTS
    chunk_rows = main + blocks

    def device(z, y, x, core):
        return ((z % n * n + y % n) * n + x % n) * 2 + core % 2

    def steps(q, i):
        kx, ky = (i // 2) % n, i // (2 * n) * SPLIT + q % SPLIT
        return i % 2, kx, ky, (q // SPLIT + 2 * n - kx - ky) % n

    def peer(q, i, sign):
        kc, kx, ky, kz = steps(q, i)
        if sign > 0:
            return device(mz + kz, my + ky, mx + kx, c + kc)
        return device(mz + n - kz, my + n - ky, mx + n - kx, c + kc)

    relayed = n == 4

    def opposite(k):
        return k == n // 2

    def is_relayed(q, i):
        _, kx, ky, kz = steps(q, i)
        return jnp.logical_or(jnp.logical_or(opposite(kx), opposite(ky)), opposite(kz))

    def relay_count(q):
        return sum(any(opposite(k) for k in steps(q, i)[1:]) for i in range(blocks))

    def hop(q, i, sign, leg):
        kc, kx, ky, kz = steps(q, i)
        way = jnp.where(kc == 0, 1, n - 1)
        move = [jnp.where(opposite(k), way, k if leg == 0 else 0) for k in (kz, ky, kx)]
        if sign < 0:
            move = [n - m for m in move]
        return device(mz + move[0], my + move[1], mx + move[2], c + kc if leg == 0 else c)

    def remote(src, dst, s_sem, r_sem, to):
        return pltpu.make_async_remote_copy(src_ref=src, dst_ref=dst, send_sem=s_sem, recv_sem=r_sem, device_id={'ep': to},
                                            device_id_type=pl.DeviceIdType.MESH)

    def wait_for(ref, sem):
        pltpu.make_async_copy(ref, ref, sem).wait()

    def rows_at(ref, start, size, unit):
        return ref.at[pl.ds(pl.multiple_of(start, unit), size)]

    barrier = pltpu.get_barrier_semaphore()

    def signal_all():
        @pl.loop(1, devices)
        def _(i):
            pl.semaphore_signal(barrier, inc=1, device_id={'ep': (me + i) % devices}, device_id_type=pl.DeviceIdType.MESH)

    pl.when(me != 0)(signal_all)

    own = [pltpu.make_async_copy(src, dst, load_sem.at[p])
           for p, (src, dst) in enumerate(((wg_ref, wg), (wu_ref, wu), (wd_ref, wd)))]
    for copy in own:
        copy.start()

    unit = d_model // (2 * n * n * n)
    unit_d, unit_c = d_ff // (n * n), d_model // (2 * n)
    parts = ((wg, hot_g, stage_g, mz, (my, mx)), (wu, hot_u, stage_u, mx, (mz, my)), (wd, hot_d, stage_d, my, (mx, mz)))

    def line_device(p, k, core):
        return (device(k, my, mx, core), device(mz, my, k, core), device(mz, k, mx, core))[p]

    def plane_device(p, a, b):
        return (device(mz, a, b, c), device(a, b, mx, c), device(b, my, a, c))[p]

    def quarter(p, ref, half, k):
        if p < 2:
            size = n * n * unit
            return rows_at(ref, half * (d_model // 2) + k * size, size, 16)
        size = n * unit_d
        return ref.at[pl.ds(pl.multiple_of(k * size, 16), size), pl.ds(pl.multiple_of(half * (d_model // 2), 128), d_model // 2)]

    def hot_piece(p, ref, half, k, a, b):
        if p < 2:
            return rows_at(ref, half * (d_model // 2) + k * (n * n * unit) + (a * n + b) * unit, unit, 16)
        return ref.at[pl.ds(pl.multiple_of(k * (n * unit_d) + a * unit_d, 16), unit_d),
                      pl.ds(pl.multiple_of(half * (d_model // 2) + b * unit_c, 128), unit_c)]

    def stage_piece(p, ref, a, b):
        if p < 2:
            return rows_at(ref, (a * n + b) * unit, unit, 16)
        return ref.at[pl.ds(pl.multiple_of(a * unit_d, 16), unit_d), pl.ds(pl.multiple_of(b * unit_c, 128), unit_c)]

    def pieces_like(p, ref):
        if p < 2:
            return ref.at[pl.ds(0, (n * n - 1) * unit)]
        return ref.at[pl.ds(0, (n * n - 1) * unit_d), pl.ds(0, unit_c)]

    def on_line(p):
        plane = parts[p][4]
        return jnp.logical_and(plane[0] == 0, plane[1] == 0)

    def sent_like(late):
        count = 1 if late else 2 * n - 2
        for p, (src, _, _, _, _) in enumerate(parts):
            wait_for(src.at[pl.ds(0, count * (n * n * unit if p < 2 else n * unit_d // 2))], from_sem.at[6 * late, p])

    def hot_root():
        for copy in own:
            copy.wait()
        pl.semaphore_wait(barrier, devices - 1)
        order = [(k, half) for k in (*range(n // 2, n), 0, *range(n // 2 - 1, 0, -1)) for half in range(2)]
        for k, half in order:
            for p, (src, _, stage, _, _) in enumerate(parts):
                if k > 0 or half > 0:
                    remote(quarter(p, src, half, k), stage, from_sem.at[0 if (k, half) != order[-1] else 6, p], to_sem.at[0, p],
                           line_device(p, k, half)).start()
        for p, (src, _, stage, _, _) in enumerate(parts):
            stage[...] = quarter(p, src, 0, 0)[...]
        sent_like(0)
        signal_all()

    def hot_scatter():
        for p, (_, hot, stage, line, _) in enumerate(parts):
            @pl.when(on_line(p))
            def _(p=p, hot=hot, stage=stage, line=line):
                @pl.when(me != 0)
                def _():
                    wait_for(stage, to_sem.at[0, p])

                @pl.loop(1, n * n)
                def _(j):
                    a, b = j // n, j % n
                    remote(stage_piece(p, stage, a, b), hot_piece(p, hot, c, line, a, b), from_sem.at[1, p], to_sem.at[1, p],
                           plane_device(p, a, b)).start()
                hot_piece(p, hot, c, line, 0, 0)[...] = stage_piece(p, stage, 0, 0)[...]

    def hot_plane():
        for p, (_, hot, _, line, plane) in enumerate(parts):
            mine = hot_piece(p, hot, c, line, plane[0], plane[1])

            @pl.when(jnp.logical_not(on_line(p)))
            def _(p=p, mine=mine):
                wait_for(mine, to_sem.at[1, p])

            @pl.loop(1, n * n)
            def _(j, p=p, mine=mine, plane=plane):
                remote(mine, mine, from_sem.at[2, p], to_sem.at[2, p], plane_device(p, plane[0] + j // n, plane[1] + j % n)).start()

    def part_of_quarter(p, ref, half, k, which):
        if p < 2:
            size = n * n * unit // 2
            return rows_at(ref, half * (d_model // 2) + (2 * k + which) * size, size, 16)
        size = n * unit_d // 2
        return ref.at[pl.ds(pl.multiple_of((2 * k + which) * size, 16), size), pl.ds(pl.multiple_of(half * (d_model // 2), 128), d_model // 2)]

    def hot_line():
        for p, (_, hot, _, line, _) in enumerate(parts):
            wait_for(pieces_like(p, hot), to_sem.at[2, p])
            mine = quarter(p, hot, c, line)
            remote(mine, mine, from_sem.at[3, p], to_sem.at[3, p], line_device(p, line + 1, c)).start()
            if n > 2:
                remote(mine, mine, from_sem.at[3, p], to_sem.at[3, p], line_device(p, line + n - 1, c)).start()

    def hot_opposite():
        for p, (_, hot, _, line, _) in enumerate(parts):
            wait_for(neighbours_like(p, hot), to_sem.at[3, p])
            if n > 2:
                first = part_of_quarter(p, hot, c, (line + n - 1) % n, 0)
                second = part_of_quarter(p, hot, c, (line + 1) % n, 1)
                remote(first, first, from_sem.at[5, p], to_sem.at[5, p], line_device(p, line + 1, c)).start()
                remote(second, second, from_sem.at[5, p], to_sem.at[5, p], line_device(p, line + n - 1, c)).start()

    def neighbours_like(p, ref):
        count = min(2, n - 1)
        if p < 2:
            return ref.at[pl.ds(0, count * n * n * unit)]
        return ref.at[pl.ds(0, count * n * unit_d), pl.ds(0, d_model // 2)]

    def half_of(p, ref, half):
        if p < 2:
            return rows_at(ref, half * (d_model // 2), d_model // 2, 16)
        return ref.at[:, pl.ds(pl.multiple_of(half * (d_model // 2), 128), d_model // 2)]

    def hot_core():
        for p, (_, hot, _, _, _) in enumerate(parts):
            if n > 2:
                wait_for(quarter(p, hot, c, 0), to_sem.at[5, p])
            mine = half_of(p, hot, c)
            remote(mine, mine, from_sem.at[4, p], to_sem.at[4, p], device(mz, my, mx, c + 1)).start()

    def hot_finish():
        for p, (_, hot, _, _, _) in enumerate(parts):
            wait_for(half_of(p, hot, 1 - c), to_sem.at[4, p])
        gate = dotf(x_ref[...], hot_g[...])
        up = dotf(x_ref[...], hot_u[...])
        u = (jax.nn.silu(gate) * up).astype(BF16)
        count = hot_tok_ref.shape[1]
        same = iota((tokens, count), 0) == hot_tok_ref[...]
        weight = jnp.sum(jnp.where(same, hot_gate_ref[...], 0.0), axis=1, keepdims=True)
        is_hot = jnp.sum(jnp.where(same, 1.0, 0.0), axis=1, keepdims=True) > 0.5
        for f in range(FOLD):
            cols = slice(f * piece, (f + 1) * piece)
            h = dotf(u, hot_d[:, cols]).astype(BF16)
            acc_ref[:, cols] += jnp.where(is_hot, weight * h.astype(F32), 0.0)

    def hot_sends_done():
        @pl.when(me == 0)
        def _():
            sent_like(1)

        for p, (_, hot, _, _, _) in enumerate(parts):
            @pl.when(on_line(p))
            def _(p=p, hot=hot):
                wait_for(pieces_like(p, hot), from_sem.at[1, p])

            wait_for(pieces_like(p, hot), from_sem.at[2, p])
            wait_for(neighbours_like(p, hot), from_sem.at[3, p])
            if n > 2:
                wait_for(quarter(p, hot, c, 0), from_sem.at[5, p])
            wait_for(half_of(p, hot, c), from_sem.at[4, p])

    def expert_of(q, i):
        return peer(q, i, 1)

    def fold(pieces):
        r = iota((main, main), 0)
        return dotf(ones_where(iota((main, main), 1) == r % FOLD * blocks + r // FOLD), pieces).astype(BF16)

    def unfold(folded):
        r = iota((main, main), 0)
        return dotf(ones_where(iota((main, main), 1) == r % blocks * FOLD + r // blocks), folded).astype(BF16)

    def pick_rows(q, count, slots):
        row = iota((count, tokens), 0)
        expert = expert_of(q, row // slots)
        member = ids_ref[0:1, :] == expert
        for j in range(1, top_k):
            member = jnp.logical_or(member, ids_ref[j:j + 1, :] == expert)
        earlier = ones_where(iota((tokens, tokens), 0) < iota((tokens, tokens), 1))
        member_f = jnp.where(member, 1.0, 0.0)
        rank = dotf(member_f.astype(BF16), earlier)
        slot = (row % slots).astype(F32) if slots > 1 else float(SLOTS)
        return jnp.where(rank == slot, member_f, 0.0).astype(BF16)

    def fill(q):
        pick = pick_rows(q, main, SLOTS)
        ninth = pick_rows(q, blocks, 1)
        for f in range(FOLD):
            cols = slice(f * piece, (f + 1) * piece)
            send[q, :, :, cols] = dotf(pick, x_ref[:, cols]).astype(BF16).reshape(blocks, SLOTS, piece)
            fold_ref[f * blocks:(f + 1) * blocks] = dotf(ninth, x_ref[:, cols]).astype(BF16)
        send[q, :, :, d_model:] = fold(fold_ref[...]).reshape(blocks, FOLD, piece)

    def start_sends(q, src, dst, relay, way, s_sem, r_sem, sign):
        first = int(q == 0) if isinstance(q, int) else jnp.where(q == 0, 1, 0)
        if relayed:
            @pl.loop(0, blocks)
            def _(i):
                @pl.when(is_relayed(q, i))
                def _():
                    remote(src.at[q, i], relay.at[q, i], s_sem.at[q], mid_sem.at[way, q], hop(q, i, sign, 0)).start()

        @pl.loop(first, blocks)
        def _(i):
            def direct():
                remote(src.at[q, i], dst.at[q, i], s_sem.at[q], r_sem.at[q], peer(q, i, sign)).start()
            if relayed:
                pl.when(jnp.logical_not(is_relayed(q, i)))(direct)
            else:
                direct()

    def wait_relay(q, relay, sem):
        for count in sorted({relay_count(k) for k in range(chunks)}):
            alike = [k for k in range(chunks) if relay_count(k) == count]
            if isinstance(q, int):
                if q in alike:
                    wait_for(relay.at[q, pl.ds(0, count)], sem)
            else:
                same = functools.reduce(jnp.logical_or, [q == k for k in alike])

                @pl.when(same)
                def _(count=count):
                    wait_for(relay.at[q, pl.ds(0, count)], sem)

    def pass_on(q, dst, relay, way, r_sem, sign):
        if not relayed:
            return
        wait_relay(q, relay, mid_sem.at[way, q])

        @pl.loop(0, blocks)
        def _(i):
            @pl.when(is_relayed(q, i))
            def _():
                remote(relay.at[q, i], dst.at[q, i], on_sem.at[way, q], r_sem.at[q], hop(q, i, sign, 1)).start()

    def pass_on_sent(q):
        pass_on(q, recv, relay_out, 0, recv_sem, 1)

    def pass_on_returned(q):
        pass_on(q, back, relay_back, 1, back_sem, -1)

    def wait_chunk(q, buf, sem):
        if isinstance(q, int):
            wait_for(buf.at[0, pl.ds(1, blocks - 1)] if q == 0 else buf.at[q], sem.at[q])
            return

        @pl.when(q == 0)
        def _():
            wait_for(buf.at[0, pl.ds(1, blocks - 1)], sem.at[0])

        @pl.when(q > 0)
        def _():
            wait_for(buf.at[q], sem.at[q])

    def load_rows(q, buf):
        rows_ref[:main] = buf[q, :, :, :d_model].reshape(main, d_model)
        pieces = unfold(buf[q, :, :, d_model:].reshape(main, piece))
        for f in range(FOLD):
            rows_ref[main:, f * piece:(f + 1) * piece] = pieces[f * blocks:(f + 1) * blocks]

    def send_chunk(q):
        start_sends(q, send, recv, relay_out, 0, send_sem, recv_sem, 1)

    width = 256 if d_ff % 256 == 0 else d_ff

    def expert(q):
        with jax.named_scope("wrecv"):
            wait_chunk(q, recv, recv_sem)
        load_rows(q, recv)
        for w in range(d_ff // width):
            cols = slice(w * width, (w + 1) * width)
            gate = dotf(rows_ref[...], wg[:, cols])
            up = dotf(rows_ref[...], wu[:, cols])
            u_ref[:, cols] = (jax.nn.silu(gate) * up).astype(BF16)
        for f in range(FOLD):
            cols = slice(f * piece, (f + 1) * piece)
            res = dotf(u_ref[...], wd[:, cols]).astype(BF16)
            out[q, :, :, cols] = res[:main].reshape(blocks, SLOTS, piece)
            fold_ref[f * blocks:(f + 1) * blocks] = res[main:]
        out[q, :, :, d_model:] = fold(fold_ref[...]).reshape(blocks, FOLD, piece)

    def return_chunk(q):
        start_sends(q, out, back, relay_back, 1, ret_sem, back_sem, -1)

    def fill_weights(q):
        def weights(count, slots):
            row = iota((count, tokens), 0)
            expert = expert_of(q, row // slots)
            member = ids_ref[0:1, :] == expert
            weight = jnp.where(member, gates_ref[0:1, :], 0.0)
            for j in range(1, top_k):
                here = ids_ref[j:j + 1, :] == expert
                member = jnp.logical_or(member, here)
                weight = jnp.where(here, gates_ref[j:j + 1, :], weight)
            earlier = ones_where(iota((tokens, tokens), 0) < iota((tokens, tokens), 1))
            rank = dotf(ones_where(member), earlier)
            slot = (row % slots).astype(F32) if slots > 1 else float(SLOTS)
            return jnp.where(rank == slot, weight, 0.0)
        weight_ref[q, :, :main] = three_terms(weights(main, SLOTS).T)
        weight_ref[q, :, main:] = three_terms(weights(blocks, 1).T)

    def add_returned(q):
        with jax.named_scope("wback"):
            wait_chunk(q, back, back_sem)
        load_rows(q, back)
        for f in range(FOLD):
            cols = slice(f * piece, (f + 1) * piece)
            terms = dotf(weight_ref[q], rows_ref[:, cols])
            acc_ref[:, cols] += terms[2 * tokens:] + terms[tokens:2 * tokens] + terms[:tokens]

    def others_wait():
        for copy in own:
            copy.wait()
        pl.semaphore_wait(barrier, devices - 1)

    with jax.named_scope("fill"):
        pl.loop(0, chunks)(fill)
    recv[0, 0] = send[0, 0]
    acc_ref[...] = jnp.zeros_like(acc_ref)
    with jax.named_scope("root"):
        pl.when(me == 0)(hot_root)
    with jax.named_scope("barrier"):
        pl.when(me != 0)(others_wait)
    with jax.named_scope("hscatter"):
        hot_scatter()
    ahead = min(AHEAD, chunks)
    pl.loop(0, LEAD)(send_chunk)
    with jax.named_scope("hplane"):
        hot_plane()
    pl.loop(LEAD, ahead)(send_chunk)
    with jax.named_scope("fweights"):
        pl.loop(0, chunks)(fill_weights)
    with jax.named_scope("psent0"):
        pl.loop(0, LEAD)(pass_on_sent)

    @pl.loop(0, chunks)
    def _(q):
        @pl.when(q < chunks - LEAD)
        def _():
            with jax.named_scope("psent"):
                pass_on_sent(q + LEAD)

        expert(q)

        @pl.when(q == 0)
        def _():
            back[0, 0] = out[0, 0]

        return_chunk(q)

        @pl.when(q < chunks - ahead)
        def _():
            send_chunk(q + ahead)

        @pl.when(q > 0)
        def _():
            with jax.named_scope("pret"):
                pass_on_returned(q - 1)

        @pl.when(q == 1)
        def _():
            with jax.named_scope("hline"):
                hot_line()

        @pl.when(q == chunks // 2)
        def _():
            with jax.named_scope("hopp"):
                hot_opposite()

    with jax.named_scope("hcore"):
        hot_core()
    pl.loop(0, chunks // 2)(add_returned)
    with jax.named_scope("pretlast"):
        pass_on_returned(chunks - 1)
    pl.loop(chunks // 2, chunks - 1)(add_returned)
    with jax.named_scope("hfinish"):
        hot_finish()
    add_returned(chunks - 1)
    y_ref[...] = acc_ref[...].astype(BF16)

    @pl.loop(0, chunks)
    def _(q):
        wait_chunk(q, send, send_sem)
        wait_chunk(q, out, ret_sem)
        if relayed:
            wait_relay(q, relay_out, on_sem.at[0, q])
            wait_relay(q, relay_back, on_sem.at[1, q])
    with jax.named_scope("hsend"):
        hot_sends_done()


def solution(mesh):
    group_size = mesh.shape['ep']
    n = 1
    while 2 * n * n * n < group_size:
        n += 1
    row_spec = P(('dp', 'ep'), None)
    list_spec = P(('dp', 'ep'))
    expert_spec = P('ep', None, None)

    def local_layer(x, ids, gates, hot_tok, hot_gates, wg, wu, wd):
        wg, wu, wd = wg[0], wu[0], wd[0]
        tokens, d_model = x.shape
        d_ff = wg.shape[1]
        chunks = SPLIT * n
        blocks = 2 * n * n // SPLIT
        piece = d_model // FOLD
        main = blocks * SLOTS
        block_buf = pltpu.VMEM((chunks, blocks, SLOTS, d_model + piece), BF16)
        in_vmem = pl.BlockSpec(memory_space=pltpu.VMEM)
        in_hbm = pl.BlockSpec(memory_space=pl.ANY)
        dma = pltpu.SemaphoreType.DMA
        weights = [pltpu.VMEM((d_model, d_ff), BF16)] * 2 + [pltpu.VMEM((d_ff, d_model), BF16)]
        return pl.pallas_call(
            functools.partial(layer_kernel, n),
            out_shape=jax.ShapeDtypeStruct((tokens, d_model), BF16),
            in_specs=[in_vmem] * 5 + [in_hbm] * 3,
            out_specs=in_vmem,
            scratch_shapes=[block_buf] * 6 + weights + weights
            + [pltpu.VMEM((d_model // (2 * n), d_ff), BF16)] * 2 + [pltpu.VMEM((d_ff // n, d_model // 2), BF16)]
            + [pltpu.VMEM((main + blocks, d_model), BF16), pltpu.VMEM((main + blocks, d_ff), BF16),
               pltpu.VMEM((main, piece), BF16), pltpu.VMEM((chunks, 3 * tokens, main + blocks), BF16), pltpu.VMEM((tokens, d_model), F32)]
            + [dma((3,))] + [dma((chunks,))] * 4 + [dma((2, chunks))] * 2 + [dma((7, 3)), dma((6, 3))],
            compiler_params=pltpu.CompilerParams(vmem_limit_bytes=VMEM_LIMIT, collective_id=0, has_side_effects=True),
            name="moe_layer",
        )(ids.T, gates.T, hot_tok[None, :], hot_gates[None, :], x, wg, wu, wd)

    return jax.shard_map(local_layer, mesh=mesh,
                         in_specs=(row_spec, row_spec, row_spec, list_spec, list_spec, expert_spec, expert_spec, expert_spec),
                         out_specs=row_spec, check_vma=False)
```

```python
import functools

import jax
import jax.numpy as jnp
from jax import lax
from jax.experimental import pallas as pl
from jax.experimental.pallas import tpu as pltpu
from jax.sharding import PartitionSpec as P

F32 = jnp.float32
BF16 = jnp.bfloat16
SLOTS = 8
FOLD = 8
VMEM_LIMIT = 60 * 1024 * 1024
SPLIT = 2
AHEAD = 6
LEAD = 2
LAG = 3


def dotf(a, b):
    return jnp.dot(a, b, preferred_element_type=F32)


def iota(shape, dim):
    return lax.broadcasted_iota(jnp.int32, shape, dim)


def ones_where(mask):
    return jnp.where(mask, 1.0, 0.0).astype(BF16)


def three_terms(a):
    hi = a.astype(BF16)
    rest = a - hi.astype(F32)
    mid = rest.astype(BF16)
    low = (rest - mid.astype(F32)).astype(BF16)
    return jnp.concatenate([hi, mid, low], axis=0)


def layer_kernel(n, ids_ref, gates_ref, hot_tok_ref, hot_gate_ref, x_ref, wg_ref, wu_ref, wd_ref, y_ref,
                 send, recv, out, back, relay_out, relay_back, wg, wu, wd, hot_g, hot_u, hot_d, stage_g, stage_u, stage_d,
                 rows_ref, u_ref, fold_ref, weight_ref, acc_ref,
                 load_sem, send_sem, recv_sem, ret_sem, back_sem, mid_sem, on_sem, from_sem, to_sem):
    me = lax.axis_index('ep')
    devices = 2 * n * n * n
    c, mx, my, mz = me % 2, (me // 2) % n, (me // (2 * n)) % n, me // (2 * n * n)
    chunks = SPLIT * n
    blocks = 2 * n * n // SPLIT
    tokens, d_model = x_ref.shape
    d_ff = wd_ref.shape[0]
    top_k = ids_ref.shape[0]
    piece = d_model // FOLD
    main = blocks * SLOTS
    chunk_rows = main + blocks

    def device(z, y, x, core):
        return ((z % n * n + y % n) * n + x % n) * 2 + core % 2

    def steps(q, i):
        kx, ky = (i // 2) % n, i // (2 * n) * SPLIT + q % SPLIT
        return i % 2, kx, ky, (q // SPLIT + 2 * n - kx - ky) % n

    def peer(q, i, sign):
        kc, kx, ky, kz = steps(q, i)
        if sign > 0:
            return device(mz + kz, my + ky, mx + kx, c + kc)
        return device(mz + n - kz, my + n - ky, mx + n - kx, c + kc)

    relayed = n == 4

    def opposite(k):
        return k == n // 2

    def is_relayed(q, i):
        _, kx, ky, kz = steps(q, i)
        return jnp.logical_or(jnp.logical_or(opposite(kx), opposite(ky)), opposite(kz))

    def relay_count(q):
        return sum(any(opposite(k) for k in steps(q, i)[1:]) for i in range(blocks))

    def hop(q, i, sign, leg):
        kc, kx, ky, kz = steps(q, i)
        way = jnp.where(kc == 0, 1, n - 1)
        move = [jnp.where(opposite(k), way, k if leg == 0 else 0) for k in (kz, ky, kx)]
        if sign < 0:
            move = [n - m for m in move]
        return device(mz + move[0], my + move[1], mx + move[2], c + kc if leg == 0 else c)

    def remote(src, dst, s_sem, r_sem, to):
        return pltpu.make_async_remote_copy(src_ref=src, dst_ref=dst, send_sem=s_sem, recv_sem=r_sem, device_id={'ep': to},
                                            device_id_type=pl.DeviceIdType.MESH)

    def wait_for(ref, sem):
        pltpu.make_async_copy(ref, ref, sem).wait()

    def rows_at(ref, start, size, unit):
        return ref.at[pl.ds(pl.multiple_of(start, unit), size)]

    barrier = pltpu.get_barrier_semaphore()

    def signal_all():
        @pl.loop(1, devices)
        def _(i):
            pl.semaphore_signal(barrier, inc=1, device_id={'ep': (me + i) % devices}, device_id_type=pl.DeviceIdType.MESH)

    pl.when(me != 0)(signal_all)

    own = [pltpu.make_async_copy(src, dst, load_sem.at[p])
           for p, (src, dst) in enumerate(((wg_ref, wg), (wu_ref, wu), (wd_ref, wd)))]
    for copy in own:
        copy.start()

    unit = d_model // (2 * n * n * n)
    unit_d, unit_c = d_ff // (n * n), d_model // (2 * n)
    parts = ((wg, hot_g, stage_g, mz, (my, mx)), (wu, hot_u, stage_u, mx, (mz, my)), (wd, hot_d, stage_d, my, (mx, mz)))

    def line_device(p, k, core):
        return (device(k, my, mx, core), device(mz, my, k, core), device(mz, k, mx, core))[p]

    def plane_device(p, a, b):
        return (device(mz, a, b, c), device(a, b, mx, c), device(b, my, a, c))[p]

    def quarter(p, ref, half, k):
        if p < 2:
            size = n * n * unit
            return rows_at(ref, half * (d_model // 2) + k * size, size, 16)
        size = n * unit_d
        return ref.at[pl.ds(pl.multiple_of(k * size, 16), size), pl.ds(pl.multiple_of(half * (d_model // 2), 128), d_model // 2)]

    def hot_piece(p, ref, half, k, a, b):
        if p < 2:
            return rows_at(ref, half * (d_model // 2) + k * (n * n * unit) + (a * n + b) * unit, unit, 16)
        return ref.at[pl.ds(pl.multiple_of(k * (n * unit_d) + a * unit_d, 16), unit_d),
                      pl.ds(pl.multiple_of(half * (d_model // 2) + b * unit_c, 128), unit_c)]

    def stage_piece(p, ref, a, b):
        if p < 2:
            return rows_at(ref, (a * n + b) * unit, unit, 16)
        return ref.at[pl.ds(pl.multiple_of(a * unit_d, 16), unit_d), pl.ds(pl.multiple_of(b * unit_c, 128), unit_c)]

    def pieces_like(p, ref):
        if p < 2:
            return ref.at[pl.ds(0, (n * n - 1) * unit)]
        return ref.at[pl.ds(0, (n * n - 1) * unit_d), pl.ds(0, unit_c)]

    def on_line(p):
        plane = parts[p][4]
        return jnp.logical_and(plane[0] == 0, plane[1] == 0)

    def sent_like(late):
        count = 1 if late else 2 * n - 2
        for p, (src, _, _, _, _) in enumerate(parts):
            wait_for(src.at[pl.ds(0, count * (n * n * unit if p < 2 else n * unit_d // 2))], from_sem.at[6 * late, p])

    def hot_root():
        for copy in own:
            copy.wait()
        pl.semaphore_wait(barrier, devices - 1)
        order = [(k, half) for k in (*range(n // 2, n), 0, *range(n // 2 - 1, 0, -1)) for half in range(2)]
        for k, half in order:
            for p, (src, _, stage, _, _) in enumerate(parts):
                if k > 0 or half > 0:
                    remote(quarter(p, src, half, k), stage, from_sem.at[0 if (k, half) != order[-1] else 6, p], to_sem.at[0, p],
                           line_device(p, k, half)).start()
        for p, (src, _, stage, _, _) in enumerate(parts):
            stage[...] = quarter(p, src, 0, 0)[...]
        sent_like(0)
        signal_all()

    def hot_scatter():
        for p, (_, hot, stage, line, _) in enumerate(parts):
            @pl.when(on_line(p))
            def _(p=p, hot=hot, stage=stage, line=line):
                @pl.when(me != 0)
                def _():
                    wait_for(stage, to_sem.at[0, p])

                @pl.loop(1, n * n)
                def _(j):
                    a, b = j // n, j % n
                    remote(stage_piece(p, stage, a, b), hot_piece(p, hot, c, line, a, b), from_sem.at[1, p], to_sem.at[1, p],
                           plane_device(p, a, b)).start()
                hot_piece(p, hot, c, line, 0, 0)[...] = stage_piece(p, stage, 0, 0)[...]

    def hot_plane():
        for p, (_, hot, _, line, plane) in enumerate(parts):
            mine = hot_piece(p, hot, c, line, plane[0], plane[1])

            @pl.when(jnp.logical_not(on_line(p)))
            def _(p=p, mine=mine):
                wait_for(mine, to_sem.at[1, p])

            @pl.loop(1, n * n)
            def _(j, p=p, mine=mine, plane=plane):
                remote(mine, mine, from_sem.at[2, p], to_sem.at[2, p], plane_device(p, plane[0] + j // n, plane[1] + j % n)).start()

    def part_of_quarter(p, ref, half, k, which):
        if p < 2:
            size = n * n * unit // 2
            return rows_at(ref, half * (d_model // 2) + (2 * k + which) * size, size, 16)
        size = n * unit_d // 2
        return ref.at[pl.ds(pl.multiple_of((2 * k + which) * size, 16), size), pl.ds(pl.multiple_of(half * (d_model // 2), 128), d_model // 2)]

    def hot_line():
        for p, (_, hot, _, line, _) in enumerate(parts):
            wait_for(pieces_like(p, hot), to_sem.at[2, p])
            mine = quarter(p, hot, c, line)
            remote(mine, mine, from_sem.at[3, p], to_sem.at[3, p], line_device(p, line + 1, c)).start()
            if n > 2:
                remote(mine, mine, from_sem.at[3, p], to_sem.at[3, p], line_device(p, line + n - 1, c)).start()

    def hot_opposite():
        for p, (_, hot, _, line, _) in enumerate(parts):
            wait_for(neighbours_like(p, hot), to_sem.at[3, p])
            if n > 2:
                first = part_of_quarter(p, hot, c, (line + n - 1) % n, 0)
                second = part_of_quarter(p, hot, c, (line + 1) % n, 1)
                remote(first, first, from_sem.at[5, p], to_sem.at[5, p], line_device(p, line + 1, c)).start()
                remote(second, second, from_sem.at[5, p], to_sem.at[5, p], line_device(p, line + n - 1, c)).start()

    def neighbours_like(p, ref):
        count = min(2, n - 1)
        if p < 2:
            return ref.at[pl.ds(0, count * n * n * unit)]
        return ref.at[pl.ds(0, count * n * unit_d), pl.ds(0, d_model // 2)]

    def half_of(p, ref, half):
        if p < 2:
            return rows_at(ref, half * (d_model // 2), d_model // 2, 16)
        return ref.at[:, pl.ds(pl.multiple_of(half * (d_model // 2), 128), d_model // 2)]

    def hot_core():
        for p, (_, hot, _, _, _) in enumerate(parts):
            if n > 2:
                wait_for(quarter(p, hot, c, 0), to_sem.at[5, p])
            mine = half_of(p, hot, c)
            remote(mine, mine, from_sem.at[4, p], to_sem.at[4, p], device(mz, my, mx, c + 1)).start()

    def hot_finish():
        for p, (_, hot, _, _, _) in enumerate(parts):
            wait_for(half_of(p, hot, 1 - c), to_sem.at[4, p])
        gate = dotf(x_ref[...], hot_g[...])
        up = dotf(x_ref[...], hot_u[...])
        u = (jax.nn.silu(gate) * up).astype(BF16)
        count = hot_tok_ref.shape[1]
        same = iota((tokens, count), 0) == hot_tok_ref[...]
        weight = jnp.sum(jnp.where(same, hot_gate_ref[...], 0.0), axis=1, keepdims=True)
        is_hot = jnp.sum(jnp.where(same, 1.0, 0.0), axis=1, keepdims=True) > 0.5
        for f in range(FOLD):
            cols = slice(f * piece, (f + 1) * piece)
            h = dotf(u, hot_d[:, cols]).astype(BF16)
            acc_ref[:, cols] += jnp.where(is_hot, weight * h.astype(F32), 0.0)

    def hot_sends_done():
        @pl.when(me == 0)
        def _():
            sent_like(1)

        for p, (_, hot, _, _, _) in enumerate(parts):
            @pl.when(on_line(p))
            def _(p=p, hot=hot):
                wait_for(pieces_like(p, hot), from_sem.at[1, p])

            wait_for(pieces_like(p, hot), from_sem.at[2, p])
            wait_for(neighbours_like(p, hot), from_sem.at[3, p])
            if n > 2:
                wait_for(quarter(p, hot, c, 0), from_sem.at[5, p])
            wait_for(half_of(p, hot, c), from_sem.at[4, p])

    def expert_of(q, i):
        return peer(q, i, 1)

    def fold(pieces):
        r = iota((main, main), 0)
        return dotf(ones_where(iota((main, main), 1) == r % FOLD * blocks + r // FOLD), pieces).astype(BF16)

    def unfold(folded):
        r = iota((main, main), 0)
        return dotf(ones_where(iota((main, main), 1) == r % blocks * FOLD + r // blocks), folded).astype(BF16)

    def pick_rows(q, count, slots):
        row = iota((count, tokens), 0)
        expert = expert_of(q, row // slots)
        member = ids_ref[0:1, :] == expert
        for j in range(1, top_k):
            member = jnp.logical_or(member, ids_ref[j:j + 1, :] == expert)
        earlier = ones_where(iota((tokens, tokens), 0) < iota((tokens, tokens), 1))
        member_f = jnp.where(member, 1.0, 0.0)
        rank = dotf(member_f.astype(BF16), earlier)
        slot = (row % slots).astype(F32) if slots > 1 else float(SLOTS)
        return jnp.where(rank == slot, member_f, 0.0).astype(BF16)

    def fill(q):
        pick = pick_rows(q, main, SLOTS)
        ninth = pick_rows(q, blocks, 1)
        for f in range(FOLD):
            cols = slice(f * piece, (f + 1) * piece)
            send[q, :, :, cols] = dotf(pick, x_ref[:, cols]).astype(BF16).reshape(blocks, SLOTS, piece)
            fold_ref[f * blocks:(f + 1) * blocks] = dotf(ninth, x_ref[:, cols]).astype(BF16)
        send[q, :, :, d_model:] = fold(fold_ref[...]).reshape(blocks, FOLD, piece)

    def start_sends(q, src, dst, relay, way, s_sem, r_sem, sign):
        first = int(q == 0) if isinstance(q, int) else jnp.where(q == 0, 1, 0)
        if relayed:
            @pl.loop(0, blocks)
            def _(i):
                @pl.when(is_relayed(q, i))
                def _():
                    remote(src.at[q, i], relay.at[q, i], s_sem.at[q], mid_sem.at[way, q], hop(q, i, sign, 0)).start()

        @pl.loop(first, blocks)
        def _(i):
            def direct():
                remote(src.at[q, i], dst.at[q, i], s_sem.at[q], r_sem.at[q], peer(q, i, sign)).start()
            if relayed:
                pl.when(jnp.logical_not(is_relayed(q, i)))(direct)
            else:
                direct()

    def wait_relay(q, relay, sem):
        for count in sorted({relay_count(k) for k in range(chunks)}):
            alike = [k for k in range(chunks) if relay_count(k) == count]
            if isinstance(q, int):
                if q in alike:
                    wait_for(relay.at[q, pl.ds(0, count)], sem)
            else:
                same = functools.reduce(jnp.logical_or, [q == k for k in alike])

                @pl.when(same)
                def _(count=count):
                    wait_for(relay.at[q, pl.ds(0, count)], sem)

    def pass_on(q, dst, relay, way, r_sem, sign):
        if not relayed:
            return
        wait_relay(q, relay, mid_sem.at[way, q])

        @pl.loop(0, blocks)
        def _(i):
            @pl.when(is_relayed(q, i))
            def _():
                remote(relay.at[q, i], dst.at[q, i], on_sem.at[way, q], r_sem.at[q], hop(q, i, sign, 1)).start()

    def pass_on_sent(q):
        pass_on(q, recv, relay_out, 0, recv_sem, 1)

    def pass_on_returned(q):
        pass_on(q, back, relay_back, 1, back_sem, -1)

    def wait_chunk(q, buf, sem):
        if isinstance(q, int):
            wait_for(buf.at[0, pl.ds(1, blocks - 1)] if q == 0 else buf.at[q], sem.at[q])
            return

        @pl.when(q == 0)
        def _():
            wait_for(buf.at[0, pl.ds(1, blocks - 1)], sem.at[0])

        @pl.when(q > 0)
        def _():
            wait_for(buf.at[q], sem.at[q])

    def load_rows(q, buf):
        rows_ref[:main] = buf[q, :, :, :d_model].reshape(main, d_model)
        pieces = unfold(buf[q, :, :, d_model:].reshape(main, piece))
        for f in range(FOLD):
            rows_ref[main:, f * piece:(f + 1) * piece] = pieces[f * blocks:(f + 1) * blocks]

    def send_chunk(q):
        start_sends(q, send, recv, relay_out, 0, send_sem, recv_sem, 1)

    width = 256 if d_ff % 256 == 0 else d_ff

    def expert(q):
        with jax.named_scope("wrecv"):
            wait_chunk(q, recv, recv_sem)
        load_rows(q, recv)
        for w in range(d_ff // width):
            cols = slice(w * width, (w + 1) * width)
            gate = dotf(rows_ref[...], wg[:, cols])
            up = dotf(rows_ref[...], wu[:, cols])
            u_ref[:, cols] = (jax.nn.silu(gate) * up).astype(BF16)
        for f in range(FOLD):
            cols = slice(f * piece, (f + 1) * piece)
            res = dotf(u_ref[...], wd[:, cols]).astype(BF16)
            out[q, :, :, cols] = res[:main].reshape(blocks, SLOTS, piece)
            fold_ref[f * blocks:(f + 1) * blocks] = res[main:]
        out[q, :, :, d_model:] = fold(fold_ref[...]).reshape(blocks, FOLD, piece)

    def return_chunk(q):
        start_sends(q, out, back, relay_back, 1, ret_sem, back_sem, -1)

    def fill_weights(q):
        def weights(count, slots):
            row = iota((count, tokens), 0)
            expert = expert_of(q, row // slots)
            member = ids_ref[0:1, :] == expert
            weight = jnp.where(member, gates_ref[0:1, :], 0.0)
            for j in range(1, top_k):
                here = ids_ref[j:j + 1, :] == expert
                member = jnp.logical_or(member, here)
                weight = jnp.where(here, gates_ref[j:j + 1, :], weight)
            earlier = ones_where(iota((tokens, tokens), 0) < iota((tokens, tokens), 1))
            rank = dotf(ones_where(member), earlier)
            slot = (row % slots).astype(F32) if slots > 1 else float(SLOTS)
            return jnp.where(rank == slot, weight, 0.0)
        weight_ref[q, :, :main] = three_terms(weights(main, SLOTS).T)
        weight_ref[q, :, main:] = three_terms(weights(blocks, 1).T)

    def add_returned(q):
        with jax.named_scope("wback"):
            wait_chunk(q, back, back_sem)
        load_rows(q, back)
        for f in range(FOLD):
            cols = slice(f * piece, (f + 1) * piece)
            terms = dotf(weight_ref[q], rows_ref[:, cols])
            acc_ref[:, cols] += terms[2 * tokens:] + terms[tokens:2 * tokens] + terms[:tokens]

    def others_wait():
        for copy in own:
            copy.wait()
        pl.semaphore_wait(barrier, devices - 1)

    with jax.named_scope("fill"):
        pl.loop(0, chunks)(fill)
    recv[0, 0] = send[0, 0]
    acc_ref[...] = jnp.zeros_like(acc_ref)
    with jax.named_scope("root"):
        pl.when(me == 0)(hot_root)
    with jax.named_scope("barrier"):
        pl.when(me != 0)(others_wait)
    with jax.named_scope("hscatter"):
        hot_scatter()
    pl.loop(0, 4)(send_chunk)
    with jax.named_scope("fweights"):
        pl.loop(0, chunks)(fill_weights)
    with jax.named_scope("psent0"):
        pass_on_sent(0)
    pl.loop(4, min(5, chunks))(send_chunk)
    with jax.named_scope("hplane"):
        hot_plane()
    with jax.named_scope("psent1"):
        pass_on_sent(1)
    pl.loop(min(5, chunks), min(AHEAD, chunks))(send_chunk)

    @pl.loop(0, chunks)
    def _(q):
        @pl.when(q < chunks - LEAD)
        def _():
            with jax.named_scope("psent"):
                pass_on_sent(q + LEAD)

        expert(q)

        @pl.when(q == 0)
        def _():
            back[0, 0] = out[0, 0]

        return_chunk(q)

        @pl.when(q < chunks - AHEAD)
        def _():
            send_chunk(q + AHEAD)

        @pl.when(q >= LAG)
        def _():
            with jax.named_scope("pret"):
                pass_on_returned(q - LAG)

        @pl.when(q == 1)
        def _():
            with jax.named_scope("hline"):
                hot_line()

        @pl.when(q == chunks // 2)
        def _():
            with jax.named_scope("hopp"):
                hot_opposite()

    @pl.loop(0, LAG)
    def _(j):
        with jax.named_scope("pretlast"):
            pass_on_returned(chunks - LAG + j)
        add_returned(j)

    with jax.named_scope("hcore"):
        hot_core()
    pl.loop(LAG, chunks - 1)(add_returned)
    with jax.named_scope("hfinish"):
        hot_finish()
    add_returned(chunks - 1)
    y_ref[...] = acc_ref[...].astype(BF16)

    @pl.loop(0, chunks)
    def _(q):
        wait_chunk(q, send, send_sem)
        wait_chunk(q, out, ret_sem)
        if relayed:
            wait_relay(q, relay_out, on_sem.at[0, q])
            wait_relay(q, relay_back, on_sem.at[1, q])
    with jax.named_scope("hsend"):
        hot_sends_done()


def solution(mesh):
    group_size = mesh.shape['ep']
    n = 1
    while 2 * n * n * n < group_size:
        n += 1
    row_spec = P(('dp', 'ep'), None)
    list_spec = P(('dp', 'ep'))
    expert_spec = P('ep', None, None)

    def local_layer(x, ids, gates, hot_tok, hot_gates, wg, wu, wd):
        wg, wu, wd = wg[0], wu[0], wd[0]
        tokens, d_model = x.shape
        d_ff = wg.shape[1]
        chunks = SPLIT * n
        blocks = 2 * n * n // SPLIT
        piece = d_model // FOLD
        main = blocks * SLOTS
        block_buf = pltpu.VMEM((chunks, blocks, SLOTS, d_model + piece), BF16)
        in_vmem = pl.BlockSpec(memory_space=pltpu.VMEM)
        in_hbm = pl.BlockSpec(memory_space=pl.ANY)
        dma = pltpu.SemaphoreType.DMA
        weights = [pltpu.VMEM((d_model, d_ff), BF16)] * 2 + [pltpu.VMEM((d_ff, d_model), BF16)]
        return pl.pallas_call(
            functools.partial(layer_kernel, n),
            out_shape=jax.ShapeDtypeStruct((tokens, d_model), BF16),
            in_specs=[in_vmem] * 5 + [in_hbm] * 3,
            out_specs=in_vmem,
            scratch_shapes=[block_buf] * 6 + weights + weights
            + [pltpu.VMEM((d_model // (2 * n), d_ff), BF16)] * 2 + [pltpu.VMEM((d_ff // n, d_model // 2), BF16)]
            + [pltpu.VMEM((main + blocks, d_model), BF16), pltpu.VMEM((main + blocks, d_ff), BF16),
               pltpu.VMEM((main, piece), BF16), pltpu.VMEM((chunks, 3 * tokens, main + blocks), BF16), pltpu.VMEM((tokens, d_model), F32)]
            + [dma((3,))] + [dma((chunks,))] * 4 + [dma((2, chunks))] * 2 + [dma((7, 3)), dma((6, 3))],
            compiler_params=pltpu.CompilerParams(vmem_limit_bytes=VMEM_LIMIT, collective_id=0, has_side_effects=True),
            name="moe_layer",
        )(ids.T, gates.T, hot_tok[None, :], hot_gates[None, :], x, wg, wu, wd)

    return jax.shard_map(local_layer, mesh=mesh,
                         in_specs=(row_spec, row_spec, row_spec, list_spec, list_spec, expert_spec, expert_spec, expert_spec),
                         out_specs=row_spec, check_vma=False)
```

```python
import functools

import jax
import jax.numpy as jnp
from jax import lax
from jax.experimental import pallas as pl
from jax.experimental.pallas import tpu as pltpu
from jax.sharding import PartitionSpec as P

F32 = jnp.float32
BF16 = jnp.bfloat16
SLOTS = 8
FOLD = 8
VMEM_LIMIT = 60 * 1024 * 1024
SPLIT = 2
LEAD = 4
LAG = 3


def dotf(a, b):
    return jnp.dot(a, b, preferred_element_type=F32)


def iota(shape, dim):
    return lax.broadcasted_iota(jnp.int32, shape, dim)


def ones_where(mask):
    return jnp.where(mask, 1.0, 0.0).astype(BF16)


def three_terms(a):
    hi = a.astype(BF16)
    rest = a - hi.astype(F32)
    mid = rest.astype(BF16)
    low = (rest - mid.astype(F32)).astype(BF16)
    return jnp.concatenate([hi, mid, low], axis=0)


def layer_kernel(n, ids_ref, gates_ref, hot_tok_ref, hot_gate_ref, x_ref, wg_ref, wu_ref, wd_ref, y_ref,
                 send, recv, out, back, relay_out, relay_back, wg, wu, wd, hot_g, hot_u, hot_d, stage_g, stage_u, stage_d,
                 rows_ref, u_ref, fold_ref, weight_ref, acc_ref,
                 load_sem, send_sem, recv_sem, ret_sem, back_sem, mid_sem, on_sem, from_sem, to_sem):
    me = lax.axis_index('ep')
    devices = 2 * n * n * n
    c, mx, my, mz = me % 2, (me // 2) % n, (me // (2 * n)) % n, me // (2 * n * n)
    chunks = SPLIT * n
    blocks = 2 * n * n // SPLIT
    tokens, d_model = x_ref.shape
    d_ff = wd_ref.shape[0]
    top_k = ids_ref.shape[0]
    piece = d_model // FOLD
    main = blocks * SLOTS
    chunk_rows = main + blocks

    def device(z, y, x, core):
        return ((z % n * n + y % n) * n + x % n) * 2 + core % 2

    def steps(q, i):
        kx, ky = (i // 2) % n, i // (2 * n) * SPLIT + q % SPLIT
        return i % 2, kx, ky, (q // SPLIT + 2 * n - kx - ky) % n

    def peer(q, i, sign):
        kc, kx, ky, kz = steps(q, i)
        if sign > 0:
            return device(mz + kz, my + ky, mx + kx, c + kc)
        return device(mz + n - kz, my + n - ky, mx + n - kx, c + kc)

    relayed = n == 4

    def opposite(k):
        return k == n // 2

    def is_relayed(q, i):
        _, kx, ky, kz = steps(q, i)
        return jnp.logical_or(jnp.logical_or(opposite(kx), opposite(ky)), opposite(kz))

    def relay_count(q):
        return sum(any(opposite(k) for k in steps(q, i)[1:]) for i in range(blocks))

    def hop(q, i, sign, leg):
        kc, kx, ky, kz = steps(q, i)
        way = jnp.where(kc == 0, 1, n - 1)
        move = [jnp.where(opposite(k), way, k if leg == 0 else 0) for k in (kz, ky, kx)]
        if sign < 0:
            move = [n - m for m in move]
        return device(mz + move[0], my + move[1], mx + move[2], c + kc if leg == 0 else c)

    def remote(src, dst, s_sem, r_sem, to):
        return pltpu.make_async_remote_copy(src_ref=src, dst_ref=dst, send_sem=s_sem, recv_sem=r_sem, device_id={'ep': to},
                                            device_id_type=pl.DeviceIdType.MESH)

    def wait_for(ref, sem):
        pltpu.make_async_copy(ref, ref, sem).wait()

    def rows_at(ref, start, size, unit):
        return ref.at[pl.ds(pl.multiple_of(start, unit), size)]

    barrier = pltpu.get_barrier_semaphore()

    def signal_all():
        @pl.loop(1, devices)
        def _(i):
            pl.semaphore_signal(barrier, inc=1, device_id={'ep': (me + i) % devices}, device_id_type=pl.DeviceIdType.MESH)

    pl.when(me != 0)(signal_all)

    own = [pltpu.make_async_copy(src, dst, load_sem.at[p])
           for p, (src, dst) in enumerate(((wg_ref, wg), (wu_ref, wu), (wd_ref, wd)))]
    for copy in own:
        copy.start()

    unit = d_model // (2 * n * n * n)
    unit_d, unit_c = d_ff // (n * n), d_model // (2 * n)
    parts = ((wg, hot_g, stage_g, mz, (my, mx)), (wu, hot_u, stage_u, mx, (mz, my)), (wd, hot_d, stage_d, my, (mx, mz)))

    def line_device(p, k, core):
        return (device(k, my, mx, core), device(mz, my, k, core), device(mz, k, mx, core))[p]

    def plane_device(p, a, b):
        return (device(mz, a, b, c), device(a, b, mx, c), device(b, my, a, c))[p]

    def quarter(p, ref, half, k):
        if p < 2:
            size = n * n * unit
            return rows_at(ref, half * (d_model // 2) + k * size, size, 16)
        size = n * unit_d
        return ref.at[pl.ds(pl.multiple_of(k * size, 16), size), pl.ds(pl.multiple_of(half * (d_model // 2), 128), d_model // 2)]

    def hot_piece(p, ref, half, k, a, b):
        if p < 2:
            return rows_at(ref, half * (d_model // 2) + k * (n * n * unit) + (a * n + b) * unit, unit, 16)
        return ref.at[pl.ds(pl.multiple_of(k * (n * unit_d) + a * unit_d, 16), unit_d),
                      pl.ds(pl.multiple_of(half * (d_model // 2) + b * unit_c, 128), unit_c)]

    def stage_piece(p, ref, a, b):
        if p < 2:
            return rows_at(ref, (a * n + b) * unit, unit, 16)
        return ref.at[pl.ds(pl.multiple_of(a * unit_d, 16), unit_d), pl.ds(pl.multiple_of(b * unit_c, 128), unit_c)]

    def pieces_like(p, ref):
        if p < 2:
            return ref.at[pl.ds(0, (n * n - 1) * unit)]
        return ref.at[pl.ds(0, (n * n - 1) * unit_d), pl.ds(0, unit_c)]

    def on_line(p):
        plane = parts[p][4]
        return jnp.logical_and(plane[0] == 0, plane[1] == 0)

    def sent_like(late):
        count = 1 if late else 2 * n - 2
        for p, (src, _, _, _, _) in enumerate(parts):
            wait_for(src.at[pl.ds(0, count * (n * n * unit if p < 2 else n * unit_d // 2))], from_sem.at[6 * late, p])

    def hot_root():
        for copy in own:
            copy.wait()
        pl.semaphore_wait(barrier, devices - 1)
        order = [(k, half) for k in (*range(n // 2, n), 0, *range(n // 2 - 1, 0, -1)) for half in range(2)]
        for k, half in order:
            for p, (src, _, stage, _, _) in enumerate(parts):
                if k > 0 or half > 0:
                    remote(quarter(p, src, half, k), stage, from_sem.at[0 if (k, half) != order[-1] else 6, p], to_sem.at[0, p],
                           line_device(p, k, half)).start()
        for p, (src, _, stage, _, _) in enumerate(parts):
            stage[...] = quarter(p, src, 0, 0)[...]
        sent_like(0)
        signal_all()

    def hot_scatter():
        for p, (_, hot, stage, line, _) in enumerate(parts):
            @pl.when(on_line(p))
            def _(p=p, hot=hot, stage=stage, line=line):
                @pl.when(me != 0)
                def _():
                    wait_for(stage, to_sem.at[0, p])

                @pl.loop(1, n * n)
                def _(j):
                    a, b = j // n, j % n
                    remote(stage_piece(p, stage, a, b), hot_piece(p, hot, c, line, a, b), from_sem.at[1, p], to_sem.at[1, p],
                           plane_device(p, a, b)).start()
                hot_piece(p, hot, c, line, 0, 0)[...] = stage_piece(p, stage, 0, 0)[...]

    def hot_plane():
        for p, (_, hot, _, line, plane) in enumerate(parts):
            mine = hot_piece(p, hot, c, line, plane[0], plane[1])

            @pl.when(jnp.logical_not(on_line(p)))
            def _(p=p, mine=mine):
                wait_for(mine, to_sem.at[1, p])

            @pl.loop(1, n * n)
            def _(j, p=p, mine=mine, plane=plane):
                remote(mine, mine, from_sem.at[2, p], to_sem.at[2, p], plane_device(p, plane[0] + j // n, plane[1] + j % n)).start()

    def part_of_quarter(p, ref, half, k, which):
        if p < 2:
            size = n * n * unit // 2
            return rows_at(ref, half * (d_model // 2) + (2 * k + which) * size, size, 16)
        size = n * unit_d // 2
        return ref.at[pl.ds(pl.multiple_of((2 * k + which) * size, 16), size), pl.ds(pl.multiple_of(half * (d_model // 2), 128), d_model // 2)]

    def hot_line():
        for p, (_, hot, _, line, _) in enumerate(parts):
            wait_for(pieces_like(p, hot), to_sem.at[2, p])
            mine = quarter(p, hot, c, line)
            remote(mine, mine, from_sem.at[3, p], to_sem.at[3, p], line_device(p, line + 1, c)).start()
            if n > 2:
                remote(mine, mine, from_sem.at[3, p], to_sem.at[3, p], line_device(p, line + n - 1, c)).start()

    def hot_opposite():
        for p, (_, hot, _, line, _) in enumerate(parts):
            wait_for(neighbours_like(p, hot), to_sem.at[3, p])
            if n > 2:
                first = part_of_quarter(p, hot, c, (line + n - 1) % n, 0)
                second = part_of_quarter(p, hot, c, (line + 1) % n, 1)
                remote(first, first, from_sem.at[5, p], to_sem.at[5, p], line_device(p, line + 1, c)).start()
                remote(second, second, from_sem.at[5, p], to_sem.at[5, p], line_device(p, line + n - 1, c)).start()

    def neighbours_like(p, ref):
        count = min(2, n - 1)
        if p < 2:
            return ref.at[pl.ds(0, count * n * n * unit)]
        return ref.at[pl.ds(0, count * n * unit_d), pl.ds(0, d_model // 2)]

    def half_of(p, ref, half):
        if p < 2:
            return rows_at(ref, half * (d_model // 2), d_model // 2, 16)
        return ref.at[:, pl.ds(pl.multiple_of(half * (d_model // 2), 128), d_model // 2)]

    def hot_core():
        for p, (_, hot, _, _, _) in enumerate(parts):
            if n > 2:
                wait_for(quarter(p, hot, c, 0), to_sem.at[5, p])
            mine = half_of(p, hot, c)
            remote(mine, mine, from_sem.at[4, p], to_sem.at[4, p], device(mz, my, mx, c + 1)).start()

    def hot_finish():
        for p, (_, hot, _, _, _) in enumerate(parts):
            wait_for(half_of(p, hot, 1 - c), to_sem.at[4, p])
        gate = dotf(x_ref[...], hot_g[...])
        up = dotf(x_ref[...], hot_u[...])
        u = (jax.nn.silu(gate) * up).astype(BF16)
        count = hot_tok_ref.shape[1]
        same = iota((tokens, count), 0) == hot_tok_ref[...]
        weight = jnp.sum(jnp.where(same, hot_gate_ref[...], 0.0), axis=1, keepdims=True)
        is_hot = jnp.sum(jnp.where(same, 1.0, 0.0), axis=1, keepdims=True) > 0.5
        for f in range(FOLD):
            cols = slice(f * piece, (f + 1) * piece)
            h = dotf(u, hot_d[:, cols]).astype(BF16)
            acc_ref[:, cols] += jnp.where(is_hot, weight * h.astype(F32), 0.0)

    def hot_sends_done():
        @pl.when(me == 0)
        def _():
            sent_like(1)

        for p, (_, hot, _, _, _) in enumerate(parts):
            @pl.when(on_line(p))
            def _(p=p, hot=hot):
                wait_for(pieces_like(p, hot), from_sem.at[1, p])

            wait_for(pieces_like(p, hot), from_sem.at[2, p])
            wait_for(neighbours_like(p, hot), from_sem.at[3, p])
            if n > 2:
                wait_for(quarter(p, hot, c, 0), from_sem.at[5, p])
            wait_for(half_of(p, hot, c), from_sem.at[4, p])

    def expert_of(q, i):
        return peer(q, i, 1)

    def fold(pieces):
        r = iota((main, main), 0)
        return dotf(ones_where(iota((main, main), 1) == r % FOLD * blocks + r // FOLD), pieces).astype(BF16)

    def unfold(folded):
        r = iota((main, main), 0)
        return dotf(ones_where(iota((main, main), 1) == r % blocks * FOLD + r // blocks), folded).astype(BF16)

    def pick_rows(q, count, slots):
        row = iota((count, tokens), 0)
        expert = expert_of(q, row // slots)
        member = ids_ref[0:1, :] == expert
        for j in range(1, top_k):
            member = jnp.logical_or(member, ids_ref[j:j + 1, :] == expert)
        earlier = ones_where(iota((tokens, tokens), 0) < iota((tokens, tokens), 1))
        member_f = jnp.where(member, 1.0, 0.0)
        rank = dotf(member_f.astype(BF16), earlier)
        slot = (row % slots).astype(F32) if slots > 1 else float(SLOTS)
        return jnp.where(rank == slot, member_f, 0.0).astype(BF16)

    def fill(q):
        pick = pick_rows(q, main, SLOTS)
        ninth = pick_rows(q, blocks, 1)
        for f in range(FOLD):
            cols = slice(f * piece, (f + 1) * piece)
            send[q, :, :, cols] = dotf(pick, x_ref[:, cols]).astype(BF16).reshape(blocks, SLOTS, piece)
            fold_ref[f * blocks:(f + 1) * blocks] = dotf(ninth, x_ref[:, cols]).astype(BF16)
        send[q, :, :, d_model:] = fold(fold_ref[...]).reshape(blocks, FOLD, piece)

    def start_sends(q, src, dst, relay, way, s_sem, r_sem, sign):
        first = int(q == 0) if isinstance(q, int) else jnp.where(q == 0, 1, 0)
        if relayed:
            @pl.loop(0, blocks)
            def _(i):
                @pl.when(is_relayed(q, i))
                def _():
                    remote(src.at[q, i], relay.at[q, i], s_sem.at[q], mid_sem.at[way, q], hop(q, i, sign, 0)).start()

        @pl.loop(first, blocks)
        def _(i):
            def direct():
                remote(src.at[q, i], dst.at[q, i], s_sem.at[q], r_sem.at[q], peer(q, i, sign)).start()
            if relayed:
                pl.when(jnp.logical_not(is_relayed(q, i)))(direct)
            else:
                direct()

    def wait_relay(q, relay, sem):
        for count in sorted({relay_count(k) for k in range(chunks)}):
            alike = [k for k in range(chunks) if relay_count(k) == count]
            if isinstance(q, int):
                if q in alike:
                    wait_for(relay.at[q, pl.ds(0, count)], sem)
            else:
                same = functools.reduce(jnp.logical_or, [q == k for k in alike])

                @pl.when(same)
                def _(count=count):
                    wait_for(relay.at[q, pl.ds(0, count)], sem)

    def pass_on(q, dst, relay, way, r_sem, sign):
        if not relayed:
            return
        wait_relay(q, relay, mid_sem.at[way, q])

        @pl.loop(0, blocks)
        def _(i):
            @pl.when(is_relayed(q, i))
            def _():
                remote(relay.at[q, i], dst.at[q, i], on_sem.at[way, q], r_sem.at[q], hop(q, i, sign, 1)).start()

    def pass_on_sent(q):
        pass_on(q, recv, relay_out, 0, recv_sem, 1)

    def pass_on_returned(q):
        pass_on(q, back, relay_back, 1, back_sem, -1)

    def wait_chunk(q, buf, sem):
        if isinstance(q, int):
            wait_for(buf.at[0, pl.ds(1, blocks - 1)] if q == 0 else buf.at[q], sem.at[q])
            return

        @pl.when(q == 0)
        def _():
            wait_for(buf.at[0, pl.ds(1, blocks - 1)], sem.at[0])

        @pl.when(q > 0)
        def _():
            wait_for(buf.at[q], sem.at[q])

    def load_rows(q, buf):
        rows_ref[:main] = buf[q, :, :, :d_model].reshape(main, d_model)
        pieces = unfold(buf[q, :, :, d_model:].reshape(main, piece))
        for f in range(FOLD):
            rows_ref[main:, f * piece:(f + 1) * piece] = pieces[f * blocks:(f + 1) * blocks]

    def send_chunk(q):
        start_sends(q, send, recv, relay_out, 0, send_sem, recv_sem, 1)

    width = 256 if d_ff % 256 == 0 else d_ff

    def expert(q):
        with jax.named_scope("wrecv"):
            wait_chunk(q, recv, recv_sem)
        load_rows(q, recv)
        for w in range(d_ff // width):
            cols = slice(w * width, (w + 1) * width)
            gate = dotf(rows_ref[...], wg[:, cols])
            up = dotf(rows_ref[...], wu[:, cols])
            u_ref[:, cols] = (jax.nn.silu(gate) * up).astype(BF16)
        for f in range(FOLD):
            cols = slice(f * piece, (f + 1) * piece)
            res = dotf(u_ref[...], wd[:, cols]).astype(BF16)
            out[q, :, :, cols] = res[:main].reshape(blocks, SLOTS, piece)
            fold_ref[f * blocks:(f + 1) * blocks] = res[main:]
        out[q, :, :, d_model:] = fold(fold_ref[...]).reshape(blocks, FOLD, piece)

    def return_chunk(q):
        start_sends(q, out, back, relay_back, 1, ret_sem, back_sem, -1)

    def fill_weights(q):
        def weights(count, slots):
            row = iota((count, tokens), 0)
            expert = expert_of(q, row // slots)
            member = ids_ref[0:1, :] == expert
            weight = jnp.where(member, gates_ref[0:1, :], 0.0)
            for j in range(1, top_k):
                here = ids_ref[j:j + 1, :] == expert
                member = jnp.logical_or(member, here)
                weight = jnp.where(here, gates_ref[j:j + 1, :], weight)
            earlier = ones_where(iota((tokens, tokens), 0) < iota((tokens, tokens), 1))
            rank = dotf(ones_where(member), earlier)
            slot = (row % slots).astype(F32) if slots > 1 else float(SLOTS)
            return jnp.where(rank == slot, weight, 0.0)
        weight_ref[q, :, :main] = three_terms(weights(main, SLOTS).T)
        weight_ref[q, :, main:] = three_terms(weights(blocks, 1).T)

    def add_returned(q):
        with jax.named_scope("wback"):
            wait_chunk(q, back, back_sem)
        load_rows(q, back)
        for f in range(FOLD):
            cols = slice(f * piece, (f + 1) * piece)
            terms = dotf(weight_ref[q], rows_ref[:, cols])
            acc_ref[:, cols] += terms[2 * tokens:] + terms[tokens:2 * tokens] + terms[:tokens]

    def others_wait():
        for copy in own:
            copy.wait()
        pl.semaphore_wait(barrier, devices - 1)

    with jax.named_scope("fill"):
        pl.loop(0, chunks)(fill)
    recv[0, 0] = send[0, 0]
    acc_ref[...] = jnp.zeros_like(acc_ref)
    with jax.named_scope("root"):
        pl.when(me == 0)(hot_root)
    with jax.named_scope("barrier"):
        pl.when(me != 0)(others_wait)
    half = chunks // 2
    pl.loop(0, half)(send_chunk)
    with jax.named_scope("fweights"):
        pl.loop(0, chunks)(fill_weights)
    with jax.named_scope("psent0"):
        pass_on_sent(0)
    with jax.named_scope("hscatter"):
        hot_scatter()
    pl.loop(half, half + half // 2)(send_chunk)
    with jax.named_scope("psent1"):
        pass_on_sent(1)
    pl.loop(half + half // 2, chunks)(send_chunk)
    with jax.named_scope("psent23"):
        pl.loop(2, min(LEAD, chunks))(pass_on_sent)
    with jax.named_scope("hplane"):
        hot_plane()

    @pl.loop(0, chunks)
    def _(q):
        @pl.when(q < chunks - LEAD)
        def _():
            with jax.named_scope("psent"):
                pass_on_sent(q + LEAD)

        expert(q)

        @pl.when(q == 0)
        def _():
            back[0, 0] = out[0, 0]

        return_chunk(q)

        @pl.when(q >= LAG)
        def _():
            with jax.named_scope("pret"):
                pass_on_returned(q - LAG)

        @pl.when(q == chunks // 2 - 1)
        def _():
            with jax.named_scope("hline"):
                hot_line()

        @pl.when(q == chunks - 2)
        def _():
            with jax.named_scope("hopp"):
                hot_opposite()

    @pl.loop(0, LAG)
    def _(j):
        with jax.named_scope("pretlast"):
            pass_on_returned(chunks - LAG + j)
        add_returned(j)

    with jax.named_scope("hcore"):
        hot_core()
    pl.loop(LAG, chunks - 1)(add_returned)
    with jax.named_scope("hfinish"):
        hot_finish()
    add_returned(chunks - 1)
    y_ref[...] = acc_ref[...].astype(BF16)

    @pl.loop(0, chunks)
    def _(q):
        wait_chunk(q, send, send_sem)
        wait_chunk(q, out, ret_sem)
        if relayed:
            wait_relay(q, relay_out, on_sem.at[0, q])
            wait_relay(q, relay_back, on_sem.at[1, q])
    with jax.named_scope("hsend"):
        hot_sends_done()


def solution(mesh):
    group_size = mesh.shape['ep']
    n = 1
    while 2 * n * n * n < group_size:
        n += 1
    row_spec = P(('dp', 'ep'), None)
    list_spec = P(('dp', 'ep'))
    expert_spec = P('ep', None, None)

    def local_layer(x, ids, gates, hot_tok, hot_gates, wg, wu, wd):
        wg, wu, wd = wg[0], wu[0], wd[0]
        tokens, d_model = x.shape
        d_ff = wg.shape[1]
        chunks = SPLIT * n
        blocks = 2 * n * n // SPLIT
        piece = d_model // FOLD
        main = blocks * SLOTS
        block_buf = pltpu.VMEM((chunks, blocks, SLOTS, d_model + piece), BF16)
        in_vmem = pl.BlockSpec(memory_space=pltpu.VMEM)
        in_hbm = pl.BlockSpec(memory_space=pl.ANY)
        dma = pltpu.SemaphoreType.DMA
        weights = [pltpu.VMEM((d_model, d_ff), BF16)] * 2 + [pltpu.VMEM((d_ff, d_model), BF16)]
        return pl.pallas_call(
            functools.partial(layer_kernel, n),
            out_shape=jax.ShapeDtypeStruct((tokens, d_model), BF16),
            in_specs=[in_vmem] * 5 + [in_hbm] * 3,
            out_specs=in_vmem,
            scratch_shapes=[block_buf] * 6 + weights + weights
            + [pltpu.VMEM((d_model // (2 * n), d_ff), BF16)] * 2 + [pltpu.VMEM((d_ff // n, d_model // 2), BF16)]
            + [pltpu.VMEM((main + blocks, d_model), BF16), pltpu.VMEM((main + blocks, d_ff), BF16),
               pltpu.VMEM((main, piece), BF16), pltpu.VMEM((chunks, 3 * tokens, main + blocks), BF16), pltpu.VMEM((tokens, d_model), F32)]
            + [dma((3,))] + [dma((chunks,))] * 4 + [dma((2, chunks))] * 2 + [dma((7, 3)), dma((6, 3))],
            compiler_params=pltpu.CompilerParams(vmem_limit_bytes=VMEM_LIMIT, collective_id=0, has_side_effects=True),
            name="moe_layer",
        )(ids.T, gates.T, hot_tok[None, :], hot_gates[None, :], x, wg, wu, wd)

    return jax.shard_map(local_layer, mesh=mesh,
                         in_specs=(row_spec, row_spec, row_spec, list_spec, list_spec, expert_spec, expert_spec, expert_spec),
                         out_specs=row_spec, check_vma=False)
```

```python
import functools

import jax
import jax.numpy as jnp
from jax import lax
from jax.experimental import pallas as pl
from jax.experimental.pallas import tpu as pltpu
from jax.sharding import PartitionSpec as P

F32 = jnp.float32
BF16 = jnp.bfloat16
SLOTS = 8
FOLD = 8
VMEM_LIMIT = 60 * 1024 * 1024
SPLIT = 2
LEAD = 4
LAG = 6


def dotf(a, b):
    return jnp.dot(a, b, preferred_element_type=F32)


def iota(shape, dim):
    return lax.broadcasted_iota(jnp.int32, shape, dim)


def ones_where(mask):
    return jnp.where(mask, 1.0, 0.0).astype(BF16)


def three_terms(a):
    hi = a.astype(BF16)
    rest = a - hi.astype(F32)
    mid = rest.astype(BF16)
    low = (rest - mid.astype(F32)).astype(BF16)
    return jnp.concatenate([hi, mid, low], axis=0)


def layer_kernel(n, ids_ref, gates_ref, hot_tok_ref, hot_gate_ref, x_ref, wg_ref, wu_ref, wd_ref, y_ref,
                 send, recv, out, back, relay_out, relay_back, wg, wu, wd, hot_g, hot_u, hot_d, stage_g, stage_u, stage_d,
                 rows_ref, u_ref, fold_ref, weight_ref, acc_ref,
                 load_sem, send_sem, recv_sem, ret_sem, back_sem, mid_sem, on_sem, from_sem, to_sem):
    me = lax.axis_index('ep')
    devices = 2 * n * n * n
    c, mx, my, mz = me % 2, (me // 2) % n, (me // (2 * n)) % n, me // (2 * n * n)
    chunks = SPLIT * n
    blocks = 2 * n * n // SPLIT
    tokens, d_model = x_ref.shape
    d_ff = wd_ref.shape[0]
    top_k = ids_ref.shape[0]
    piece = d_model // FOLD
    main = blocks * SLOTS
    chunk_rows = main + blocks

    def device(z, y, x, core):
        return ((z % n * n + y % n) * n + x % n) * 2 + core % 2

    def steps(q, i):
        kx, ky = (i // 2) % n, i // (2 * n) * SPLIT + q % SPLIT
        return i % 2, kx, ky, (q // SPLIT + 2 * n - kx - ky) % n

    def peer(q, i, sign):
        kc, kx, ky, kz = steps(q, i)
        if sign > 0:
            return device(mz + kz, my + ky, mx + kx, c + kc)
        return device(mz + n - kz, my + n - ky, mx + n - kx, c + kc)

    relayed = n == 4

    def opposite(k):
        return k == n // 2

    def is_relayed(q, i):
        _, kx, ky, kz = steps(q, i)
        return jnp.logical_or(jnp.logical_or(opposite(kx), opposite(ky)), opposite(kz))

    def relay_count(q):
        return sum(any(opposite(k) for k in steps(q, i)[1:]) for i in range(blocks))

    def hop(q, i, sign, leg):
        kc, kx, ky, kz = steps(q, i)
        way = jnp.where(kc == 0, 1, n - 1)
        move = [jnp.where(opposite(k), way, k if leg == 0 else 0) for k in (kz, ky, kx)]
        if sign < 0:
            move = [n - m for m in move]
        return device(mz + move[0], my + move[1], mx + move[2], c + kc if leg == 0 else c)

    def remote(src, dst, s_sem, r_sem, to):
        return pltpu.make_async_remote_copy(src_ref=src, dst_ref=dst, send_sem=s_sem, recv_sem=r_sem, device_id={'ep': to},
                                            device_id_type=pl.DeviceIdType.MESH)

    def wait_for(ref, sem):
        pltpu.make_async_copy(ref, ref, sem).wait()

    def rows_at(ref, start, size, unit):
        return ref.at[pl.ds(pl.multiple_of(start, unit), size)]

    barrier = pltpu.get_barrier_semaphore()

    def signal_all():
        @pl.loop(1, devices)
        def _(i):
            pl.semaphore_signal(barrier, inc=1, device_id={'ep': (me + i) % devices}, device_id_type=pl.DeviceIdType.MESH)

    pl.when(me != 0)(signal_all)

    own = [pltpu.make_async_copy(src, dst, load_sem.at[p])
           for p, (src, dst) in enumerate(((wg_ref, wg), (wu_ref, wu), (wd_ref, wd)))]
    for copy in own:
        copy.start()

    unit = d_model // (2 * n * n * n)
    unit_d, unit_c = d_ff // (n * n), d_model // (2 * n)
    parts = ((wg, hot_g, stage_g, mz, (my, mx)), (wu, hot_u, stage_u, mx, (mz, my)), (wd, hot_d, stage_d, my, (mx, mz)))

    def line_device(p, k, core):
        return (device(k, my, mx, core), device(mz, my, k, core), device(mz, k, mx, core))[p]

    def plane_device(p, a, b):
        return (device(mz, a, b, c), device(a, b, mx, c), device(b, my, a, c))[p]

    def quarter(p, ref, half, k):
        if p < 2:
            size = n * n * unit
            return rows_at(ref, half * (d_model // 2) + k * size, size, 16)
        size = n * unit_d
        return ref.at[pl.ds(pl.multiple_of(k * size, 16), size), pl.ds(pl.multiple_of(half * (d_model // 2), 128), d_model // 2)]

    def hot_piece(p, ref, half, k, a, b):
        if p < 2:
            return rows_at(ref, half * (d_model // 2) + k * (n * n * unit) + (a * n + b) * unit, unit, 16)
        return ref.at[pl.ds(pl.multiple_of(k * (n * unit_d) + a * unit_d, 16), unit_d),
                      pl.ds(pl.multiple_of(half * (d_model // 2) + b * unit_c, 128), unit_c)]

    def stage_piece(p, ref, a, b):
        if p < 2:
            return rows_at(ref, (a * n + b) * unit, unit, 16)
        return ref.at[pl.ds(pl.multiple_of(a * unit_d, 16), unit_d), pl.ds(pl.multiple_of(b * unit_c, 128), unit_c)]

    def pieces_like(p, ref):
        if p < 2:
            return ref.at[pl.ds(0, (n * n - 1) * unit)]
        return ref.at[pl.ds(0, (n * n - 1) * unit_d), pl.ds(0, unit_c)]

    def on_line(p):
        plane = parts[p][4]
        return jnp.logical_and(plane[0] == 0, plane[1] == 0)

    def sent_like(late):
        count = 1 if late else 2 * n - 2
        for p, (src, _, _, _, _) in enumerate(parts):
            wait_for(src.at[pl.ds(0, count * (n * n * unit if p < 2 else n * unit_d // 2))], from_sem.at[6 * late, p])

    def hot_root():
        for copy in own:
            copy.wait()
        pl.semaphore_wait(barrier, devices - 1)
        order = [(k, half) for k in (*range(n // 2, n), 0, *range(n // 2 - 1, 0, -1)) for half in range(2)]
        for k, half in order:
            for p, (src, _, stage, _, _) in enumerate(parts):
                if k > 0 or half > 0:
                    remote(quarter(p, src, half, k), stage, from_sem.at[0 if (k, half) != order[-1] else 6, p], to_sem.at[0, p],
                           line_device(p, k, half)).start()
        for p, (src, _, stage, _, _) in enumerate(parts):
            stage[...] = quarter(p, src, 0, 0)[...]
        sent_like(0)
        signal_all()

    def hot_scatter():
        for p, (_, hot, stage, line, _) in enumerate(parts):
            @pl.when(on_line(p))
            def _(p=p, hot=hot, stage=stage, line=line):
                @pl.when(me != 0)
                def _():
                    wait_for(stage, to_sem.at[0, p])

                @pl.loop(1, n * n)
                def _(j):
                    a, b = j // n, j % n
                    remote(stage_piece(p, stage, a, b), hot_piece(p, hot, c, line, a, b), from_sem.at[1, p], to_sem.at[1, p],
                           plane_device(p, a, b)).start()
                hot_piece(p, hot, c, line, 0, 0)[...] = stage_piece(p, stage, 0, 0)[...]

    def hot_plane():
        for p, (_, hot, _, line, plane) in enumerate(parts):
            mine = hot_piece(p, hot, c, line, plane[0], plane[1])

            @pl.when(jnp.logical_not(on_line(p)))
            def _(p=p, mine=mine):
                wait_for(mine, to_sem.at[1, p])

            @pl.loop(1, n * n)
            def _(j, p=p, mine=mine, plane=plane):
                remote(mine, mine, from_sem.at[2, p], to_sem.at[2, p], plane_device(p, plane[0] + j // n, plane[1] + j % n)).start()

    def part_of_quarter(p, ref, half, k, which):
        if p < 2:
            size = n * n * unit // 2
            return rows_at(ref, half * (d_model // 2) + (2 * k + which) * size, size, 16)
        size = n * unit_d // 2
        return ref.at[pl.ds(pl.multiple_of((2 * k + which) * size, 16), size), pl.ds(pl.multiple_of(half * (d_model // 2), 128), d_model // 2)]

    def hot_line():
        for p, (_, hot, _, line, _) in enumerate(parts):
            wait_for(pieces_like(p, hot), to_sem.at[2, p])
            mine = quarter(p, hot, c, line)
            remote(mine, mine, from_sem.at[3, p], to_sem.at[3, p], line_device(p, line + 1, c)).start()
            if n > 2:
                remote(mine, mine, from_sem.at[3, p], to_sem.at[3, p], line_device(p, line + n - 1, c)).start()

    def hot_opposite():
        for p, (_, hot, _, line, _) in enumerate(parts):
            wait_for(neighbours_like(p, hot), to_sem.at[3, p])
            if n > 2:
                first = part_of_quarter(p, hot, c, (line + n - 1) % n, 0)
                second = part_of_quarter(p, hot, c, (line + 1) % n, 1)
                remote(first, first, from_sem.at[5, p], to_sem.at[5, p], line_device(p, line + 1, c)).start()
                remote(second, second, from_sem.at[5, p], to_sem.at[5, p], line_device(p, line + n - 1, c)).start()

    def neighbours_like(p, ref):
        count = min(2, n - 1)
        if p < 2:
            return ref.at[pl.ds(0, count * n * n * unit)]
        return ref.at[pl.ds(0, count * n * unit_d), pl.ds(0, d_model // 2)]

    def half_of(p, ref, half):
        if p < 2:
            return rows_at(ref, half * (d_model // 2), d_model // 2, 16)
        return ref.at[:, pl.ds(pl.multiple_of(half * (d_model // 2), 128), d_model // 2)]

    def hot_core():
        for p, (_, hot, _, _, _) in enumerate(parts):
            if n > 2:
                wait_for(quarter(p, hot, c, 0), to_sem.at[5, p])
            mine = half_of(p, hot, c)
            remote(mine, mine, from_sem.at[4, p], to_sem.at[4, p], device(mz, my, mx, c + 1)).start()

    def hot_finish():
        for p, (_, hot, _, _, _) in enumerate(parts):
            wait_for(half_of(p, hot, 1 - c), to_sem.at[4, p])
        gate = dotf(x_ref[...], hot_g[...])
        up = dotf(x_ref[...], hot_u[...])
        u = (jax.nn.silu(gate) * up).astype(BF16)
        count = hot_tok_ref.shape[1]
        same = iota((tokens, count), 0) == hot_tok_ref[...]
        weight = jnp.sum(jnp.where(same, hot_gate_ref[...], 0.0), axis=1, keepdims=True)
        is_hot = jnp.sum(jnp.where(same, 1.0, 0.0), axis=1, keepdims=True) > 0.5
        for f in range(FOLD):
            cols = slice(f * piece, (f + 1) * piece)
            h = dotf(u, hot_d[:, cols]).astype(BF16)
            acc_ref[:, cols] += jnp.where(is_hot, weight * h.astype(F32), 0.0)

    def hot_sends_done():
        @pl.when(me == 0)
        def _():
            sent_like(1)

        for p, (_, hot, _, _, _) in enumerate(parts):
            @pl.when(on_line(p))
            def _(p=p, hot=hot):
                wait_for(pieces_like(p, hot), from_sem.at[1, p])

            wait_for(pieces_like(p, hot), from_sem.at[2, p])
            wait_for(neighbours_like(p, hot), from_sem.at[3, p])
            if n > 2:
                wait_for(quarter(p, hot, c, 0), from_sem.at[5, p])
            wait_for(half_of(p, hot, c), from_sem.at[4, p])

    def expert_of(q, i):
        return peer(q, i, 1)

    def fold(pieces):
        r = iota((main, main), 0)
        return dotf(ones_where(iota((main, main), 1) == r % FOLD * blocks + r // FOLD), pieces).astype(BF16)

    def unfold(folded):
        r = iota((main, main), 0)
        return dotf(ones_where(iota((main, main), 1) == r % blocks * FOLD + r // blocks), folded).astype(BF16)

    def pick_rows(q, count, slots):
        row = iota((count, tokens), 0)
        expert = expert_of(q, row // slots)
        member = ids_ref[0:1, :] == expert
        for j in range(1, top_k):
            member = jnp.logical_or(member, ids_ref[j:j + 1, :] == expert)
        earlier = ones_where(iota((tokens, tokens), 0) < iota((tokens, tokens), 1))
        member_f = jnp.where(member, 1.0, 0.0)
        rank = dotf(member_f.astype(BF16), earlier)
        slot = (row % slots).astype(F32) if slots > 1 else float(SLOTS)
        return jnp.where(rank == slot, member_f, 0.0).astype(BF16)

    def fill(q):
        pick = pick_rows(q, main, SLOTS)
        ninth = pick_rows(q, blocks, 1)
        for f in range(FOLD):
            cols = slice(f * piece, (f + 1) * piece)
            send[q, :, :, cols] = dotf(pick, x_ref[:, cols]).astype(BF16).reshape(blocks, SLOTS, piece)
            fold_ref[f * blocks:(f + 1) * blocks] = dotf(ninth, x_ref[:, cols]).astype(BF16)
        send[q, :, :, d_model:] = fold(fold_ref[...]).reshape(blocks, FOLD, piece)

    def start_sends(q, src, dst, relay, way, s_sem, r_sem, sign):
        first = int(q == 0) if isinstance(q, int) else jnp.where(q == 0, 1, 0)
        if relayed:
            @pl.loop(0, blocks)
            def _(i):
                @pl.when(is_relayed(q, i))
                def _():
                    remote(src.at[q, i], relay.at[q, i], s_sem.at[q], mid_sem.at[way, q], hop(q, i, sign, 0)).start()

        @pl.loop(first, blocks)
        def _(i):
            def direct():
                remote(src.at[q, i], dst.at[q, i], s_sem.at[q], r_sem.at[q], peer(q, i, sign)).start()
            if relayed:
                pl.when(jnp.logical_not(is_relayed(q, i)))(direct)
            else:
                direct()

    def wait_relay(q, relay, sem):
        for count in sorted({relay_count(k) for k in range(chunks)}):
            alike = [k for k in range(chunks) if relay_count(k) == count]
            if isinstance(q, int):
                if q in alike:
                    wait_for(relay.at[q, pl.ds(0, count)], sem)
            else:
                same = functools.reduce(jnp.logical_or, [q == k for k in alike])

                @pl.when(same)
                def _(count=count):
                    wait_for(relay.at[q, pl.ds(0, count)], sem)

    def pass_on(q, dst, relay, way, r_sem, sign):
        if not relayed:
            return
        wait_relay(q, relay, mid_sem.at[way, q])

        @pl.loop(0, blocks)
        def _(i):
            @pl.when(is_relayed(q, i))
            def _():
                remote(relay.at[q, i], dst.at[q, i], on_sem.at[way, q], r_sem.at[q], hop(q, i, sign, 1)).start()

    def pass_on_sent(q):
        pass_on(q, recv, relay_out, 0, recv_sem, 1)

    def pass_on_returned(q):
        pass_on(q, back, relay_back, 1, back_sem, -1)

    def wait_chunk(q, buf, sem):
        if isinstance(q, int):
            wait_for(buf.at[0, pl.ds(1, blocks - 1)] if q == 0 else buf.at[q], sem.at[q])
            return

        @pl.when(q == 0)
        def _():
            wait_for(buf.at[0, pl.ds(1, blocks - 1)], sem.at[0])

        @pl.when(q > 0)
        def _():
            wait_for(buf.at[q], sem.at[q])

    def load_rows(q, buf):
        rows_ref[:main] = buf[q, :, :, :d_model].reshape(main, d_model)
        pieces = unfold(buf[q, :, :, d_model:].reshape(main, piece))
        for f in range(FOLD):
            rows_ref[main:, f * piece:(f + 1) * piece] = pieces[f * blocks:(f + 1) * blocks]

    def send_chunk(q):
        start_sends(q, send, recv, relay_out, 0, send_sem, recv_sem, 1)

    width = 256 if d_ff % 256 == 0 else d_ff

    def expert(q):
        with jax.named_scope("wrecv"):
            wait_chunk(q, recv, recv_sem)
        load_rows(q, recv)
        for w in range(d_ff // width):
            cols = slice(w * width, (w + 1) * width)
            gate = dotf(rows_ref[...], wg[:, cols])
            up = dotf(rows_ref[...], wu[:, cols])
            u_ref[:, cols] = (jax.nn.silu(gate) * up).astype(BF16)
        for f in range(FOLD):
            cols = slice(f * piece, (f + 1) * piece)
            res = dotf(u_ref[...], wd[:, cols]).astype(BF16)
            out[q, :, :, cols] = res[:main].reshape(blocks, SLOTS, piece)
            fold_ref[f * blocks:(f + 1) * blocks] = res[main:]
        out[q, :, :, d_model:] = fold(fold_ref[...]).reshape(blocks, FOLD, piece)

    def return_chunk(q):
        start_sends(q, out, back, relay_back, 1, ret_sem, back_sem, -1)

    def fill_weights(q):
        def weights(count, slots):
            row = iota((count, tokens), 0)
            expert = expert_of(q, row // slots)
            member = ids_ref[0:1, :] == expert
            weight = jnp.where(member, gates_ref[0:1, :], 0.0)
            for j in range(1, top_k):
                here = ids_ref[j:j + 1, :] == expert
                member = jnp.logical_or(member, here)
                weight = jnp.where(here, gates_ref[j:j + 1, :], weight)
            earlier = ones_where(iota((tokens, tokens), 0) < iota((tokens, tokens), 1))
            rank = dotf(ones_where(member), earlier)
            slot = (row % slots).astype(F32) if slots > 1 else float(SLOTS)
            return jnp.where(rank == slot, weight, 0.0)
        weight_ref[q, :, :main] = three_terms(weights(main, SLOTS).T)
        weight_ref[q, :, main:] = three_terms(weights(blocks, 1).T)

    def add_returned(q):
        with jax.named_scope("wback"):
            wait_chunk(q, back, back_sem)
        load_rows(q, back)
        for f in range(FOLD):
            cols = slice(f * piece, (f + 1) * piece)
            terms = dotf(weight_ref[q], rows_ref[:, cols])
            acc_ref[:, cols] += terms[2 * tokens:] + terms[tokens:2 * tokens] + terms[:tokens]

    def others_wait():
        for copy in own:
            copy.wait()
        pl.semaphore_wait(barrier, devices - 1)

    with jax.named_scope("fill"):
        pl.loop(0, chunks)(fill)
    recv[0, 0] = send[0, 0]
    acc_ref[...] = jnp.zeros_like(acc_ref)
    with jax.named_scope("root"):
        pl.when(me == 0)(hot_root)
    with jax.named_scope("barrier"):
        pl.when(me != 0)(others_wait)
    half = chunks // 2
    pl.loop(0, half)(send_chunk)
    with jax.named_scope("fweights"):
        pl.loop(0, chunks)(fill_weights)
    with jax.named_scope("psent0"):
        pass_on_sent(0)
    with jax.named_scope("hscatter"):
        hot_scatter()
    pl.loop(half, half + half // 2)(send_chunk)
    with jax.named_scope("psent1"):
        pass_on_sent(1)
    pl.loop(half + half // 2, chunks)(send_chunk)
    with jax.named_scope("psent23"):
        pl.loop(2, min(LEAD, chunks))(pass_on_sent)
    with jax.named_scope("hplane"):
        hot_plane()

    @pl.loop(0, chunks)
    def _(q):
        @pl.when(q < chunks - LEAD)
        def _():
            with jax.named_scope("psent"):
                pass_on_sent(q + LEAD)

        expert(q)

        @pl.when(q == 0)
        def _():
            back[0, 0] = out[0, 0]

        return_chunk(q)

        @pl.when(q >= min(LAG, chunks))
        def _():
            with jax.named_scope("pret"):
                pass_on_returned(q - min(LAG, chunks))

        @pl.when(q == 2)
        def _():
            with jax.named_scope("hline"):
                hot_line()

    lag = min(LAG, chunks)

    @pl.loop(0, lag)
    def _(j):
        with jax.named_scope("pretlast"):
            pass_on_returned(chunks - lag + j)

        @pl.when(j == lag // 3)
        def _():
            with jax.named_scope("hopp"):
                hot_opposite()

        @pl.when(j >= lag // 2)
        def _():
            add_returned(j - lag // 2)

    pl.loop(lag - lag // 2, chunks // 2)(add_returned)
    with jax.named_scope("hcore"):
        hot_core()
    pl.loop(chunks // 2, chunks - 1)(add_returned)
    with jax.named_scope("hfinish"):
        hot_finish()
    add_returned(chunks - 1)
    y_ref[...] = acc_ref[...].astype(BF16)

    @pl.loop(0, chunks)
    def _(q):
        wait_chunk(q, send, send_sem)
        wait_chunk(q, out, ret_sem)
        if relayed:
            wait_relay(q, relay_out, on_sem.at[0, q])
            wait_relay(q, relay_back, on_sem.at[1, q])
    with jax.named_scope("hsend"):
        hot_sends_done()


def solution(mesh):
    group_size = mesh.shape['ep']
    n = 1
    while 2 * n * n * n < group_size:
        n += 1
    row_spec = P(('dp', 'ep'), None)
    list_spec = P(('dp', 'ep'))
    expert_spec = P('ep', None, None)

    def local_layer(x, ids, gates, hot_tok, hot_gates, wg, wu, wd):
        wg, wu, wd = wg[0], wu[0], wd[0]
        tokens, d_model = x.shape
        d_ff = wg.shape[1]
        chunks = SPLIT * n
        blocks = 2 * n * n // SPLIT
        piece = d_model // FOLD
        main = blocks * SLOTS
        block_buf = pltpu.VMEM((chunks, blocks, SLOTS, d_model + piece), BF16)
        in_vmem = pl.BlockSpec(memory_space=pltpu.VMEM)
        in_hbm = pl.BlockSpec(memory_space=pl.ANY)
        dma = pltpu.SemaphoreType.DMA
        weights = [pltpu.VMEM((d_model, d_ff), BF16)] * 2 + [pltpu.VMEM((d_ff, d_model), BF16)]
        return pl.pallas_call(
            functools.partial(layer_kernel, n),
            out_shape=jax.ShapeDtypeStruct((tokens, d_model), BF16),
            in_specs=[in_vmem] * 5 + [in_hbm] * 3,
            out_specs=in_vmem,
            scratch_shapes=[block_buf] * 6 + weights + weights
            + [pltpu.VMEM((d_model // (2 * n), d_ff), BF16)] * 2 + [pltpu.VMEM((d_ff // n, d_model // 2), BF16)]
            + [pltpu.VMEM((main + blocks, d_model), BF16), pltpu.VMEM((main + blocks, d_ff), BF16),
               pltpu.VMEM((main, piece), BF16), pltpu.VMEM((chunks, 3 * tokens, main + blocks), BF16), pltpu.VMEM((tokens, d_model), F32)]
            + [dma((3,))] + [dma((chunks,))] * 4 + [dma((2, chunks))] * 2 + [dma((7, 3)), dma((6, 3))],
            compiler_params=pltpu.CompilerParams(vmem_limit_bytes=VMEM_LIMIT, collective_id=0, has_side_effects=True),
            name="moe_layer",
        )(ids.T, gates.T, hot_tok[None, :], hot_gates[None, :], x, wg, wu, wd)

    return jax.shard_map(local_layer, mesh=mesh,
                         in_specs=(row_spec, row_spec, row_spec, list_spec, list_spec, expert_spec, expert_spec, expert_spec),
                         out_specs=row_spec, check_vma=False)
```

```python
import functools

import jax
import jax.numpy as jnp
from jax import lax
from jax.experimental import pallas as pl
from jax.experimental.pallas import tpu as pltpu
from jax.sharding import PartitionSpec as P

F32 = jnp.float32
BF16 = jnp.bfloat16
SLOTS = 8
FOLD = 8
VMEM_LIMIT = 60 * 1024 * 1024
SPLIT = 2
LEAD = 4
LAG = 6


def dotf(a, b):
    return jnp.dot(a, b, preferred_element_type=F32)


def iota(shape, dim):
    return lax.broadcasted_iota(jnp.int32, shape, dim)


def ones_where(mask):
    return jnp.where(mask, 1.0, 0.0).astype(BF16)


def three_terms(a):
    hi = a.astype(BF16)
    rest = a - hi.astype(F32)
    mid = rest.astype(BF16)
    low = (rest - mid.astype(F32)).astype(BF16)
    return jnp.concatenate([hi, mid, low], axis=0)


def layer_kernel(n, ids_ref, gates_ref, hot_tok_ref, hot_gate_ref, x_ref, wg_ref, wu_ref, wd_ref, y_ref,
                 send, recv, out, back, relay_out, relay_back, wg, wu, wd, hot_g, hot_u, hot_d, stage_g, stage_u, stage_d,
                 rows_ref, u_ref, fold_ref, weight_ref, acc_ref,
                 load_sem, send_sem, recv_sem, ret_sem, back_sem, mid_sem, on_sem, from_sem, to_sem):
    me = lax.axis_index('ep')
    devices = 2 * n * n * n
    c, mx, my, mz = me % 2, (me // 2) % n, (me // (2 * n)) % n, me // (2 * n * n)
    chunks = SPLIT * n
    blocks = 2 * n * n // SPLIT
    tokens, d_model = x_ref.shape
    d_ff = wd_ref.shape[0]
    top_k = ids_ref.shape[0]
    piece = d_model // FOLD
    main = blocks * SLOTS
    chunk_rows = main + blocks

    def device(z, y, x, core):
        return ((z % n * n + y % n) * n + x % n) * 2 + core % 2

    def steps(q, i):
        kx, ky = (i // 2) % n, i // (2 * n) * SPLIT + q % SPLIT
        return i % 2, kx, ky, (q // SPLIT + 2 * n - kx - ky) % n

    def peer(q, i, sign):
        kc, kx, ky, kz = steps(q, i)
        if sign > 0:
            return device(mz + kz, my + ky, mx + kx, c + kc)
        return device(mz + n - kz, my + n - ky, mx + n - kx, c + kc)

    relayed = n == 4

    def opposite(k):
        return k == n // 2

    def is_relayed(q, i):
        _, kx, ky, kz = steps(q, i)
        return jnp.logical_or(jnp.logical_or(opposite(kx), opposite(ky)), opposite(kz))

    def relay_count(q):
        return sum(any(opposite(k) for k in steps(q, i)[1:]) for i in range(blocks))

    def hop(q, i, sign, leg):
        kc, kx, ky, kz = steps(q, i)
        way = jnp.where(kc == 0, 1, n - 1)
        move = [jnp.where(opposite(k), way, k if leg == 0 else 0) for k in (kz, ky, kx)]
        if sign < 0:
            move = [n - m for m in move]
        return device(mz + move[0], my + move[1], mx + move[2], c + kc if leg == 0 else c)

    def remote(src, dst, s_sem, r_sem, to):
        return pltpu.make_async_remote_copy(src_ref=src, dst_ref=dst, send_sem=s_sem, recv_sem=r_sem, device_id={'ep': to},
                                            device_id_type=pl.DeviceIdType.MESH)

    def wait_for(ref, sem):
        pltpu.make_async_copy(ref, ref, sem).wait()

    def rows_at(ref, start, size, unit):
        return ref.at[pl.ds(pl.multiple_of(start, unit), size)]

    barrier = pltpu.get_barrier_semaphore()

    def signal_all():
        @pl.loop(1, devices)
        def _(i):
            pl.semaphore_signal(barrier, inc=1, device_id={'ep': (me + i) % devices}, device_id_type=pl.DeviceIdType.MESH)

    pl.when(me != 0)(signal_all)

    own = [pltpu.make_async_copy(src, dst, load_sem.at[p])
           for p, (src, dst) in enumerate(((wg_ref, wg), (wu_ref, wu), (wd_ref, wd)))]
    for copy in own:
        copy.start()

    unit = d_model // (2 * n * n * n)
    unit_d, unit_c = d_ff // (n * n), d_model // (2 * n)
    parts = ((wg, hot_g, stage_g, mz, (my, mx)), (wu, hot_u, stage_u, mx, (mz, my)), (wd, hot_d, stage_d, my, (mx, mz)))

    def line_device(p, k, core):
        return (device(k, my, mx, core), device(mz, my, k, core), device(mz, k, mx, core))[p]

    def plane_device(p, a, b):
        return (device(mz, a, b, c), device(a, b, mx, c), device(b, my, a, c))[p]

    def quarter(p, ref, half, k):
        if p < 2:
            size = n * n * unit
            return rows_at(ref, half * (d_model // 2) + k * size, size, 16)
        size = n * unit_d
        return ref.at[pl.ds(pl.multiple_of(k * size, 16), size), pl.ds(pl.multiple_of(half * (d_model // 2), 128), d_model // 2)]

    def hot_piece(p, ref, half, k, a, b):
        if p < 2:
            return rows_at(ref, half * (d_model // 2) + k * (n * n * unit) + (a * n + b) * unit, unit, 16)
        return ref.at[pl.ds(pl.multiple_of(k * (n * unit_d) + a * unit_d, 16), unit_d),
                      pl.ds(pl.multiple_of(half * (d_model // 2) + b * unit_c, 128), unit_c)]

    def stage_piece(p, ref, a, b):
        if p < 2:
            return rows_at(ref, (a * n + b) * unit, unit, 16)
        return ref.at[pl.ds(pl.multiple_of(a * unit_d, 16), unit_d), pl.ds(pl.multiple_of(b * unit_c, 128), unit_c)]

    def pieces_like(p, ref):
        if p < 2:
            return ref.at[pl.ds(0, (n * n - 1) * unit)]
        return ref.at[pl.ds(0, (n * n - 1) * unit_d), pl.ds(0, unit_c)]

    def on_line(p):
        plane = parts[p][4]
        return jnp.logical_and(plane[0] == 0, plane[1] == 0)

    def sent_like(late):
        count = 1 if late else 2 * n - 2
        for p, (src, _, _, _, _) in enumerate(parts):
            wait_for(src.at[pl.ds(0, count * (n * n * unit if p < 2 else n * unit_d // 2))], from_sem.at[6 * late, p])

    def hot_root():
        for copy in own:
            copy.wait()
        pl.semaphore_wait(barrier, devices - 1)
        order = [(k, half) for k in (*range(n // 2, n), 0, *range(n // 2 - 1, 0, -1)) for half in range(2)]
        for k, half in order:
            for p, (src, _, stage, _, _) in enumerate(parts):
                if k > 0 or half > 0:
                    remote(quarter(p, src, half, k), stage, from_sem.at[0 if (k, half) != order[-1] else 6, p], to_sem.at[0, p],
                           line_device(p, k, half)).start()
        for p, (src, _, stage, _, _) in enumerate(parts):
            stage[...] = quarter(p, src, 0, 0)[...]
        sent_like(0)
        signal_all()

    def hot_scatter():
        for p, (_, hot, stage, line, _) in enumerate(parts):
            @pl.when(on_line(p))
            def _(p=p, hot=hot, stage=stage, line=line):
                @pl.when(me != 0)
                def _():
                    wait_for(stage, to_sem.at[0, p])

                @pl.loop(1, n * n)
                def _(j):
                    a, b = j // n, j % n
                    remote(stage_piece(p, stage, a, b), hot_piece(p, hot, c, line, a, b), from_sem.at[1, p], to_sem.at[1, p],
                           plane_device(p, a, b)).start()
                hot_piece(p, hot, c, line, 0, 0)[...] = stage_piece(p, stage, 0, 0)[...]

    def hot_plane():
        for p, (_, hot, _, line, plane) in enumerate(parts):
            mine = hot_piece(p, hot, c, line, plane[0], plane[1])

            @pl.when(jnp.logical_not(on_line(p)))
            def _(p=p, mine=mine):
                wait_for(mine, to_sem.at[1, p])

            @pl.loop(1, n * n)
            def _(j, p=p, mine=mine, plane=plane):
                remote(mine, mine, from_sem.at[2, p], to_sem.at[2, p], plane_device(p, plane[0] + j // n, plane[1] + j % n)).start()

    def part_of_quarter(p, ref, half, k, which):
        if p < 2:
            size = n * n * unit // 2
            return rows_at(ref, half * (d_model // 2) + (2 * k + which) * size, size, 16)
        size = n * unit_d // 2
        return ref.at[pl.ds(pl.multiple_of((2 * k + which) * size, 16), size), pl.ds(pl.multiple_of(half * (d_model // 2), 128), d_model // 2)]

    def hot_line():
        for p, (_, hot, _, line, _) in enumerate(parts):
            wait_for(pieces_like(p, hot), to_sem.at[2, p])
            mine = quarter(p, hot, c, line)
            remote(mine, mine, from_sem.at[3, p], to_sem.at[3, p], line_device(p, line + 1, c)).start()
            if n > 2:
                remote(mine, mine, from_sem.at[3, p], to_sem.at[3, p], line_device(p, line + n - 1, c)).start()

    def hot_opposite():
        for p, (_, hot, _, line, _) in enumerate(parts):
            wait_for(neighbours_like(p, hot), to_sem.at[3, p])
            if n > 2:
                first = part_of_quarter(p, hot, c, (line + n - 1) % n, 0)
                second = part_of_quarter(p, hot, c, (line + 1) % n, 1)
                remote(first, first, from_sem.at[5, p], to_sem.at[5, p], line_device(p, line + 1, c)).start()
                remote(second, second, from_sem.at[5, p], to_sem.at[5, p], line_device(p, line + n - 1, c)).start()

    def neighbours_like(p, ref):
        count = min(2, n - 1)
        if p < 2:
            return ref.at[pl.ds(0, count * n * n * unit)]
        return ref.at[pl.ds(0, count * n * unit_d), pl.ds(0, d_model // 2)]

    def half_of(p, ref, half):
        if p < 2:
            return rows_at(ref, half * (d_model // 2), d_model // 2, 16)
        return ref.at[:, pl.ds(pl.multiple_of(half * (d_model // 2), 128), d_model // 2)]

    def hot_core():
        for p, (_, hot, _, _, _) in enumerate(parts):
            if n > 2:
                wait_for(quarter(p, hot, c, 0), to_sem.at[5, p])
            mine = half_of(p, hot, c)
            remote(mine, mine, from_sem.at[4, p], to_sem.at[4, p], device(mz, my, mx, c + 1)).start()

    def hot_finish():
        for p, (_, hot, _, _, _) in enumerate(parts):
            wait_for(half_of(p, hot, 1 - c), to_sem.at[4, p])
        gate = dotf(x_ref[...], hot_g[...])
        up = dotf(x_ref[...], hot_u[...])
        u = (jax.nn.silu(gate) * up).astype(BF16)
        count = hot_tok_ref.shape[1]
        same = iota((tokens, count), 0) == hot_tok_ref[...]
        weight = jnp.sum(jnp.where(same, hot_gate_ref[...], 0.0), axis=1, keepdims=True)
        is_hot = jnp.sum(jnp.where(same, 1.0, 0.0), axis=1, keepdims=True) > 0.5
        for f in range(FOLD):
            cols = slice(f * piece, (f + 1) * piece)
            h = dotf(u, hot_d[:, cols]).astype(BF16)
            acc_ref[:, cols] += jnp.where(is_hot, weight * h.astype(F32), 0.0)

    def hot_sends_done():
        @pl.when(me == 0)
        def _():
            sent_like(1)

        for p, (_, hot, _, _, _) in enumerate(parts):
            @pl.when(on_line(p))
            def _(p=p, hot=hot):
                wait_for(pieces_like(p, hot), from_sem.at[1, p])

            wait_for(pieces_like(p, hot), from_sem.at[2, p])
            wait_for(neighbours_like(p, hot), from_sem.at[3, p])
            if n > 2:
                wait_for(quarter(p, hot, c, 0), from_sem.at[5, p])
            wait_for(half_of(p, hot, c), from_sem.at[4, p])

    def expert_of(q, i):
        return peer(q, i, 1)

    def fold(pieces):
        r = iota((main, main), 0)
        return dotf(ones_where(iota((main, main), 1) == r % FOLD * blocks + r // FOLD), pieces).astype(BF16)

    def unfold(folded):
        r = iota((main, main), 0)
        return dotf(ones_where(iota((main, main), 1) == r % blocks * FOLD + r // blocks), folded).astype(BF16)

    def pick_rows(q, count, slots):
        row = iota((count, tokens), 0)
        expert = expert_of(q, row // slots)
        member = ids_ref[0:1, :] == expert
        for j in range(1, top_k):
            member = jnp.logical_or(member, ids_ref[j:j + 1, :] == expert)
        earlier = ones_where(iota((tokens, tokens), 0) < iota((tokens, tokens), 1))
        member_f = jnp.where(member, 1.0, 0.0)
        rank = dotf(member_f.astype(BF16), earlier)
        slot = (row % slots).astype(F32) if slots > 1 else float(SLOTS)
        return jnp.where(rank == slot, member_f, 0.0).astype(BF16)

    def fill(q):
        pick = pick_rows(q, main, SLOTS)
        ninth = pick_rows(q, blocks, 1)
        for f in range(FOLD):
            cols = slice(f * piece, (f + 1) * piece)
            send[q, :, :, cols] = dotf(pick, x_ref[:, cols]).astype(BF16).reshape(blocks, SLOTS, piece)
            fold_ref[f * blocks:(f + 1) * blocks] = dotf(ninth, x_ref[:, cols]).astype(BF16)
        send[q, :, :, d_model:] = fold(fold_ref[...]).reshape(blocks, FOLD, piece)

    def start_sends(q, src, dst, relay, way, s_sem, r_sem, sign):
        first = int(q == 0) if isinstance(q, int) else jnp.where(q == 0, 1, 0)
        if relayed:
            @pl.loop(0, blocks)
            def _(i):
                @pl.when(is_relayed(q, i))
                def _():
                    remote(src.at[q, i], relay.at[q, i], s_sem.at[q], mid_sem.at[way, q], hop(q, i, sign, 0)).start()

        @pl.loop(first, blocks)
        def _(i):
            def direct():
                remote(src.at[q, i], dst.at[q, i], s_sem.at[q], r_sem.at[q], peer(q, i, sign)).start()
            if relayed:
                pl.when(jnp.logical_not(is_relayed(q, i)))(direct)
            else:
                direct()

    def wait_relay(q, relay, sem):
        for count in sorted({relay_count(k) for k in range(chunks)}):
            alike = [k for k in range(chunks) if relay_count(k) == count]
            if isinstance(q, int):
                if q in alike:
                    wait_for(relay.at[q, pl.ds(0, count)], sem)
            else:
                same = functools.reduce(jnp.logical_or, [q == k for k in alike])

                @pl.when(same)
                def _(count=count):
                    wait_for(relay.at[q, pl.ds(0, count)], sem)

    def pass_on(q, dst, relay, way, r_sem, sign):
        if not relayed:
            return
        wait_relay(q, relay, mid_sem.at[way, q])

        @pl.loop(0, blocks)
        def _(i):
            @pl.when(is_relayed(q, i))
            def _():
                remote(relay.at[q, i], dst.at[q, i], on_sem.at[way, q], r_sem.at[q], hop(q, i, sign, 1)).start()

    def pass_on_sent(q):
        pass_on(q, recv, relay_out, 0, recv_sem, 1)

    def pass_on_returned(q):
        pass_on(q, back, relay_back, 1, back_sem, -1)

    def wait_chunk(q, buf, sem):
        if isinstance(q, int):
            wait_for(buf.at[0, pl.ds(1, blocks - 1)] if q == 0 else buf.at[q], sem.at[q])
            return

        @pl.when(q == 0)
        def _():
            wait_for(buf.at[0, pl.ds(1, blocks - 1)], sem.at[0])

        @pl.when(q > 0)
        def _():
            wait_for(buf.at[q], sem.at[q])

    def load_rows(q, buf):
        rows_ref[:main] = buf[q, :, :, :d_model].reshape(main, d_model)
        pieces = unfold(buf[q, :, :, d_model:].reshape(main, piece))
        for f in range(FOLD):
            rows_ref[main:, f * piece:(f + 1) * piece] = pieces[f * blocks:(f + 1) * blocks]

    def send_chunk(q):
        start_sends(q, send, recv, relay_out, 0, send_sem, recv_sem, 1)

    width = 256 if d_ff % 256 == 0 else d_ff

    def expert(q):
        wait_chunk(q, recv, recv_sem)
        load_rows(q, recv)
        for w in range(d_ff // width):
            cols = slice(w * width, (w + 1) * width)
            gate = dotf(rows_ref[...], wg[:, cols])
            up = dotf(rows_ref[...], wu[:, cols])
            u_ref[:, cols] = (jax.nn.silu(gate) * up).astype(BF16)
        for f in range(FOLD):
            cols = slice(f * piece, (f + 1) * piece)
            res = dotf(u_ref[...], wd[:, cols]).astype(BF16)
            out[q, :, :, cols] = res[:main].reshape(blocks, SLOTS, piece)
            fold_ref[f * blocks:(f + 1) * blocks] = res[main:]
        out[q, :, :, d_model:] = fold(fold_ref[...]).reshape(blocks, FOLD, piece)

    def return_chunk(q):
        start_sends(q, out, back, relay_back, 1, ret_sem, back_sem, -1)

    def fill_weights(q):
        def weights(count, slots):
            row = iota((count, tokens), 0)
            expert = expert_of(q, row // slots)
            member = ids_ref[0:1, :] == expert
            weight = jnp.where(member, gates_ref[0:1, :], 0.0)
            for j in range(1, top_k):
                here = ids_ref[j:j + 1, :] == expert
                member = jnp.logical_or(member, here)
                weight = jnp.where(here, gates_ref[j:j + 1, :], weight)
            earlier = ones_where(iota((tokens, tokens), 0) < iota((tokens, tokens), 1))
            rank = dotf(ones_where(member), earlier)
            slot = (row % slots).astype(F32) if slots > 1 else float(SLOTS)
            return jnp.where(rank == slot, weight, 0.0)
        weight_ref[q, :, :main] = three_terms(weights(main, SLOTS).T)
        weight_ref[q, :, main:] = three_terms(weights(blocks, 1).T)

    def add_returned(q):
        wait_chunk(q, back, back_sem)
        load_rows(q, back)
        for f in range(FOLD):
            cols = slice(f * piece, (f + 1) * piece)
            terms = dotf(weight_ref[q], rows_ref[:, cols])
            acc_ref[:, cols] += terms[2 * tokens:] + terms[tokens:2 * tokens] + terms[:tokens]

    def others_wait():
        for copy in own:
            copy.wait()
        pl.semaphore_wait(barrier, devices - 1)

    pl.loop(0, chunks)(fill)
    recv[0, 0] = send[0, 0]
    acc_ref[...] = jnp.zeros_like(acc_ref)
    pl.when(me == 0)(hot_root)
    pl.when(me != 0)(others_wait)
    half = chunks // 2
    pl.loop(0, half)(send_chunk)
    pl.loop(0, chunks)(fill_weights)
    pass_on_sent(0)
    pl.loop(half, half + half // 2)(send_chunk)
    pass_on_sent(1)
    hot_scatter()
    pl.loop(half + half // 2, chunks)(send_chunk)
    pl.loop(2, min(LEAD, chunks))(pass_on_sent)
    hot_plane()

    @pl.loop(0, chunks)
    def _(q):
        @pl.when(q < chunks - LEAD)
        def _():
            pass_on_sent(q + LEAD)

        expert(q)

        @pl.when(q == 0)
        def _():
            back[0, 0] = out[0, 0]

        return_chunk(q)

        @pl.when(q >= min(LAG, chunks))
        def _():
            pass_on_returned(q - min(LAG, chunks))

        @pl.when(q == chunks // 2 + 1)
        def _():
            hot_line()

    lag = min(LAG, chunks)

    @pl.loop(0, lag)
    def _(j):
        pass_on_returned(chunks - lag + j)

        @pl.when(j == lag // 2)
        def _():
            hot_opposite()

        @pl.when(j >= lag // 2)
        def _():
            add_returned(j - lag // 2)

    pl.loop(lag - lag // 2, chunks // 2)(add_returned)
    hot_core()
    pl.loop(chunks // 2, chunks - 1)(add_returned)
    hot_finish()
    add_returned(chunks - 1)
    y_ref[...] = acc_ref[...].astype(BF16)

    @pl.loop(0, chunks)
    def _(q):
        wait_chunk(q, send, send_sem)
        wait_chunk(q, out, ret_sem)
        if relayed:
            wait_relay(q, relay_out, on_sem.at[0, q])
            wait_relay(q, relay_back, on_sem.at[1, q])
    hot_sends_done()


def solution(mesh):
    group_size = mesh.shape['ep']
    n = 1
    while 2 * n * n * n < group_size:
        n += 1
    row_spec = P(('dp', 'ep'), None)
    list_spec = P(('dp', 'ep'))
    expert_spec = P('ep', None, None)

    def local_layer(x, ids, gates, hot_tok, hot_gates, wg, wu, wd):
        wg, wu, wd = wg[0], wu[0], wd[0]
        tokens, d_model = x.shape
        d_ff = wg.shape[1]
        chunks = SPLIT * n
        blocks = 2 * n * n // SPLIT
        piece = d_model // FOLD
        main = blocks * SLOTS
        block_buf = pltpu.VMEM((chunks, blocks, SLOTS, d_model + piece), BF16)
        in_vmem = pl.BlockSpec(memory_space=pltpu.VMEM)
        in_hbm = pl.BlockSpec(memory_space=pl.ANY)
        dma = pltpu.SemaphoreType.DMA
        weights = [pltpu.VMEM((d_model, d_ff), BF16)] * 2 + [pltpu.VMEM((d_ff, d_model), BF16)]
        return pl.pallas_call(
            functools.partial(layer_kernel, n),
            out_shape=jax.ShapeDtypeStruct((tokens, d_model), BF16),
            in_specs=[in_vmem] * 5 + [in_hbm] * 3,
            out_specs=in_vmem,
            scratch_shapes=[block_buf] * 6 + weights + weights
            + [pltpu.VMEM((d_model // (2 * n), d_ff), BF16)] * 2 + [pltpu.VMEM((d_ff // n, d_model // 2), BF16)]
            + [pltpu.VMEM((main + blocks, d_model), BF16), pltpu.VMEM((main + blocks, d_ff), BF16),
               pltpu.VMEM((main, piece), BF16), pltpu.VMEM((chunks, 3 * tokens, main + blocks), BF16), pltpu.VMEM((tokens, d_model), F32)]
            + [dma((3,))] + [dma((chunks,))] * 4 + [dma((2, chunks))] * 2 + [dma((7, 3)), dma((6, 3))],
            compiler_params=pltpu.CompilerParams(vmem_limit_bytes=VMEM_LIMIT, collective_id=0, has_side_effects=True),
            name="moe_layer",
        )(ids.T, gates.T, hot_tok[None, :], hot_gates[None, :], x, wg, wu, wd)

    return jax.shard_map(local_layer, mesh=mesh,
                         in_specs=(row_spec, row_spec, row_spec, list_spec, list_spec, expert_spec, expert_spec, expert_spec),
                         out_specs=row_spec, check_vma=False)
```

```python
import functools

import jax
import jax.numpy as jnp
from jax import lax
from jax.experimental import pallas as pl
from jax.experimental.pallas import tpu as pltpu
from jax.sharding import PartitionSpec as P

F32 = jnp.float32
BF16 = jnp.bfloat16
SLOTS = 8
FOLD = 8
VMEM_LIMIT = 60 * 1024 * 1024
SPLIT = 2
LEAD = 4
LAG = 6


def dotf(a, b):
    return jnp.dot(a, b, preferred_element_type=F32)


def iota(shape, dim):
    return lax.broadcasted_iota(jnp.int32, shape, dim)


def ones_where(mask):
    return jnp.where(mask, 1.0, 0.0).astype(BF16)


def three_terms(a):
    hi = a.astype(BF16)
    rest = a - hi.astype(F32)
    mid = rest.astype(BF16)
    low = (rest - mid.astype(F32)).astype(BF16)
    return jnp.concatenate([hi, mid, low], axis=0)


def layer_kernel(n, ids_ref, gates_ref, hot_tok_ref, hot_gate_ref, x_ref, wg_ref, wu_ref, wd_ref, y_ref,
                 send, recv, out, back, relay_out, relay_back, wg, wu, wd, hot_g, hot_u, hot_d, stage_g, stage_u, stage_d,
                 rows_ref, u_ref, fold_ref, weight_ref, acc_ref,
                 load_sem, send_sem, recv_sem, ret_sem, back_sem, mid_sem, on_sem, from_sem, to_sem):
    me = lax.axis_index('ep')
    devices = 2 * n * n * n
    c, mx, my, mz = me % 2, (me // 2) % n, (me // (2 * n)) % n, me // (2 * n * n)
    chunks = SPLIT * n
    blocks = 2 * n * n // SPLIT
    tokens, d_model = x_ref.shape
    d_ff = wd_ref.shape[0]
    top_k = ids_ref.shape[0]
    piece = d_model // FOLD
    main = blocks * SLOTS
    chunk_rows = main + blocks

    def device(z, y, x, core):
        return ((z % n * n + y % n) * n + x % n) * 2 + core % 2

    def steps(q, i):
        kx, ky = (i // 2) % n, i // (2 * n) * SPLIT + q % SPLIT
        return i % 2, kx, ky, (q // SPLIT + 2 * n - kx - ky) % n

    def peer(q, i, sign):
        kc, kx, ky, kz = steps(q, i)
        if sign > 0:
            return device(mz + kz, my + ky, mx + kx, c + kc)
        return device(mz + n - kz, my + n - ky, mx + n - kx, c + kc)

    relayed = n == 4

    def opposite(k):
        return k == n // 2

    def is_relayed(q, i):
        kc, kx, ky, kz = steps(q, i)
        return jnp.logical_and(kc == 1, jnp.logical_or(jnp.logical_or(opposite(kx), opposite(ky)), opposite(kz)))

    def relay_count(q):
        return sum(any(opposite(k) for k in steps(q, i)[1:]) for i in range(1, blocks, 2))

    def hop(q, i, sign, leg):
        kc, kx, ky, kz = steps(q, i)
        move = [jnp.where(opposite(k), n - 1, k if leg == 0 else 0) for k in (kz, ky, kx)]
        if sign < 0:
            move = [n - m for m in move]
        return device(mz + move[0], my + move[1], mx + move[2], c + kc if leg == 0 else c)

    def remote(src, dst, s_sem, r_sem, to):
        return pltpu.make_async_remote_copy(src_ref=src, dst_ref=dst, send_sem=s_sem, recv_sem=r_sem, device_id={'ep': to},
                                            device_id_type=pl.DeviceIdType.MESH)

    def wait_for(ref, sem):
        pltpu.make_async_copy(ref, ref, sem).wait()

    def rows_at(ref, start, size, unit):
        return ref.at[pl.ds(pl.multiple_of(start, unit), size)]

    barrier = pltpu.get_barrier_semaphore()

    def signal_all():
        @pl.loop(1, devices)
        def _(i):
            pl.semaphore_signal(barrier, inc=1, device_id={'ep': (me + i) % devices}, device_id_type=pl.DeviceIdType.MESH)

    pl.when(me != 0)(signal_all)

    own = [pltpu.make_async_copy(src, dst, load_sem.at[p])
           for p, (src, dst) in enumerate(((wg_ref, wg), (wu_ref, wu), (wd_ref, wd)))]
    for copy in own:
        copy.start()

    unit = d_model // (2 * n * n * n)
    unit_d, unit_c = d_ff // (n * n), d_model // (2 * n)
    parts = ((wg, hot_g, stage_g, mz, (my, mx)), (wu, hot_u, stage_u, mx, (mz, my)), (wd, hot_d, stage_d, my, (mx, mz)))

    def line_device(p, k, core):
        return (device(k, my, mx, core), device(mz, my, k, core), device(mz, k, mx, core))[p]

    def plane_device(p, a, b):
        return (device(mz, a, b, c), device(a, b, mx, c), device(b, my, a, c))[p]

    def quarter(p, ref, half, k):
        if p < 2:
            size = n * n * unit
            return rows_at(ref, half * (d_model // 2) + k * size, size, 16)
        size = n * unit_d
        return ref.at[pl.ds(pl.multiple_of(k * size, 16), size), pl.ds(pl.multiple_of(half * (d_model // 2), 128), d_model // 2)]

    def hot_piece(p, ref, half, k, a, b):
        if p < 2:
            return rows_at(ref, half * (d_model // 2) + k * (n * n * unit) + (a * n + b) * unit, unit, 16)
        return ref.at[pl.ds(pl.multiple_of(k * (n * unit_d) + a * unit_d, 16), unit_d),
                      pl.ds(pl.multiple_of(half * (d_model // 2) + b * unit_c, 128), unit_c)]

    def stage_piece(p, ref, a, b):
        if p < 2:
            return rows_at(ref, (a * n + b) * unit, unit, 16)
        return ref.at[pl.ds(pl.multiple_of(a * unit_d, 16), unit_d), pl.ds(pl.multiple_of(b * unit_c, 128), unit_c)]

    def pieces_like(p, ref):
        if p < 2:
            return ref.at[pl.ds(0, (n * n - 1) * unit)]
        return ref.at[pl.ds(0, (n * n - 1) * unit_d), pl.ds(0, unit_c)]

    def on_line(p):
        plane = parts[p][4]
        return jnp.logical_and(plane[0] == 0, plane[1] == 0)

    def sent_like(late):
        count = 1 if late else 2 * n - 2
        for p, (src, _, _, _, _) in enumerate(parts):
            wait_for(src.at[pl.ds(0, count * (n * n * unit if p < 2 else n * unit_d // 2))], from_sem.at[6 * late, p])

    def hot_root():
        for copy in own:
            copy.wait()
        pl.semaphore_wait(barrier, devices - 1)
        order = [(k, half) for k in (*range(n // 2, n), 0, *range(n // 2 - 1, 0, -1)) for half in range(2)]
        for k, half in order:
            for p, (src, _, stage, _, _) in enumerate(parts):
                if k > 0 or half > 0:
                    remote(quarter(p, src, half, k), stage, from_sem.at[0 if (k, half) != order[-1] else 6, p], to_sem.at[0, p],
                           line_device(p, k, half)).start()
        for p, (src, _, stage, _, _) in enumerate(parts):
            stage[...] = quarter(p, src, 0, 0)[...]
        sent_like(0)
        signal_all()

    def hot_scatter():
        for p, (_, hot, stage, line, _) in enumerate(parts):
            @pl.when(on_line(p))
            def _(p=p, hot=hot, stage=stage, line=line):
                @pl.when(me != 0)
                def _():
                    wait_for(stage, to_sem.at[0, p])

                @pl.loop(1, n * n)
                def _(j):
                    a, b = j // n, j % n
                    remote(stage_piece(p, stage, a, b), hot_piece(p, hot, c, line, a, b), from_sem.at[1, p], to_sem.at[1, p],
                           plane_device(p, a, b)).start()
                hot_piece(p, hot, c, line, 0, 0)[...] = stage_piece(p, stage, 0, 0)[...]

    def hot_plane():
        for p, (_, hot, _, line, plane) in enumerate(parts):
            mine = hot_piece(p, hot, c, line, plane[0], plane[1])

            @pl.when(jnp.logical_not(on_line(p)))
            def _(p=p, mine=mine):
                wait_for(mine, to_sem.at[1, p])

            @pl.loop(1, n * n)
            def _(j, p=p, mine=mine, plane=plane):
                remote(mine, mine, from_sem.at[2, p], to_sem.at[2, p], plane_device(p, plane[0] + j // n, plane[1] + j % n)).start()

    def part_of_quarter(p, ref, half, k, which):
        if p < 2:
            size = n * n * unit // 2
            return rows_at(ref, half * (d_model // 2) + (2 * k + which) * size, size, 16)
        size = n * unit_d // 2
        return ref.at[pl.ds(pl.multiple_of((2 * k + which) * size, 16), size), pl.ds(pl.multiple_of(half * (d_model // 2), 128), d_model // 2)]

    def hot_line():
        for p, (_, hot, _, line, _) in enumerate(parts):
            wait_for(pieces_like(p, hot), to_sem.at[2, p])
            mine = quarter(p, hot, c, line)
            remote(mine, mine, from_sem.at[3, p], to_sem.at[3, p], line_device(p, line + 1, c)).start()
            if n > 2:
                remote(mine, mine, from_sem.at[3, p], to_sem.at[3, p], line_device(p, line + n - 1, c)).start()

    def hot_opposite():
        for p, (_, hot, _, line, _) in enumerate(parts):
            wait_for(neighbours_like(p, hot), to_sem.at[3, p])
            if n > 2:
                first = part_of_quarter(p, hot, c, (line + n - 1) % n, 0)
                second = part_of_quarter(p, hot, c, (line + 1) % n, 1)
                remote(first, first, from_sem.at[5, p], to_sem.at[5, p], line_device(p, line + 1, c)).start()
                remote(second, second, from_sem.at[5, p], to_sem.at[5, p], line_device(p, line + n - 1, c)).start()

    def neighbours_like(p, ref):
        count = min(2, n - 1)
        if p < 2:
            return ref.at[pl.ds(0, count * n * n * unit)]
        return ref.at[pl.ds(0, count * n * unit_d), pl.ds(0, d_model // 2)]

    def half_of(p, ref, half):
        if p < 2:
            return rows_at(ref, half * (d_model // 2), d_model // 2, 16)
        return ref.at[:, pl.ds(pl.multiple_of(half * (d_model // 2), 128), d_model // 2)]

    def hot_core():
        for p, (_, hot, _, _, _) in enumerate(parts):
            if n > 2:
                wait_for(quarter(p, hot, c, 0), to_sem.at[5, p])
            mine = half_of(p, hot, c)
            remote(mine, mine, from_sem.at[4, p], to_sem.at[4, p], device(mz, my, mx, c + 1)).start()

    def hot_finish():
        for p, (_, hot, _, _, _) in enumerate(parts):
            wait_for(half_of(p, hot, 1 - c), to_sem.at[4, p])
        gate = dotf(x_ref[...], hot_g[...])
        up = dotf(x_ref[...], hot_u[...])
        u = (jax.nn.silu(gate) * up).astype(BF16)
        count = hot_tok_ref.shape[1]
        same = iota((tokens, count), 0) == hot_tok_ref[...]
        weight = jnp.sum(jnp.where(same, hot_gate_ref[...], 0.0), axis=1, keepdims=True)
        is_hot = jnp.sum(jnp.where(same, 1.0, 0.0), axis=1, keepdims=True) > 0.5
        for f in range(FOLD):
            cols = slice(f * piece, (f + 1) * piece)
            h = dotf(u, hot_d[:, cols]).astype(BF16)
            acc_ref[:, cols] += jnp.where(is_hot, weight * h.astype(F32), 0.0)

    def hot_sends_done():
        @pl.when(me == 0)
        def _():
            sent_like(1)

        for p, (_, hot, _, _, _) in enumerate(parts):
            @pl.when(on_line(p))
            def _(p=p, hot=hot):
                wait_for(pieces_like(p, hot), from_sem.at[1, p])

            wait_for(pieces_like(p, hot), from_sem.at[2, p])
            wait_for(neighbours_like(p, hot), from_sem.at[3, p])
            if n > 2:
                wait_for(quarter(p, hot, c, 0), from_sem.at[5, p])
            wait_for(half_of(p, hot, c), from_sem.at[4, p])

    def expert_of(q, i):
        return peer(q, i, 1)

    def fold(pieces):
        r = iota((main, main), 0)
        return dotf(ones_where(iota((main, main), 1) == r % FOLD * blocks + r // FOLD), pieces).astype(BF16)

    def unfold(folded):
        r = iota((main, main), 0)
        return dotf(ones_where(iota((main, main), 1) == r % blocks * FOLD + r // blocks), folded).astype(BF16)

    def pick_rows(q, count, slots):
        row = iota((count, tokens), 0)
        expert = expert_of(q, row // slots)
        member = ids_ref[0:1, :] == expert
        for j in range(1, top_k):
            member = jnp.logical_or(member, ids_ref[j:j + 1, :] == expert)
        earlier = ones_where(iota((tokens, tokens), 0) < iota((tokens, tokens), 1))
        member_f = jnp.where(member, 1.0, 0.0)
        rank = dotf(member_f.astype(BF16), earlier)
        slot = (row % slots).astype(F32) if slots > 1 else float(SLOTS)
        return jnp.where(rank == slot, member_f, 0.0).astype(BF16)

    def fill(q):
        pick = pick_rows(q, main, SLOTS)
        ninth = pick_rows(q, blocks, 1)
        for f in range(FOLD):
            cols = slice(f * piece, (f + 1) * piece)
            send[q, :, :, cols] = dotf(pick, x_ref[:, cols]).astype(BF16).reshape(blocks, SLOTS, piece)
            fold_ref[f * blocks:(f + 1) * blocks] = dotf(ninth, x_ref[:, cols]).astype(BF16)
        send[q, :, :, d_model:] = fold(fold_ref[...]).reshape(blocks, FOLD, piece)

    def start_sends(q, src, dst, relay, way, s_sem, r_sem, sign):
        first = int(q == 0) if isinstance(q, int) else jnp.where(q == 0, 1, 0)
        if relayed:
            @pl.loop(0, blocks)
            def _(i):
                @pl.when(is_relayed(q, i))
                def _():
                    remote(src.at[q, i], relay.at[q, i], s_sem.at[q], mid_sem.at[way, q], hop(q, i, sign, 0)).start()

        @pl.loop(first, blocks)
        def _(i):
            def direct():
                remote(src.at[q, i], dst.at[q, i], s_sem.at[q], r_sem.at[q], peer(q, i, sign)).start()
            if relayed:
                pl.when(jnp.logical_not(is_relayed(q, i)))(direct)
            else:
                direct()

    def wait_relay(q, relay, sem):
        for count in sorted({relay_count(k) for k in range(chunks)}):
            alike = [k for k in range(chunks) if relay_count(k) == count]
            if isinstance(q, int):
                if q in alike:
                    wait_for(relay.at[q, pl.ds(0, count)], sem)
            else:
                same = functools.reduce(jnp.logical_or, [q == k for k in alike])

                @pl.when(same)
                def _(count=count):
                    wait_for(relay.at[q, pl.ds(0, count)], sem)

    def pass_on(q, dst, relay, way, r_sem, sign):
        if not relayed:
            return
        wait_relay(q, relay, mid_sem.at[way, q])

        @pl.loop(0, blocks)
        def _(i):
            @pl.when(is_relayed(q, i))
            def _():
                remote(relay.at[q, i], dst.at[q, i], on_sem.at[way, q], r_sem.at[q], hop(q, i, sign, 1)).start()

    def pass_on_sent(q):
        pass_on(q, recv, relay_out, 0, recv_sem, 1)

    def pass_on_returned(q):
        pass_on(q, back, relay_back, 1, back_sem, -1)

    def wait_chunk(q, buf, sem):
        if isinstance(q, int):
            wait_for(buf.at[0, pl.ds(1, blocks - 1)] if q == 0 else buf.at[q], sem.at[q])
            return

        @pl.when(q == 0)
        def _():
            wait_for(buf.at[0, pl.ds(1, blocks - 1)], sem.at[0])

        @pl.when(q > 0)
        def _():
            wait_for(buf.at[q], sem.at[q])

    def load_rows(q, buf):
        rows_ref[:main] = buf[q, :, :, :d_model].reshape(main, d_model)
        pieces = unfold(buf[q, :, :, d_model:].reshape(main, piece))
        for f in range(FOLD):
            rows_ref[main:, f * piece:(f + 1) * piece] = pieces[f * blocks:(f + 1) * blocks]

    def send_chunk(q):
        start_sends(q, send, recv, relay_out, 0, send_sem, recv_sem, 1)

    width = 256 if d_ff % 256 == 0 else d_ff

    def expert(q):
        wait_chunk(q, recv, recv_sem)
        load_rows(q, recv)
        for w in range(d_ff // width):
            cols = slice(w * width, (w + 1) * width)
            gate = dotf(rows_ref[...], wg[:, cols])
            up = dotf(rows_ref[...], wu[:, cols])
            u_ref[:, cols] = (jax.nn.silu(gate) * up).astype(BF16)
        for f in range(FOLD):
            cols = slice(f * piece, (f + 1) * piece)
            res = dotf(u_ref[...], wd[:, cols]).astype(BF16)
            out[q, :, :, cols] = res[:main].reshape(blocks, SLOTS, piece)
            fold_ref[f * blocks:(f + 1) * blocks] = res[main:]
        out[q, :, :, d_model:] = fold(fold_ref[...]).reshape(blocks, FOLD, piece)

    def return_chunk(q):
        start_sends(q, out, back, relay_back, 1, ret_sem, back_sem, -1)

    def fill_weights(q):
        def weights(count, slots):
            row = iota((count, tokens), 0)
            expert = expert_of(q, row // slots)
            member = ids_ref[0:1, :] == expert
            weight = jnp.where(member, gates_ref[0:1, :], 0.0)
            for j in range(1, top_k):
                here = ids_ref[j:j + 1, :] == expert
                member = jnp.logical_or(member, here)
                weight = jnp.where(here, gates_ref[j:j + 1, :], weight)
            earlier = ones_where(iota((tokens, tokens), 0) < iota((tokens, tokens), 1))
            rank = dotf(ones_where(member), earlier)
            slot = (row % slots).astype(F32) if slots > 1 else float(SLOTS)
            return jnp.where(rank == slot, weight, 0.0)
        weight_ref[q, :, :main] = three_terms(weights(main, SLOTS).T)
        weight_ref[q, :, main:] = three_terms(weights(blocks, 1).T)

    def add_returned(q):
        wait_chunk(q, back, back_sem)
        load_rows(q, back)
        for f in range(FOLD):
            cols = slice(f * piece, (f + 1) * piece)
            terms = dotf(weight_ref[q], rows_ref[:, cols])
            acc_ref[:, cols] += terms[2 * tokens:] + terms[tokens:2 * tokens] + terms[:tokens]

    def others_wait():
        for copy in own:
            copy.wait()
        pl.semaphore_wait(barrier, devices - 1)

    pl.loop(0, chunks)(fill)
    recv[0, 0] = send[0, 0]
    acc_ref[...] = jnp.zeros_like(acc_ref)
    pl.when(me == 0)(hot_root)
    pl.when(me != 0)(others_wait)
    half = chunks // 2
    pl.loop(0, half)(send_chunk)
    pl.loop(0, chunks)(fill_weights)
    pass_on_sent(0)
    pl.loop(half, half + half // 2)(send_chunk)
    pass_on_sent(1)
    hot_scatter()
    pl.loop(half + half // 2, chunks)(send_chunk)
    pl.loop(2, min(LEAD, chunks))(pass_on_sent)

    @pl.loop(0, chunks)
    def _(q):
        @pl.when(q < chunks - LEAD)
        def _():
            pass_on_sent(q + LEAD)

        expert(q)

        @pl.when(q == 0)
        def _():
            back[0, 0] = out[0, 0]
            hot_plane()

        return_chunk(q)

        @pl.when(q >= min(LAG, chunks))
        def _():
            pass_on_returned(q - min(LAG, chunks))

        @pl.when(q == chunks // 2 + 1)
        def _():
            hot_line()

    lag = min(LAG, chunks)

    @pl.loop(0, lag)
    def _(j):
        pass_on_returned(chunks - lag + j)

        @pl.when(j == lag // 2)
        def _():
            hot_opposite()

        @pl.when(j >= lag // 2)
        def _():
            add_returned(j - lag // 2)

    pl.loop(lag - lag // 2, chunks // 2)(add_returned)
    hot_core()
    pl.loop(chunks // 2, chunks - 1)(add_returned)
    hot_finish()
    add_returned(chunks - 1)
    y_ref[...] = acc_ref[...].astype(BF16)

    @pl.loop(0, chunks)
    def _(q):
        wait_chunk(q, send, send_sem)
        wait_chunk(q, out, ret_sem)
        if relayed:
            wait_relay(q, relay_out, on_sem.at[0, q])
            wait_relay(q, relay_back, on_sem.at[1, q])
    hot_sends_done()


def solution(mesh):
    group_size = mesh.shape['ep']
    n = 1
    while 2 * n * n * n < group_size:
        n += 1
    row_spec = P(('dp', 'ep'), None)
    list_spec = P(('dp', 'ep'))
    expert_spec = P('ep', None, None)

    def local_layer(x, ids, gates, hot_tok, hot_gates, wg, wu, wd):
        wg, wu, wd = wg[0], wu[0], wd[0]
        tokens, d_model = x.shape
        d_ff = wg.shape[1]
        chunks = SPLIT * n
        blocks = 2 * n * n // SPLIT
        piece = d_model // FOLD
        main = blocks * SLOTS
        block_buf = pltpu.VMEM((chunks, blocks, SLOTS, d_model + piece), BF16)
        in_vmem = pl.BlockSpec(memory_space=pltpu.VMEM)
        in_hbm = pl.BlockSpec(memory_space=pl.ANY)
        dma = pltpu.SemaphoreType.DMA
        weights = [pltpu.VMEM((d_model, d_ff), BF16)] * 2 + [pltpu.VMEM((d_ff, d_model), BF16)]
        return pl.pallas_call(
            functools.partial(layer_kernel, n),
            out_shape=jax.ShapeDtypeStruct((tokens, d_model), BF16),
            in_specs=[in_vmem] * 5 + [in_hbm] * 3,
            out_specs=in_vmem,
            scratch_shapes=[block_buf] * 6 + weights + weights
            + [pltpu.VMEM((d_model // (2 * n), d_ff), BF16)] * 2 + [pltpu.VMEM((d_ff // n, d_model // 2), BF16)]
            + [pltpu.VMEM((main + blocks, d_model), BF16), pltpu.VMEM((main + blocks, d_ff), BF16),
               pltpu.VMEM((main, piece), BF16), pltpu.VMEM((chunks, 3 * tokens, main + blocks), BF16), pltpu.VMEM((tokens, d_model), F32)]
            + [dma((3,))] + [dma((chunks,))] * 4 + [dma((2, chunks))] * 2 + [dma((7, 3)), dma((6, 3))],
            compiler_params=pltpu.CompilerParams(vmem_limit_bytes=VMEM_LIMIT, collective_id=0, has_side_effects=True),
            name="moe_layer",
        )(ids.T, gates.T, hot_tok[None, :], hot_gates[None, :], x, wg, wu, wd)

    return jax.shard_map(local_layer, mesh=mesh,
                         in_specs=(row_spec, row_spec, row_spec, list_spec, list_spec, expert_spec, expert_spec, expert_spec),
                         out_specs=row_spec, check_vma=False)
```

```python
import functools

import jax
import jax.numpy as jnp
from jax import lax
from jax.experimental import pallas as pl
from jax.experimental.pallas import tpu as pltpu
from jax.sharding import PartitionSpec as P

F32 = jnp.float32
BF16 = jnp.bfloat16
SLOTS = 8
FOLD = 8
VMEM_LIMIT = 60 * 1024 * 1024
SPLIT = 2
LEAD = 4
LAG = 6


def dotf(a, b):
    return jnp.dot(a, b, preferred_element_type=F32)


def iota(shape, dim):
    return lax.broadcasted_iota(jnp.int32, shape, dim)


def ones_where(mask):
    return jnp.where(mask, 1.0, 0.0).astype(BF16)


def three_terms(a):
    hi = a.astype(BF16)
    rest = a - hi.astype(F32)
    mid = rest.astype(BF16)
    low = (rest - mid.astype(F32)).astype(BF16)
    return jnp.concatenate([hi, mid, low], axis=0)


def layer_kernel(n, ids_ref, gates_ref, hot_tok_ref, hot_gate_ref, x_ref, wg_ref, wu_ref, wd_ref, y_ref,
                 send, recv, out, back, relay_out, relay_back, wg, wu, wd, hot_g, hot_u, hot_d, stage_g, stage_u, stage_d,
                 rows_ref, u_ref, fold_ref, weight_ref, acc_ref,
                 load_sem, send_sem, recv_sem, ret_sem, back_sem, mid_sem, on_sem, from_sem, to_sem):
    me = lax.axis_index('ep')
    devices = 2 * n * n * n
    c, mx, my, mz = me % 2, (me // 2) % n, (me // (2 * n)) % n, me // (2 * n * n)
    chunks = SPLIT * n
    blocks = 2 * n * n // SPLIT
    tokens, d_model = x_ref.shape
    d_ff = wd_ref.shape[0]
    top_k = ids_ref.shape[0]
    piece = d_model // FOLD
    main = blocks * SLOTS
    chunk_rows = main + blocks

    def device(z, y, x, core):
        return ((z % n * n + y % n) * n + x % n) * 2 + core % 2

    def steps(q, i):
        kx, ky = (i // 2) % n, i // (2 * n) * SPLIT + q % SPLIT
        return i % 2, kx, ky, (q // SPLIT + 2 * n - kx - ky) % n

    def peer(q, i, sign):
        kc, kx, ky, kz = steps(q, i)
        if sign > 0:
            return device(mz + kz, my + ky, mx + kx, c + kc)
        return device(mz + n - kz, my + n - ky, mx + n - kx, c + kc)

    relayed = n == 4

    def opposite(k):
        return k == n // 2

    def is_relayed(q, i):
        _, kx, ky, kz = steps(q, i)
        return jnp.logical_or(jnp.logical_or(opposite(kx), opposite(ky)), opposite(kz))

    def relay_count(q):
        return sum(any(opposite(k) for k in steps(q, i)[1:]) for i in range(blocks))

    def hop(q, i, sign, leg):
        kc, kx, ky, kz = steps(q, i)
        way = jnp.where(kc == 0, 1, n - 1)
        move = [jnp.where(opposite(k), way, k if leg == 0 else 0) for k in (kz, ky, kx)]
        if sign < 0:
            move = [n - m for m in move]
        return device(mz + move[0], my + move[1], mx + move[2], c + kc if leg == 0 else c)

    def remote(src, dst, s_sem, r_sem, to):
        return pltpu.make_async_remote_copy(src_ref=src, dst_ref=dst, send_sem=s_sem, recv_sem=r_sem, device_id={'ep': to},
                                            device_id_type=pl.DeviceIdType.MESH)

    def wait_for(ref, sem):
        pltpu.make_async_copy(ref, ref, sem).wait()

    def rows_at(ref, start, size, unit):
        return ref.at[pl.ds(pl.multiple_of(start, unit), size)]

    barrier = pltpu.get_barrier_semaphore()

    def signal_all():
        @pl.loop(1, devices)
        def _(i):
            pl.semaphore_signal(barrier, inc=1, device_id={'ep': (me + i) % devices}, device_id_type=pl.DeviceIdType.MESH)

    pl.when(me != 0)(signal_all)

    own = [pltpu.make_async_copy(src, dst, load_sem.at[p])
           for p, (src, dst) in enumerate(((wg_ref, wg), (wu_ref, wu), (wd_ref, wd)))]
    for copy in own:
        copy.start()

    unit = d_model // (2 * n * n * n)
    unit_d, unit_c = d_ff // (n * n), d_model // (2 * n)
    parts = ((wg, hot_g, stage_g, mz, (my, mx)), (wu, hot_u, stage_u, mx, (mz, my)), (wd, hot_d, stage_d, my, (mx, mz)))

    def line_device(p, k, core):
        return (device(k, my, mx, core), device(mz, my, k, core), device(mz, k, mx, core))[p]

    def plane_device(p, a, b):
        return (device(mz, a, b, c), device(a, b, mx, c), device(b, my, a, c))[p]

    def quarter(p, ref, half, k):
        if p < 2:
            size = n * n * unit
            return rows_at(ref, half * (d_model // 2) + k * size, size, 16)
        size = n * unit_d
        return ref.at[pl.ds(pl.multiple_of(k * size, 16), size), pl.ds(pl.multiple_of(half * (d_model // 2), 128), d_model // 2)]

    def hot_piece(p, ref, half, k, a, b):
        if p < 2:
            return rows_at(ref, half * (d_model // 2) + k * (n * n * unit) + (a * n + b) * unit, unit, 16)
        return ref.at[pl.ds(pl.multiple_of(k * (n * unit_d) + a * unit_d, 16), unit_d),
                      pl.ds(pl.multiple_of(half * (d_model // 2) + b * unit_c, 128), unit_c)]

    def stage_piece(p, ref, a, b):
        if p < 2:
            return rows_at(ref, (a * n + b) * unit, unit, 16)
        return ref.at[pl.ds(pl.multiple_of(a * unit_d, 16), unit_d), pl.ds(pl.multiple_of(b * unit_c, 128), unit_c)]

    def pieces_like(p, ref):
        if p < 2:
            return ref.at[pl.ds(0, (n * n - 1) * unit)]
        return ref.at[pl.ds(0, (n * n - 1) * unit_d), pl.ds(0, unit_c)]

    def on_line(p):
        plane = parts[p][4]
        return jnp.logical_and(plane[0] == 0, plane[1] == 0)

    def sent_like(late):
        count = 1 if late else 2 * n - 2
        for p, (src, _, _, _, _) in enumerate(parts):
            wait_for(src.at[pl.ds(0, count * (n * n * unit if p < 2 else n * unit_d // 2))], from_sem.at[6 * late, p])

    def hot_root():
        for copy in own:
            copy.wait()
        pl.semaphore_wait(barrier, devices - 1)
        order = [(k, half) for k in (*range(n // 2, n), 0, *range(n // 2 - 1, 0, -1)) for half in range(2)]
        for k, half in order:
            for p, (src, _, stage, _, _) in enumerate(parts):
                if k > 0 or half > 0:
                    remote(quarter(p, src, half, k), stage, from_sem.at[0 if (k, half) != order[-1] else 6, p], to_sem.at[0, p],
                           line_device(p, k, half)).start()
        for p, (src, _, stage, _, _) in enumerate(parts):
            stage[...] = quarter(p, src, 0, 0)[...]
        sent_like(0)
        signal_all()

    def hot_scatter():
        for p, (_, hot, stage, line, _) in enumerate(parts):
            @pl.when(on_line(p))
            def _(p=p, hot=hot, stage=stage, line=line):
                @pl.when(me != 0)
                def _():
                    wait_for(stage, to_sem.at[0, p])

                @pl.loop(1, n * n)
                def _(j):
                    a, b = j // n, j % n
                    remote(stage_piece(p, stage, a, b), hot_piece(p, hot, c, line, a, b), from_sem.at[1, p], to_sem.at[1, p],
                           plane_device(p, a, b)).start()
                hot_piece(p, hot, c, line, 0, 0)[...] = stage_piece(p, stage, 0, 0)[...]

    def hot_plane():
        for p, (_, hot, _, line, plane) in enumerate(parts):
            mine = hot_piece(p, hot, c, line, plane[0], plane[1])

            @pl.when(jnp.logical_not(on_line(p)))
            def _(p=p, mine=mine):
                wait_for(mine, to_sem.at[1, p])

            @pl.loop(1, n * n)
            def _(j, p=p, mine=mine, plane=plane):
                remote(mine, mine, from_sem.at[2, p], to_sem.at[2, p], plane_device(p, plane[0] + j // n, plane[1] + j % n)).start()

    def part_of_quarter(p, ref, half, k, which):
        if p < 2:
            size = n * n * unit // 2
            return rows_at(ref, half * (d_model // 2) + (2 * k + which) * size, size, 16)
        size = n * unit_d // 2
        return ref.at[pl.ds(pl.multiple_of((2 * k + which) * size, 16), size), pl.ds(pl.multiple_of(half * (d_model // 2), 128), d_model // 2)]

    def hot_line():
        for p, (_, hot, _, line, _) in enumerate(parts):
            wait_for(pieces_like(p, hot), to_sem.at[2, p])
            mine = quarter(p, hot, c, line)
            remote(mine, mine, from_sem.at[3, p], to_sem.at[3, p], line_device(p, line + 1, c)).start()
            if n > 2:
                remote(mine, mine, from_sem.at[3, p], to_sem.at[3, p], line_device(p, line + n - 1, c)).start()

    def hot_opposite():
        for p, (_, hot, _, line, _) in enumerate(parts):
            wait_for(neighbours_like(p, hot), to_sem.at[3, p])
            if n > 2:
                first = part_of_quarter(p, hot, c, (line + n - 1) % n, 0)
                second = part_of_quarter(p, hot, c, (line + 1) % n, 1)
                remote(first, first, from_sem.at[5, p], to_sem.at[5, p], line_device(p, line + 1, c)).start()
                remote(second, second, from_sem.at[5, p], to_sem.at[5, p], line_device(p, line + n - 1, c)).start()

    def neighbours_like(p, ref):
        count = min(2, n - 1)
        if p < 2:
            return ref.at[pl.ds(0, count * n * n * unit)]
        return ref.at[pl.ds(0, count * n * unit_d), pl.ds(0, d_model // 2)]

    def half_of(p, ref, half):
        if p < 2:
            return rows_at(ref, half * (d_model // 2), d_model // 2, 16)
        return ref.at[:, pl.ds(pl.multiple_of(half * (d_model // 2), 128), d_model // 2)]

    def hot_core():
        for p, (_, hot, _, _, _) in enumerate(parts):
            if n > 2:
                wait_for(quarter(p, hot, c, 0), to_sem.at[5, p])
            mine = half_of(p, hot, c)
            remote(mine, mine, from_sem.at[4, p], to_sem.at[4, p], device(mz, my, mx, c + 1)).start()

    def hot_finish():
        for p, (_, hot, _, _, _) in enumerate(parts):
            wait_for(half_of(p, hot, 1 - c), to_sem.at[4, p])
        gate = dotf(x_ref[...], hot_g[...])
        up = dotf(x_ref[...], hot_u[...])
        u = (jax.nn.silu(gate) * up).astype(BF16)
        count = hot_tok_ref.shape[1]
        same = iota((tokens, count), 0) == hot_tok_ref[...]
        weight = jnp.sum(jnp.where(same, hot_gate_ref[...], 0.0), axis=1, keepdims=True)
        is_hot = jnp.sum(jnp.where(same, 1.0, 0.0), axis=1, keepdims=True) > 0.5
        for f in range(FOLD):
            cols = slice(f * piece, (f + 1) * piece)
            h = dotf(u, hot_d[:, cols]).astype(BF16)
            acc_ref[:, cols] += jnp.where(is_hot, weight * h.astype(F32), 0.0)

    def hot_sends_done():
        @pl.when(me == 0)
        def _():
            sent_like(1)

        for p, (_, hot, _, _, _) in enumerate(parts):
            @pl.when(on_line(p))
            def _(p=p, hot=hot):
                wait_for(pieces_like(p, hot), from_sem.at[1, p])

            wait_for(pieces_like(p, hot), from_sem.at[2, p])
            wait_for(neighbours_like(p, hot), from_sem.at[3, p])
            if n > 2:
                wait_for(quarter(p, hot, c, 0), from_sem.at[5, p])
            wait_for(half_of(p, hot, c), from_sem.at[4, p])

    def expert_of(q, i):
        return peer(q, i, 1)

    def fold(pieces):
        r = iota((main, main), 0)
        return dotf(ones_where(iota((main, main), 1) == r % FOLD * blocks + r // FOLD), pieces).astype(BF16)

    def unfold(folded):
        r = iota((main, main), 0)
        return dotf(ones_where(iota((main, main), 1) == r % blocks * FOLD + r // blocks), folded).astype(BF16)

    def pick_rows(q, count, slots):
        row = iota((count, tokens), 0)
        expert = expert_of(q, row // slots)
        member = ids_ref[0:1, :] == expert
        for j in range(1, top_k):
            member = jnp.logical_or(member, ids_ref[j:j + 1, :] == expert)
        earlier = ones_where(iota((tokens, tokens), 0) < iota((tokens, tokens), 1))
        member_f = jnp.where(member, 1.0, 0.0)
        rank = dotf(member_f.astype(BF16), earlier)
        slot = (row % slots).astype(F32) if slots > 1 else float(SLOTS)
        return jnp.where(rank == slot, member_f, 0.0).astype(BF16)

    def fill(q):
        pick = pick_rows(q, main, SLOTS)
        ninth = pick_rows(q, blocks, 1)
        for f in range(FOLD):
            cols = slice(f * piece, (f + 1) * piece)
            send[q, :, :, cols] = dotf(pick, x_ref[:, cols]).astype(BF16).reshape(blocks, SLOTS, piece)
            fold_ref[f * blocks:(f + 1) * blocks] = dotf(ninth, x_ref[:, cols]).astype(BF16)
        send[q, :, :, d_model:] = fold(fold_ref[...]).reshape(blocks, FOLD, piece)

    def start_sends(q, src, dst, relay, way, s_sem, r_sem, sign):
        first = int(q == 0) if isinstance(q, int) else jnp.where(q == 0, 1, 0)
        if relayed:
            @pl.loop(0, blocks)
            def _(i):
                @pl.when(is_relayed(q, i))
                def _():
                    remote(src.at[q, i], relay.at[q, i], s_sem.at[q], mid_sem.at[way, q], hop(q, i, sign, 0)).start()

        @pl.loop(first, blocks)
        def _(i):
            def direct():
                remote(src.at[q, i], dst.at[q, i], s_sem.at[q], r_sem.at[q], peer(q, i, sign)).start()
            if relayed:
                pl.when(jnp.logical_not(is_relayed(q, i)))(direct)
            else:
                direct()

    def wait_relay(q, relay, sem):
        for count in sorted({relay_count(k) for k in range(chunks)}):
            alike = [k for k in range(chunks) if relay_count(k) == count]
            if isinstance(q, int):
                if q in alike:
                    wait_for(relay.at[q, pl.ds(0, count)], sem)
            else:
                same = functools.reduce(jnp.logical_or, [q == k for k in alike])

                @pl.when(same)
                def _(count=count):
                    wait_for(relay.at[q, pl.ds(0, count)], sem)

    def pass_on(q, dst, relay, way, r_sem, sign):
        if not relayed:
            return
        wait_relay(q, relay, mid_sem.at[way, q])

        @pl.loop(0, blocks)
        def _(i):
            @pl.when(is_relayed(q, i))
            def _():
                remote(relay.at[q, i], dst.at[q, i], on_sem.at[way, q], r_sem.at[q], hop(q, i, sign, 1)).start()

    def pass_on_sent(q):
        pass_on(q, recv, relay_out, 0, recv_sem, 1)

    def pass_on_returned(q):
        pass_on(q, back, relay_back, 1, back_sem, -1)

    def wait_chunk(q, buf, sem):
        if isinstance(q, int):
            wait_for(buf.at[0, pl.ds(1, blocks - 1)] if q == 0 else buf.at[q], sem.at[q])
            return

        @pl.when(q == 0)
        def _():
            wait_for(buf.at[0, pl.ds(1, blocks - 1)], sem.at[0])

        @pl.when(q > 0)
        def _():
            wait_for(buf.at[q], sem.at[q])

    def load_rows(q, buf):
        rows_ref[:main] = buf[q, :, :, :d_model].reshape(main, d_model)
        pieces = unfold(buf[q, :, :, d_model:].reshape(main, piece))
        for f in range(FOLD):
            rows_ref[main:, f * piece:(f + 1) * piece] = pieces[f * blocks:(f + 1) * blocks]

    def send_chunk(q):
        start_sends(q, send, recv, relay_out, 0, send_sem, recv_sem, 1)

    width = 256 if d_ff % 256 == 0 else d_ff

    def expert(q):
        wait_chunk(q, recv, recv_sem)
        load_rows(q, recv)
        for w in range(d_ff // width):
            cols = slice(w * width, (w + 1) * width)
            gate = dotf(rows_ref[...], wg[:, cols])
            up = dotf(rows_ref[...], wu[:, cols])
            u_ref[:, cols] = (jax.nn.silu(gate) * up).astype(BF16)
        for f in range(FOLD):
            cols = slice(f * piece, (f + 1) * piece)
            res = dotf(u_ref[...], wd[:, cols]).astype(BF16)
            out[q, :, :, cols] = res[:main].reshape(blocks, SLOTS, piece)
            fold_ref[f * blocks:(f + 1) * blocks] = res[main:]
        out[q, :, :, d_model:] = fold(fold_ref[...]).reshape(blocks, FOLD, piece)

    def return_chunk(q):
        start_sends(q, out, back, relay_back, 1, ret_sem, back_sem, -1)

    def fill_weights(q):
        def weights(count, slots):
            row = iota((count, tokens), 0)
            expert = expert_of(q, row // slots)
            member = ids_ref[0:1, :] == expert
            weight = jnp.where(member, gates_ref[0:1, :], 0.0)
            for j in range(1, top_k):
                here = ids_ref[j:j + 1, :] == expert
                member = jnp.logical_or(member, here)
                weight = jnp.where(here, gates_ref[j:j + 1, :], weight)
            earlier = ones_where(iota((tokens, tokens), 0) < iota((tokens, tokens), 1))
            rank = dotf(ones_where(member), earlier)
            slot = (row % slots).astype(F32) if slots > 1 else float(SLOTS)
            return jnp.where(rank == slot, weight, 0.0)
        weight_ref[q, :, :main] = three_terms(weights(main, SLOTS).T)
        weight_ref[q, :, main:] = three_terms(weights(blocks, 1).T)

    def add_returned(q):
        wait_chunk(q, back, back_sem)
        load_rows(q, back)
        for f in range(FOLD):
            cols = slice(f * piece, (f + 1) * piece)
            terms = dotf(weight_ref[q], rows_ref[:, cols])
            acc_ref[:, cols] += terms[2 * tokens:] + terms[tokens:2 * tokens] + terms[:tokens]

    def others_wait():
        for copy in own:
            copy.wait()
        pl.semaphore_wait(barrier, devices - 1)

    pl.loop(0, chunks)(fill)
    recv[0, 0] = send[0, 0]
    acc_ref[...] = jnp.zeros_like(acc_ref)
    pl.when(me == 0)(hot_root)
    pl.when(me != 0)(others_wait)
    half = chunks // 2
    pl.loop(0, half)(send_chunk)
    pl.loop(0, chunks)(fill_weights)
    pass_on_sent(0)
    pl.loop(half, half + half // 2)(send_chunk)
    pass_on_sent(1)
    hot_scatter()
    pl.loop(half + half // 2, chunks)(send_chunk)
    pl.loop(2, min(LEAD, chunks))(pass_on_sent)

    @pl.loop(0, chunks)
    def _(q):
        @pl.when(q < chunks - LEAD)
        def _():
            pass_on_sent(q + LEAD)

        expert(q)

        @pl.when(q == 0)
        def _():
            back[0, 0] = out[0, 0]
            hot_plane()

        return_chunk(q)

        @pl.when(q >= min(LAG, chunks))
        def _():
            pass_on_returned(q - min(LAG, chunks))

        @pl.when(q == chunks // 2 + 1)
        def _():
            hot_line()

    lag = min(LAG, chunks)

    @pl.loop(0, lag)
    def _(j):
        pass_on_returned(chunks - lag + j)

        @pl.when(j == lag // 2)
        def _():
            hot_opposite()

        @pl.when(j >= lag // 2)
        def _():
            add_returned(j - lag // 2)

    pl.loop(lag - lag // 2, chunks // 2)(add_returned)
    hot_core()
    pl.loop(chunks // 2, chunks - 1)(add_returned)
    hot_finish()
    add_returned(chunks - 1)
    y_ref[...] = acc_ref[...].astype(BF16)

    @pl.loop(0, chunks)
    def _(q):
        wait_chunk(q, send, send_sem)
        wait_chunk(q, out, ret_sem)
        if relayed:
            wait_relay(q, relay_out, on_sem.at[0, q])
            wait_relay(q, relay_back, on_sem.at[1, q])
    hot_sends_done()


def solution(mesh):
    group_size = mesh.shape['ep']
    n = 1
    while 2 * n * n * n < group_size:
        n += 1
    row_spec = P(('dp', 'ep'), None)
    list_spec = P(('dp', 'ep'))
    expert_spec = P('ep', None, None)

    def local_layer(x, ids, gates, hot_tok, hot_gates, wg, wu, wd):
        wg, wu, wd = wg[0], wu[0], wd[0]
        tokens, d_model = x.shape
        d_ff = wg.shape[1]
        chunks = SPLIT * n
        blocks = 2 * n * n // SPLIT
        piece = d_model // FOLD
        main = blocks * SLOTS
        block_buf = pltpu.VMEM((chunks, blocks, SLOTS, d_model + piece), BF16)
        in_vmem = pl.BlockSpec(memory_space=pltpu.VMEM)
        in_hbm = pl.BlockSpec(memory_space=pl.ANY)
        dma = pltpu.SemaphoreType.DMA
        weights = [pltpu.VMEM((d_model, d_ff), BF16)] * 2 + [pltpu.VMEM((d_ff, d_model), BF16)]
        return pl.pallas_call(
            functools.partial(layer_kernel, n),
            out_shape=jax.ShapeDtypeStruct((tokens, d_model), BF16),
            in_specs=[in_vmem] * 5 + [in_hbm] * 3,
            out_specs=in_vmem,
            scratch_shapes=[block_buf] * 6 + weights + weights
            + [pltpu.VMEM((d_model // (2 * n), d_ff), BF16)] * 2 + [pltpu.VMEM((d_ff // n, d_model // 2), BF16)]
            + [pltpu.VMEM((main + blocks, d_model), BF16), pltpu.VMEM((main + blocks, d_ff), BF16),
               pltpu.VMEM((main, piece), BF16), pltpu.VMEM((chunks, 3 * tokens, main + blocks), BF16), pltpu.VMEM((tokens, d_model), F32)]
            + [dma((3,))] + [dma((chunks,))] * 4 + [dma((2, chunks))] * 2 + [dma((7, 3)), dma((6, 3))],
            compiler_params=pltpu.CompilerParams(vmem_limit_bytes=VMEM_LIMIT, collective_id=0, has_side_effects=True),
            name="moe_layer",
        )(ids.T, gates.T, hot_tok[None, :], hot_gates[None, :], x, wg, wu, wd)

    return jax.shard_map(local_layer, mesh=mesh,
                         in_specs=(row_spec, row_spec, row_spec, list_spec, list_spec, expert_spec, expert_spec, expert_spec),
                         out_specs=row_spec, check_vma=False)
```
